256 devices in a mesh: row: 8 (over y, core), col: 16 (over z_lo, x), mp: 2 (over z_hi).
Axes of the slice: x: 4, y: 4, z: 8 (z_hi: 2, z_lo: 4; z = z_hi * 4 + z_lo), core: 2. Of those that a mesh axis runs over, the one named last changes fastest.
Arguments:
- video: bfloat16 [3, 4, 192, 6144], P(None, None, 'row', 'col'), may hold values from -6 to 6
- grad_tokens: bfloat16 [2, 16, 512, 1024], P(None, 'row', 'col', 'mp'), may hold values from -6 to 6
- weight: bfloat16 [3072, 1024], P(None, 'mp'), may hold values from -0.1875 to 0.1875
Outputs:
- video_grad: float32 [3, 4, 192, 6144], P(None, 'mp', 'row', 'col')
- weight_grad: float32 [3072, 1024], P(('row', 'col'), 'mp')
The draws below stay inside these ranges and needn't reach their ends.
All inputs are finite; a program needn't handle non-finite values.
Results may differ from the reference program's by a relative error of at most 0.0003.
Values may be sent and summed in bfloat16 or wider, within the bound.
A program may use at most 64 MiB of HBM per device.

```python
import jax
import jax.numpy as jnp
from jax import lax

D = 1024
PATCH = 3072
TT = 2
FRAMES = 4
NTH = 16
NTW = 512
HEIGHT = 192
WIDTH = 6144


def shard_levels(rng, dims, split, smallest, largest):
    factor_of = 1.0
    for dim, shards_of in split:
        heights = jax.random.uniform(jax.random.fold_in(jax.random.fold_in(rng, 6), dim), (shards_of,), jnp.float32, smallest / len(split), largest / len(split))
        factor_of = factor_of * jnp.repeat(jnp.exp(heights), dims[dim] // shards_of).reshape((-1,) + (1,) * (len(dims) - 1 - dim))
    return factor_of


def gaussian(own_key, extent, spread, bound, cuts=(), kind=jnp.bfloat16):
    result = spread * jax.random.normal(own_key, extent, jnp.float32)
    if cuts:
        result = result * shard_levels(own_key, extent, cuts, -0.22, 0.18)
    return jnp.clip(result, -bound, bound).astype(kind)


def setup_inputs(seed: int = 0) -> dict:
    key_of = jax.random.split(jax.random.key(seed), 4)
    return {
        "video": gaussian(key_of[0], (3, FRAMES, HEIGHT, WIDTH), 1.0, 6.0, ((2, 8), (3, 16))),
        "grad_tokens": gaussian(key_of[1], (TT, NTH, NTW, D), 1.0, 6.0, ((1, 8), (2, 16), (3, 2))),
        "weight": gaussian(key_of[2], (PATCH, D), D ** -0.5, 0.1875, ((1, 2),)),
    }


def unfold_axis(ext, axis, count, stride, kernel):
    extra = max(0, 2 * stride - kernel)
    widths = [(0, 0)] * ext.ndim
    widths[axis] = (0, extra)
    ext = jnp.pad(ext, widths)
    lower = lax.slice_in_dim(ext, 0, count * stride, axis=axis)
    upper = lax.slice_in_dim(ext, stride, stride + count * stride, axis=axis)
    shaped = ext.shape[:axis] + (count, stride) + ext.shape[axis + 1:]
    lower = lower.reshape(shaped)
    upper = lax.slice_in_dim(upper.reshape(shaped), 0, kernel - stride, axis=axis + 1)
    return jnp.concatenate([lower, upper], axis=axis + 1)

def fold_axis(pieces, axis, stride, kernel):
    count = pieces.shape[axis]
    lower = lax.slice_in_dim(pieces, 0, stride, axis=axis + 1)
    upper = lax.slice_in_dim(pieces, stride, kernel, axis=axis + 1)
    pad_lower = [(0, 0)] * pieces.ndim
    pad_upper = [(0, 0)] * pieces.ndim
    pad_lower[axis] = (0, 1)
    pad_upper[axis] = (1, 0)
    pad_upper[axis + 1] = (0, 2 * stride - kernel)
    total = jnp.pad(lower, pad_lower) + jnp.pad(upper, pad_upper)
    merged = total.reshape(pieces.shape[:axis] + ((count + 1) * stride,) + pieces.shape[axis + 2:])
    return lax.slice_in_dim(merged, 0, count * stride + kernel - stride, axis=axis)

def reference(video, grad_tokens, weight):
    padded = jnp.pad(video, ((0, 0), (1, 1), (2, 2), (2, 2)))
    steps, rows, cols, width = grad_tokens.shape
    patch = weight.shape[0]
    zero = jnp.int32(0)
    field = jnp.zeros((3, 2 * steps + 2, padded.shape[2], padded.shape[3]), jnp.float32)
    weight_sum = jnp.zeros((patch, width), jnp.float32)

    def one_step(carry, index):
        weight_sum, field = carry
        start = (2 * index).astype(jnp.int32)
        frames = lax.dynamic_slice_in_dim(padded, start, 4, 1)
        pieces = unfold_axis(unfold_axis(frames, 2, rows, 12, 16), 4, cols, 12, 16)
        pieces = pieces.transpose(2, 4, 0, 1, 3, 5).reshape(rows * cols, patch)
        tokens = lax.dynamic_index_in_dim(grad_tokens, index, 0, keepdims=False).reshape(rows * cols, width)
        weight_sum = weight_sum + lax.dot_general(pieces, tokens, (((0,), (0,)), ((), ())), preferred_element_type=jnp.float32)
        grads = lax.dot_general(tokens, weight, (((1,), (1,)), ((), ())), preferred_element_type=jnp.float32)
        grads = grads.reshape(rows, cols, 3, 4, 16, 16).transpose(2, 3, 0, 4, 1, 5)
        grads = fold_axis(fold_axis(grads, 4, 12, 16), 2, 12, 16)
        old = lax.dynamic_slice(field, (zero, start, zero, zero), grads.shape)
        field = lax.dynamic_update_slice(field, old + grads, (zero, start, zero, zero))
        return ((weight_sum, field), None)
    (weight_sum, field), unused = lax.scan(one_step, (weight_sum, field), jnp.arange(steps, dtype=jnp.int32))
    video_grad = field[:, 1:-1, 2:-2, 2:-2]
    weight_grad = weight_sum * lax.rsqrt(jnp.float32(steps * rows * cols))
    return (video_grad, weight_grad)
```

```python
import jax
import jax.numpy as jnp
import numpy as np
from jax import lax
from jax.experimental import pallas as pl
from jax.experimental.pallas import tpu as pltpu
from jax.sharding import PartitionSpec as P

MESH = pl.DeviceIdType.MESH
F32 = jnp.float32
BF16 = jnp.bfloat16
N_SEMS = 37


def selections():
    cols = np.zeros((384, 512), np.float32)
    for e in range(16):
        for j in range(32):
            x = 12 * j + e - 2
            if 0 <= x < 384:
                cols[x, e * 32 + j] = 1
    side = np.zeros((32, 512), np.float32)
    side[2, 0] = side[3, 32] = 1
    side[16, 14 * 32 + 31] = side[17, 15 * 32 + 31] = 1
    rows = np.zeros((384, 384), np.float32)
    for cf in range(12):
        for i in range(2):
            for b in range(16):
                y = 12 * i + b - 2
                src = cf * 24 + y if 0 <= y < 24 else 288 + cf * 2 + y + 2 if y < 0 else 320 + cf * 2 + y - 24
                rows[cf * 32 + i * 16 + b, src] = 1
    pick = np.zeros((16, 384), np.float32)
    for k, x in enumerate((0, 1, 382, 383)):
        pick[k, x] = 1
    rim = np.zeros((64, 288), np.float32)
    for cf in range(12):
        for k in range(2):
            rim[cf * 2 + k, cf * 24 + 22 + k] = 1
            rim[32 + cf * 2 + k, cf * 24 + k] = 1
    ends = np.zeros((16, 128), np.float32)
    for ti in range(4):
        ends[ti, ti * 32] = 1
        ends[4 + ti, ti * 32 + 31] = 1
    beside = np.zeros((256, 128), np.float32)
    for t in range(2):
        for i4 in range(4):
            i = (1, 0, 1, 0)[i4]
            left = (2, 0, 0, 3)[i4]
            right = (4, 1, 1, 5)[i4]
            beside[t * 128 + i4 * 32, left * 16 + 4 + t * 2 + i] = 1
            beside[t * 128 + i4 * 32 + 31, right * 16 + t * 2 + i] = 1
    back = np.zeros((384, 384), np.float32)
    for e in range(12):
        for j in range(32):
            back[e * 32 + j, 12 * j + e] = 1
    return [cols, side, rows, pick, rim, ends, beside, back]


def chosen(at, values):
    out = jnp.int32(values[3])
    for k in range(3):
        out = jnp.where(at == k, jnp.int32(values[k]), out)
    return out


FRAMES_OF = ((0, 1, 2, 3), (2, 4, 5, 6), (5, 6, 7, 9), (8, 9, 10, 11))
SLOTS_OF = (
    (((4, 0, 1), (1, 2, 3))),
    (((0, 4, 1), (4, 2, 3))),
    (((0, 1, 4), (2, 4, 3))),
    (((0, 1, 2), (2, 3, 4))),
)


def dot(a, b, dims=((1,), (0,))):
    return lax.dot_general(a, b, (dims, ((), ())), preferred_element_type=F32)


def kernel(
    video, tokens, weight, cols_h, side_h, rows_h, pick_h, rim_h, ends_h, beside_h, back_h,
    vout, wout,
    cols, side, rows, pick, rim, ends, beside, back,
    wv, vs, hv, he, sb, hs, gx, ge, gbuf, qs, qw, sq, qr, rq, lm, pg, fs, ll, vg, mr,
    wg, cr, a1, xa, xb, xr1, xr2, xs1, xs2, a2, zr,
    load, send, recv,
):
    r = lax.axis_index("row")
    c = lax.axis_index("col")
    m = lax.axis_index("mp")
    y, core = r // 2, r % 2
    z, x = c // 4, c % 4

    pairs = [
        (video, vs.at[0:288]), (rim_h, rim), (pick_h, pick), (tokens, gx.at[:, 1:3]), (ends_h, ends),
        (tokens, gbuf.at[:, 0]), (cols_h, cols), (side_h, side), (rows_h, rows),
        (beside_h, beside), (back_h, back), (weight, wv),
    ]
    loads = [pltpu.make_async_copy(a, b, load.at[k]) for k, (a, b) in enumerate(pairs)]
    for one in loads:
        one.start()

    hv[...] = jnp.zeros_like(hv)
    he[...] = jnp.zeros_like(he)
    vs[288:384, :] = jnp.zeros((96, 384), BF16)
    for i4 in (0, 3):
        gx[:, i4] = jnp.zeros((2, 32, 512), BF16)
    lm[4] = jnp.zeros((16, 16, 256), BF16)

    barrier = pltpu.get_barrier_semaphore()
    up, down, lef, rig = r > 0, r < 7, c > 0, c < 15
    near = [
        (up, {"row": r - 1}), (down, {"row": r + 1}), (lef, {"col": c - 1}), (rig, {"col": c + 1}),
        (up & lef, {"row": r - 1, "col": c - 1}), (up & rig, {"row": r - 1, "col": c + 1}),
        (down & lef, {"row": r + 1, "col": c - 1}), (down & rig, {"row": r + 1, "col": c + 1}),
    ]
    yp, ym = {"row": (r + 2) % 8}, {"row": (r + 6) % 8}
    xp, xm = {"col": z * 4 + (x + 1) % 4}, {"col": z * 4 + (x + 3) % 4}
    other = {"row": y * 2 + 1 - core}
    zs = [{"col": ((z + d) % 4) * 4 + x} for d in (1, 2, 3)]
    partner = {"mp": 1 - m}

    def greet(to):
        pl.semaphore_signal(barrier, inc=1, device_id=to, device_id_type=MESH)

    for to in (yp, ym, xp, xm, other, *zs, partner):
        greet(to)
    for there, to in near:
        pl.when(there)(lambda to=to: greet(to))

    def one_if(p):
        return jnp.where(p, jnp.int32(1), jnp.int32(0))

    n_near = (1 + one_if(up) + one_if(down)) * (1 + one_if(lef) + one_if(rig)) - 1

    def remote(k, src, dst, to):
        return pltpu.make_async_remote_copy(
            src_ref=src, dst_ref=dst, send_sem=send.at[k], recv_sem=recv.at[k],
            device_id=to, device_id_type=MESH,
        )

    for k in range(5):
        loads[k].wait()
    vs[288:352, :] = dot(rim[...], vs[0:288, :]).astype(BF16)
    sb[:, 384:896] = dot(ends[...], gx[:, 1:3].reshape(128, 512)).astype(BF16)
    sb[:, 0:384] = dot(pick[...], vs[...], ((1,), (1,))).astype(BF16)
    loads[5].wait()

    pl.semaphore_wait(barrier, 9 + n_near)

    halo = [
        (remote(2, vs.at[288:320], hv.at[0:32], {"row": r + 1}), down, up),
        (remote(3, vs.at[320:352], hv.at[32:64], {"row": r - 1}), up, down),
        (remote(4, sb, he.at[0], {"col": c + 1}), rig, lef),
        (remote(5, sb, he.at[1], {"col": c - 1}), lef, rig),
        (remote(6, sb, he.at[2], {"row": r + 1, "col": c + 1}), down & rig, up & lef),
        (remote(7, sb, he.at[3], {"row": r - 1, "col": c + 1}), up & rig, down & lef),
        (remote(8, sb, he.at[4], {"row": r + 1, "col": c - 1}), down & lef, up & rig),
        (remote(9, sb, he.at[5], {"row": r - 1, "col": c - 1}), up & lef, down & rig),
        (remote(0, gx.at[:, 1], gx.at[:, 3], {"row": r - 1}), up, down),
        (remote(1, gx.at[:, 2], gx.at[:, 0], {"row": r + 1}), down, up),
    ]
    for copy, sent, _ in halo[:8]:
        pl.when(sent)(lambda copy=copy: copy.start())
    g_p = remote(16, gbuf.at[:, 0], gbuf.at[:, 1], yp)
    g_m = remote(17, gbuf.at[:, 0], gbuf.at[:, 2], ym)
    g_p.start()
    g_m.start()
    for copy, sent, _ in halo[8:]:
        pl.when(sent)(lambda copy=copy: copy.start())

    for k in (6, 7, 8):
        loads[k].wait()
    for copy, _, got in halo[:8]:
        pl.when(got)(lambda copy=copy: copy.wait_recv())
    lane = lax.broadcasted_iota(jnp.int32, (16, 128), 1)
    for k, (a, b, d) in enumerate(((0, 2, 3), (1, 4, 5))):
        hs[16 * k : 16 * k + 16, 0:256] = he[a, :, 0:256]
        tile = jnp.where(
            lane < 32, he[a, :, 256:384].astype(F32),
            jnp.where(lane < 64, he[b, :, 256:384].astype(F32), he[d, :, 256:384].astype(F32)),
        )
        hs[16 * k : 16 * k + 16, 256:384] = tile.astype(BF16)
    from_side = dot(hs[...], side[...], ((0,), (0,)))
    qs[0:288, :] = (dot(vs[0:288, :], cols[...]) + from_side[0:288]).astype(BF16)
    qs[288:384, :] = (dot(hv[...], cols[...]) + from_side[288:384]).astype(BF16)
    qw[...] = dot(rows[...], qs[...]).astype(BF16).reshape(12, 2, 16, 512)

    for d, to in ((2, 2), (0, 1), (1, 3)):
        for s in range(4):
            at = chosen((y + to) % 4, [f[s] for f in FRAMES_OF])
            sq[d, :, s] = qw[at]
    q_far_p = remote(22, sq.at[2, :, 0:2], rq.at[0], yp)
    q_far_m = remote(23, sq.at[2, :, 2:4], rq.at[1], ym)
    q_p = remote(20, sq.at[0], qr.at[1], yp)
    q_m = remote(21, sq.at[1], qr.at[2], ym)
    for one in (q_far_p, q_far_m, q_p, q_m):
        one.start()
    for s in range(4):
        at = chosen(y, [f[s] for f in FRAMES_OF])
        qr[0, :, s] = qw[at]

    g_p.wait_recv()
    gf_p = remote(18, gbuf.at[0, 1], gbuf.at[0, 3], yp)
    gf_p.start()
    g_m.wait_recv()
    gf_m = remote(19, gbuf.at[1, 2], gbuf.at[1, 3], ym)
    gf_m.start()

    for copy, _, got in halo[8:]:
        pl.when(got)(lambda copy=copy: copy.wait_recv())
    loads[9].wait()
    ge[...] = dot(beside[...], he[:, :, 384:896].reshape(128, 512)).astype(BF16)
    loads[11].wait()

    @pl.loop(0, 12)
    def _(k):
        at = pl.ds(pl.multiple_of(k * 256, 256), 256)
        for n, right in enumerate((gx[...].reshape(256, 512), ge[...])):
            block = dot(wv[at, :], right, ((1,), (1,)))
            pg[2 * n, at, :] = block[:, 0:128]
            pg[2 * n + 1, at, :] = block[:, 128:256]

    q_far_p.wait_recv()
    qf_p = remote(24, rq.at[0], qr.at[3, :, 0:2], yp)
    qf_p.start()
    q_far_m.wait_recv()
    qf_m = remote(25, rq.at[1], qr.at[3, :, 2:4], ym)
    qf_m.start()

    def frames(e, first):
        early = pg[first, pl.ds(e, 192, stride=16), :].reshape(12, 16, 128)
        late = pg[first + 1, pl.ds(e, 192, stride=16), :].reshape(12, 16, 128)
        out = []
        for ch in range(0, 12, 4):
            out += [
                early[ch + 1], early[ch + 2] + late[ch], early[ch + 3] + late[ch + 1], late[ch + 2],
            ]
        return jnp.stack(out)

    j = lax.broadcasted_iota(jnp.int32, (12, 16, 128), 2) % 32
    sub = lax.broadcasted_iota(jnp.int32, (12, 8, 128), 1)
    wrap = {0: (14, 0, 1), 1: (15, 0, 1), 10: (0, 31, 127), 11: (1, 31, 127)}
    for e in range(12):
        cell = frames(e + 2, 0)
        if e in wrap:
            far, at, by = wrap[e]
            cell = cell + jnp.where(j == at, frames(far, 2), pltpu.roll(frames(far, 0), by, 2))
        low, high = cell[:, 0:8], cell[:, 8:16]
        to_low = pltpu.roll(pltpu.roll(high, 32, 2), 4, 1)
        to_high = pltpu.roll(pltpu.roll(low, 96, 2), 4, 1)
        fs[e, :, 0:8] = low + jnp.where((sub == 2) | (sub == 3), to_low, 0.0)
        fs[e, :, 8:16] = high + jnp.where((sub == 4) | (sub == 5), to_high, 0.0)
    block = lax.broadcasted_iota(jnp.int32, (192, 128), 1) // 32
    for i in range(2):
        for k in range(3):
            row = None
            for q in range(4):
                part = fs[4 * k + q].reshape(192, 128)
                by = ((q - i - 1) * 32) % 128
                if by:
                    part = pltpu.roll(part, by, 1)
                row = part if row is None else jnp.where(block == q, part, row)
            upper = row.astype(BF16)
            ll[192 * i : 192 * i + 192, 128 * k : 128 * k + 128] = upper
            ll[384 + 192 * i : 576 + 192 * i, 128 * k : 128 * k + 128] = (row - upper.astype(F32)).astype(BF16)
    loads[10].wait()
    pixels = (dot(ll[0:384, :], back[...]) + dot(ll[384:768, :], back[...])).reshape(2, 12, 16, 384)
    for i in range(2):
        for cf in range(12):
            ch, f = cf // 4, cf % 4
            vg[f // 2, ch * 2 + f % 2, 12 * i : 12 * i + 12, :] = pixels[i, cf, 2:14, :]
    v_x = remote(36, vg.at[1 - m], mr, partner)
    v_x.start()

    for one in (q_p, q_m, qf_p, qf_m, gf_p, gf_m):
        one.wait_recv()
    block = lax.broadcasted_iota(jnp.int32, (64, 128), 1) // 32
    for k in range(4):
        for half in range(2):
            parts = [
                qr[2 * half + n // 2, n % 2, :, :, 128 * k : 128 * k + 128].astype(F32).reshape(64, 128)
                for n in range(4)
            ]
            for q in range(4):
                row = None
                for n in range(4):
                    by = ((n - q) * 32) % 128
                    part = pltpu.roll(parts[n], by, 1) if by else parts[n]
                    row = part if row is None else jnp.where(block == n, part, row)
                lm[0:4, 4 * k + q, :, 128 * half : 128 * half + 128] = row.astype(BF16).reshape(4, 16, 128)
    for ca in range(3):
        total = None
        for t in range(2):
            at = chosen(y, [s[t][ca] for s in SLOTS_OF])
            part = dot(lm[at].reshape(256, 256), gbuf[t].reshape(256, 512))
            total = part if total is None else total + part
        for e in range(16):
            for n in range(4):
                wg[n, pl.ds(ca * 256 + e, 16, stride=16), :] = total[16 * e : 16 * e + 16, 128 * n : 128 * n + 128]

    give = remote(26, wg.at[:, pl.ds((1 - core) * 384, 384)], cr, other)
    give.start()
    give.wait_recv()
    for k in range(16):
        for n in range(4):
            a1[k // 4, k % 4, :, 128 * n : 128 * n + 128] = (
                wg[n, pl.ds(core * 384 + 24 * k, 24), :] + cr[n, 24 * k : 24 * k + 24, :]
            )

    x1, x2, x3 = (x + 1) % 4, (x + 2) % 4, (x + 3) % 4
    far_p = remote(27, a1.at[0:2, x2], xa, xp)
    far_m = remote(28, a1.at[2:4, x2], xb, xm)
    near_p = remote(29, a1.at[2:4, x1], xr1.at[2:4], xp)
    near_m = remote(30, a1.at[0:2, x3], xr2.at[0:2], xm)
    for one in (far_p, far_m, near_p, near_m):
        one.start()
    far_p.wait_recv()
    xs1[...] = a1[0:2, x1] + xa[...]
    last_p = remote(31, xs1, xr1.at[0:2], xp)
    last_p.start()
    far_m.wait_recv()
    xs2[...] = a1[2:4, x3] + xb[...]
    last_m = remote(32, xs2, xr2.at[2:4], xm)
    last_m.start()
    for one in (near_p, near_m, last_p, last_m):
        one.wait_recv()
    a2[...] = a1[:, x] + xr1[...] + xr2[...]

    z_out = [remote(33 + d, a2.at[(z + d + 1) % 4], zr.at[d], zs[d]) for d in (0, 1, 2)]
    for one in z_out:
        one.start()
    v_x.wait_recv()
    vout[...] = vg[m] + mr[...]
    for one in z_out:
        one.wait_recv()
    wout[...] = (a2[z] + zr[0] + (zr[1] + zr[2])) * (1.0 / 128.0)

    for copy, sent, _ in halo:
        pl.when(sent)(lambda copy=copy: copy.wait_send())
    for one in (
        g_p, g_m, gf_p, gf_m, q_far_p, q_far_m, q_p, q_m, qf_p, qf_m, v_x, give,
        far_p, far_m, near_p, near_m, last_p, last_m, *z_out,
    ):
        one.wait_send()


def shards(video, grad_tokens, weight):
    constants = [jnp.asarray(one, BF16) for one in selections()]
    anywhere = pl.BlockSpec(memory_space=pl.ANY)
    in_vmem = pl.BlockSpec(memory_space=pltpu.VMEM)

    def v(*shape, kind=F32):
        return pltpu.VMEM(shape, kind)

    def b(*shape):
        return pltpu.VMEM(shape, BF16)

    video_grad, weight_grad = pl.pallas_call(
        kernel,
        out_shape=(
            jax.ShapeDtypeStruct((6, 24, 384), F32),
            jax.ShapeDtypeStruct((24, 512), F32),
        ),
        in_specs=[anywhere] * 11,
        out_specs=(in_vmem, in_vmem),
        scratch_shapes=[b(*one.shape) for one in constants]
        + [
            b(3072, 512), b(384, 384), b(96, 384), b(8, 16, 896), b(16, 896), b(32, 384),
            b(2, 4, 32, 512), b(256, 512), b(2, 4, 2, 32, 512), b(384, 512), b(12, 2, 16, 512),
            b(3, 2, 4, 16, 512), b(4, 2, 4, 16, 512), b(2, 2, 2, 16, 512), b(5, 16, 16, 256),
            v(4, 3072, 128), v(12, 12, 16, 128), b(768, 384), v(2, 6, 24, 384), v(6, 24, 384),
            v(4, 768, 128), v(4, 384, 128), v(4, 4, 24, 512), v(2, 24, 512), v(2, 24, 512),
            v(4, 24, 512), v(4, 24, 512), v(2, 24, 512), v(2, 24, 512), v(4, 24, 512), v(3, 24, 512),
            pltpu.SemaphoreType.DMA((12,)),
            pltpu.SemaphoreType.DMA((N_SEMS,)),
            pltpu.SemaphoreType.DMA((N_SEMS,)),
        ],
        compiler_params=pltpu.CompilerParams(
            collective_id=0, has_side_effects=True, vmem_limit_bytes=48 * 1024 * 1024
        ),
        name="tubelet_backward",
    )(video.reshape(288, 384), grad_tokens, weight, *constants)
    return video_grad.reshape(3, 2, 24, 384), weight_grad


def solution(mesh):
    return jax.shard_map(
        shards,
        mesh=mesh,
        in_specs=(P(None, None, "row", "col"), P(None, "row", "col", "mp"), P(None, "mp")),
        out_specs=(P(None, "mp", "row", "col"), P(("row", "col"), "mp")),
        check_vma=False,
    )
```

```python
import jax
import jax.numpy as jnp
import numpy as np
from jax import lax
from jax.experimental import pallas as pl
from jax.experimental.pallas import tpu as pltpu
from jax.sharding import PartitionSpec as P

MESH = pl.DeviceIdType.MESH
F32 = jnp.float32
BF16 = jnp.bfloat16
N_SEMS = 37


def selections():
    cols = np.zeros((384, 512), np.float32)
    for e in range(16):
        for j in range(32):
            x = 12 * j + e - 2
            if 0 <= x < 384:
                cols[x, e * 32 + j] = 1
    side = np.zeros((32, 512), np.float32)
    side[2, 0] = side[3, 32] = 1
    side[16, 14 * 32 + 31] = side[17, 15 * 32 + 31] = 1
    rows = np.zeros((384, 384), np.float32)
    for cf in range(12):
        for i in range(2):
            for b in range(16):
                y = 12 * i + b - 2
                src = cf * 24 + y if 0 <= y < 24 else 288 + cf * 2 + y + 2 if y < 0 else 320 + cf * 2 + y - 24
                rows[cf * 32 + i * 16 + b, src] = 1
    pick = np.zeros((16, 384), np.float32)
    for k, x in enumerate((0, 1, 382, 383)):
        pick[k, x] = 1
    rim = np.zeros((64, 288), np.float32)
    for cf in range(12):
        for k in range(2):
            rim[cf * 2 + k, cf * 24 + 22 + k] = 1
            rim[32 + cf * 2 + k, cf * 24 + k] = 1
    ends = np.zeros((16, 128), np.float32)
    for ti in range(4):
        ends[ti, ti * 32] = 1
        ends[4 + ti, ti * 32 + 31] = 1
    beside = np.zeros((256, 128), np.float32)
    for t in range(2):
        for i4 in range(4):
            i = (1, 0, 1, 0)[i4]
            left = (2, 0, 0, 3)[i4]
            right = (4, 1, 1, 5)[i4]
            beside[t * 128 + i4 * 32, left * 16 + 4 + t * 2 + i] = 1
            beside[t * 128 + i4 * 32 + 31, right * 16 + t * 2 + i] = 1
    back = np.zeros((384, 384), np.float32)
    for e in range(12):
        for j in range(32):
            back[e * 32 + j, 12 * j + e] = 1
    return [cols, side, rows, pick, rim, ends, beside, back]


def chosen(at, values):
    out = jnp.int32(values[3])
    for k in range(3):
        out = jnp.where(at == k, jnp.int32(values[k]), out)
    return out


FRAMES_OF = ((0, 1, 2, 3), (2, 4, 5, 6), (5, 6, 7, 9), (8, 9, 10, 11))
SLOTS_OF = (
    (((4, 0, 1), (1, 2, 3))),
    (((0, 4, 1), (4, 2, 3))),
    (((0, 1, 4), (2, 4, 3))),
    (((0, 1, 2), (2, 3, 4))),
)


def dot(a, b, dims=((1,), (0,))):
    return lax.dot_general(a, b, (dims, ((), ())), preferred_element_type=F32)


def kernel(
    video, tokens, weight, cols_h, side_h, rows_h, pick_h, rim_h, ends_h, beside_h, back_h,
    vout, wout,
    cols, side, rows, pick, rim, ends, beside, back,
    wv, vs, hv, he, sb, hs, gx, ge, gbuf, qs, qw, sq, qr, rq, lm, pg, fs, ll, vg, mr,
    wg, cr, a1, xa, xb, xr1, xr2, xs1, xs2, a2, zr,
    load, send, recv,
):
    r = lax.axis_index("row")
    c = lax.axis_index("col")
    m = lax.axis_index("mp")
    y, core = r // 2, r % 2
    z, x = c // 4, c % 4

    pairs = [
        (video, vs.at[0:288]), (rim_h, rim), (pick_h, pick), (tokens, gx.at[:, 1:3]), (ends_h, ends),
        (tokens, gbuf.at[:, 0]), (cols_h, cols), (side_h, side), (rows_h, rows),
        (beside_h, beside), (back_h, back), (weight, wv),
    ]
    loads = [pltpu.make_async_copy(a, b, load.at[k]) for k, (a, b) in enumerate(pairs)]
    for one in loads:
        one.start()

    hv[...] = jnp.zeros_like(hv)
    he[...] = jnp.zeros_like(he)
    vs[288:384, :] = jnp.zeros((96, 384), BF16)
    for i4 in (0, 3):
        gx[:, i4] = jnp.zeros((2, 32, 512), BF16)
    lm[4] = jnp.zeros((16, 16, 256), BF16)

    barrier = pltpu.get_barrier_semaphore()
    up, down, lef, rig = r > 0, r < 7, c > 0, c < 15
    near = [
        (up, {"row": r - 1}), (down, {"row": r + 1}), (lef, {"col": c - 1}), (rig, {"col": c + 1}),
        (up & lef, {"row": r - 1, "col": c - 1}), (up & rig, {"row": r - 1, "col": c + 1}),
        (down & lef, {"row": r + 1, "col": c - 1}), (down & rig, {"row": r + 1, "col": c + 1}),
    ]
    yp, ym = {"row": (r + 2) % 8}, {"row": (r + 6) % 8}
    xp, xm = {"col": z * 4 + (x + 1) % 4}, {"col": z * 4 + (x + 3) % 4}
    other = {"row": y * 2 + 1 - core}
    zs = [{"col": ((z + d) % 4) * 4 + x} for d in (1, 2, 3)]
    partner = {"mp": 1 - m}

    def greet(to):
        pl.semaphore_signal(barrier, inc=1, device_id=to, device_id_type=MESH)

    for to in (yp, ym, xp, xm, other, *zs, partner):
        greet(to)
    for there, to in near:
        pl.when(there)(lambda to=to: greet(to))

    def one_if(p):
        return jnp.where(p, jnp.int32(1), jnp.int32(0))

    n_near = (1 + one_if(up) + one_if(down)) * (1 + one_if(lef) + one_if(rig)) - 1

    def remote(k, src, dst, to):
        return pltpu.make_async_remote_copy(
            src_ref=src, dst_ref=dst, send_sem=send.at[k], recv_sem=recv.at[k],
            device_id=to, device_id_type=MESH,
        )

    for k in range(5):
        loads[k].wait()
    vs[288:352, :] = dot(rim[...], vs[0:288, :]).astype(BF16)
    sb[:, 384:896] = dot(ends[...], gx[:, 1:3].reshape(128, 512)).astype(BF16)
    sb[:, 0:384] = dot(pick[...], vs[...], ((1,), (1,))).astype(BF16)
    loads[5].wait()

    pl.semaphore_wait(barrier, 9 + n_near)

    halo = [
        (remote(2, vs.at[288:320], hv.at[0:32], {"row": r + 1}), down, up),
        (remote(3, vs.at[320:352], hv.at[32:64], {"row": r - 1}), up, down),
        (remote(4, sb, he.at[0], {"col": c + 1}), rig, lef),
        (remote(5, sb, he.at[1], {"col": c - 1}), lef, rig),
        (remote(6, sb, he.at[2], {"row": r + 1, "col": c + 1}), down & rig, up & lef),
        (remote(7, sb, he.at[3], {"row": r - 1, "col": c + 1}), up & rig, down & lef),
        (remote(8, sb, he.at[4], {"row": r + 1, "col": c - 1}), down & lef, up & rig),
        (remote(9, sb, he.at[5], {"row": r - 1, "col": c - 1}), up & lef, down & rig),
        (remote(0, gx.at[:, 1], gx.at[:, 3], {"row": r - 1}), up, down),
        (remote(1, gx.at[:, 2], gx.at[:, 0], {"row": r + 1}), down, up),
    ]
    for copy, sent, _ in halo[:8]:
        pl.when(sent)(lambda copy=copy: copy.start())
    g_p = remote(16, gbuf.at[:, 0], gbuf.at[:, 1], yp)
    g_m = remote(17, gbuf.at[:, 0], gbuf.at[:, 2], ym)
    g_p.start()
    g_m.start()
    for copy, sent, _ in halo[8:]:
        pl.when(sent)(lambda copy=copy: copy.start())

    for k in (6, 7, 8):
        loads[k].wait()
    for copy, _, got in halo[:8]:
        pl.when(got)(lambda copy=copy: copy.wait_recv())
    lane = lax.broadcasted_iota(jnp.int32, (16, 128), 1)
    for k, (a, b, d) in enumerate(((0, 2, 3), (1, 4, 5))):
        hs[16 * k : 16 * k + 16, 0:256] = he[a, :, 0:256]
        tile = jnp.where(
            lane < 32, he[a, :, 256:384].astype(F32),
            jnp.where(lane < 64, he[b, :, 256:384].astype(F32), he[d, :, 256:384].astype(F32)),
        )
        hs[16 * k : 16 * k + 16, 256:384] = tile.astype(BF16)
    from_side = dot(hs[...], side[...], ((0,), (0,)))
    qs[0:288, :] = (dot(vs[0:288, :], cols[...]) + from_side[0:288]).astype(BF16)
    qs[288:384, :] = (dot(hv[...], cols[...]) + from_side[288:384]).astype(BF16)
    qw[...] = dot(rows[...], qs[...]).astype(BF16).reshape(12, 2, 16, 512)

    for d, to in ((2, 2), (0, 1), (1, 3)):
        for s in range(4):
            at = chosen((y + to) % 4, [f[s] for f in FRAMES_OF])
            sq[d, :, s] = qw[at]
    q_far_p = remote(22, sq.at[2, :, 0:2], rq.at[0], yp)
    q_far_m = remote(23, sq.at[2, :, 2:4], rq.at[1], ym)
    q_p = remote(20, sq.at[0], qr.at[1], yp)
    q_m = remote(21, sq.at[1], qr.at[2], ym)
    for one in (q_far_p, q_far_m, q_p, q_m):
        one.start()
    for s in range(4):
        at = chosen(y, [f[s] for f in FRAMES_OF])
        qr[0, :, s] = qw[at]

    g_p.wait_recv()
    gf_p = remote(18, gbuf.at[0, 1], gbuf.at[0, 3], yp)
    gf_p.start()
    g_m.wait_recv()
    gf_m = remote(19, gbuf.at[1, 2], gbuf.at[1, 3], ym)
    gf_m.start()

    for copy, _, got in halo[8:]:
        pl.when(got)(lambda copy=copy: copy.wait_recv())
    loads[9].wait()
    ge[...] = dot(beside[...], he[:, :, 384:896].reshape(128, 512)).astype(BF16)
    loads[11].wait()

    @pl.loop(0, 12)
    def _(k):
        at = pl.ds(pl.multiple_of(k * 256, 256), 256)
        for n, right in enumerate((gx[...].reshape(256, 512), ge[...])):
            block = dot(wv[at, :], right, ((1,), (1,)))
            pg[2 * n, at, :] = block[:, 0:128]
            pg[2 * n + 1, at, :] = block[:, 128:256]

    q_far_p.wait_recv()
    qf_p = remote(24, rq.at[0], qr.at[3, :, 0:2], yp)
    qf_p.start()
    q_far_m.wait_recv()
    qf_m = remote(25, rq.at[1], qr.at[3, :, 2:4], ym)
    qf_m.start()

    def frames(e, first):
        early = pg[first, pl.ds(e, 192, stride=16), :].reshape(12, 16, 128)
        late = pg[first + 1, pl.ds(e, 192, stride=16), :].reshape(12, 16, 128)
        out = []
        for ch in range(0, 12, 4):
            out += [
                early[ch + 1], early[ch + 2] + late[ch], early[ch + 3] + late[ch + 1], late[ch + 2],
            ]
        return jnp.stack(out)

    j = lax.broadcasted_iota(jnp.int32, (12, 16, 128), 2) % 32
    sub = lax.broadcasted_iota(jnp.int32, (12, 8, 128), 1)
    wrap = {0: (14, 0, 1), 1: (15, 0, 1), 10: (0, 31, 127), 11: (1, 31, 127)}
    for e in range(12):
        cell = frames(e + 2, 0)
        if e in wrap:
            far, at, by = wrap[e]
            cell = cell + jnp.where(j == at, frames(far, 2), pltpu.roll(frames(far, 0), by, 2))
        low, high = cell[:, 0:8], cell[:, 8:16]
        to_low = pltpu.roll(pltpu.roll(high, 32, 2), 4, 1)
        to_high = pltpu.roll(pltpu.roll(low, 96, 2), 4, 1)
        fs[e, :, 0:8] = low + jnp.where((sub == 2) | (sub == 3), to_low, 0.0)
        fs[e, :, 8:16] = high + jnp.where((sub == 4) | (sub == 5), to_high, 0.0)
    block = lax.broadcasted_iota(jnp.int32, (192, 128), 1) // 32
    for i in range(2):
        for k in range(3):
            row = None
            for q in range(4):
                part = fs[4 * k + q].reshape(192, 128)
                by = ((q - i - 1) * 32) % 128
                if by:
                    part = pltpu.roll(part, by, 1)
                row = part if row is None else jnp.where(block == q, part, row)
            upper = row.astype(BF16)
            ll[192 * i : 192 * i + 192, 128 * k : 128 * k + 128] = upper
            ll[384 + 192 * i : 576 + 192 * i, 128 * k : 128 * k + 128] = (row - upper.astype(F32)).astype(BF16)
    loads[10].wait()
    pixels = (dot(ll[0:384, :], back[...]) + dot(ll[384:768, :], back[...])).reshape(2, 12, 16, 384)
    for i in range(2):
        for cf in range(12):
            ch, f = cf // 4, cf % 4
            vg[f // 2, ch * 2 + f % 2, 12 * i : 12 * i + 12, :] = pixels[i, cf, 2:14, :]
    v_x = remote(36, vg.at[1 - m], mr, partner)
    v_x.start()

    for one in (q_p, q_m, qf_p, qf_m, gf_p, gf_m):
        one.wait_recv()
    block = lax.broadcasted_iota(jnp.int32, (64, 128), 1) // 32
    for k in range(4):
        for half in range(2):
            parts = [
                qr[2 * half + n // 2, n % 2, :, :, 128 * k : 128 * k + 128].astype(F32).reshape(64, 128)
                for n in range(4)
            ]
            for q in range(4):
                row = None
                for n in range(4):
                    by = ((n - q) * 32) % 128
                    part = pltpu.roll(parts[n], by, 1) if by else parts[n]
                    row = part if row is None else jnp.where(block == n, part, row)
                lm[0:4, 4 * k + q, :, 128 * half : 128 * half + 128] = row.astype(BF16).reshape(4, 16, 128)
    for ca in range(3):
        total = None
        for t in range(2):
            at = chosen(y, [s[t][ca] for s in SLOTS_OF])
            part = dot(lm[at].reshape(256, 256), gbuf[t].reshape(256, 512))
            total = part if total is None else total + part
        for e in range(16):
            for n in range(4):
                wg[n, pl.ds(ca * 256 + e, 16, stride=16), :] = total[16 * e : 16 * e + 16, 128 * n : 128 * n + 128]

    give = remote(26, wg.at[:, pl.ds((1 - core) * 384, 384)], cr, other)
    give.start()
    give.wait_recv()
    for k in range(16):
        for n in range(4):
            a1[k // 4, k % 4, :, 128 * n : 128 * n + 128] = (
                wg[n, pl.ds(core * 384 + 24 * k, 24), :] + cr[n, 24 * k : 24 * k + 24, :]
            )

    x1, x2, x3 = (x + 1) % 4, (x + 2) % 4, (x + 3) % 4
    far_p = remote(27, a1.at[0:2, x2], xa, xp)
    far_m = remote(28, a1.at[2:4, x2], xb, xm)
    near_p = remote(29, a1.at[2:4, x1], xr1.at[2:4], xp)
    near_m = remote(30, a1.at[0:2, x3], xr2.at[0:2], xm)
    for one in (far_p, far_m, near_p, near_m):
        one.start()
    far_p.wait_recv()
    xs1[...] = a1[0:2, x1] + xa[...]
    last_p = remote(31, xs1, xr1.at[0:2], xp)
    last_p.start()
    far_m.wait_recv()
    xs2[...] = a1[2:4, x3] + xb[...]
    last_m = remote(32, xs2, xr2.at[2:4], xm)
    last_m.start()
    for one in (near_p, near_m, last_p, last_m):
        one.wait_recv()
    a2[...] = a1[:, x] + xr1[...] + xr2[...]

    z_out = [remote(33 + d, a2.at[(z + d + 1) % 4], zr.at[d], zs[d]) for d in (0, 1, 2)]
    for one in z_out:
        one.start()
    v_x.wait_recv()
    vout[...] = vg[m] + mr[...]
    for one in z_out:
        one.wait_recv()
    wout[...] = (a2[z] + zr[0] + (zr[1] + zr[2])) * (1.0 / 128.0)

    for copy, sent, _ in halo:
        pl.when(sent)(lambda copy=copy: copy.wait_send())
    for one in (
        g_p, g_m, gf_p, gf_m, q_far_p, q_far_m, q_p, q_m, qf_p, qf_m, v_x, give,
        far_p, far_m, near_p, near_m, last_p, last_m, *z_out,
    ):
        one.wait_send()


def shards(video, grad_tokens, weight):
    constants = [jnp.asarray(one, BF16) for one in selections()]
    anywhere = pl.BlockSpec(memory_space=pl.ANY)
    in_vmem = pl.BlockSpec(memory_space=pltpu.VMEM)

    def v(*shape, kind=F32):
        return pltpu.VMEM(shape, kind)

    def b(*shape):
        return pltpu.VMEM(shape, BF16)

    video_grad, weight_grad = pl.pallas_call(
        kernel,
        out_shape=(
            jax.ShapeDtypeStruct((6, 24, 384), F32),
            jax.ShapeDtypeStruct((24, 512), F32),
        ),
        in_specs=[anywhere] * 11,
        out_specs=(in_vmem, in_vmem),
        scratch_shapes=[b(*one.shape) for one in constants]
        + [
            b(3072, 512), b(384, 384), b(96, 384), b(8, 16, 896), b(16, 896), b(32, 384),
            b(2, 4, 32, 512), b(256, 512), b(2, 4, 2, 32, 512), b(384, 512), b(12, 2, 16, 512),
            b(3, 2, 4, 16, 512), b(4, 2, 4, 16, 512), b(2, 2, 2, 16, 512), b(5, 16, 16, 256),
            v(4, 3072, 128), v(12, 12, 16, 128), b(768, 384), v(2, 6, 24, 384), v(6, 24, 384),
            v(4, 768, 128), v(4, 384, 128), v(4, 4, 24, 512), v(2, 24, 512), v(2, 24, 512),
            v(4, 24, 512), v(4, 24, 512), v(2, 24, 512), v(2, 24, 512), v(4, 24, 512), v(3, 24, 512),
            pltpu.SemaphoreType.DMA((12,)),
            pltpu.SemaphoreType.DMA((N_SEMS,)),
            pltpu.SemaphoreType.DMA((N_SEMS,)),
        ],
        compiler_params=pltpu.CompilerParams(
            collective_id=0, has_side_effects=True, vmem_limit_bytes=67043328
        ),
        name="tubelet_backward",
    )(video.reshape(288, 384), grad_tokens, weight, *constants)
    return video_grad.reshape(3, 2, 24, 384), weight_grad


def solution(mesh):
    return jax.shard_map(
        shards,
        mesh=mesh,
        in_specs=(P(None, None, "row", "col"), P(None, "row", "col", "mp"), P(None, "mp")),
        out_specs=(P(None, "mp", "row", "col"), P(("row", "col"), "mp")),
        check_vma=False,
    )
```

```python
import jax
import jax.numpy as jnp
import numpy as np
from jax import lax
from jax.experimental import pallas as pl
from jax.experimental.pallas import tpu as pltpu
from jax.sharding import PartitionSpec as P

MESH = pl.DeviceIdType.MESH
F32 = jnp.float32
BF16 = jnp.bfloat16
N_SEMS = 64
VMEM_BYTES = 56500000
PIECES = 2
WIDE = 4 // PIECES
SELECTION_AT = (0, 16, 80, 96, 480, 512, 896, 1152)
SELECTION_ROWS = 1536


def selections():
    cols = np.zeros((384, 512), np.float32)
    for e in range(16):
        for j in range(32):
            x = 12 * j + e - 2
            if 0 <= x < 384:
                cols[x, e * 32 + j] = 1
    side = np.zeros((32, 512), np.float32)
    side[2, 0] = side[3, 32] = 1
    side[16, 14 * 32 + 31] = side[17, 15 * 32 + 31] = 1
    rows = np.zeros((384, 384), np.float32)
    for cf in range(12):
        for i in range(2):
            for b in range(16):
                y = 12 * i + b - 2
                src = cf * 24 + y if 0 <= y < 24 else 288 + cf * 2 + y + 2 if y < 0 else 320 + cf * 2 + y - 24
                rows[cf * 32 + i * 16 + b, src] = 1
    pick = np.zeros((16, 384), np.float32)
    for k, x in enumerate((0, 1, 382, 383)):
        pick[k, x] = 1
    rim = np.zeros((64, 288), np.float32)
    for cf in range(12):
        for k in range(2):
            rim[cf * 2 + k, cf * 24 + 22 + k] = 1
            rim[32 + cf * 2 + k, cf * 24 + k] = 1
    ends = np.zeros((16, 128), np.float32)
    for ti in range(4):
        ends[ti, ti * 32] = 1
        ends[4 + ti, ti * 32 + 31] = 1
    beside = np.zeros((256, 128), np.float32)
    for t in range(2):
        for i4 in range(4):
            i = (1, 0, 1, 0)[i4]
            left = (2, 0, 0, 3)[i4]
            right = (4, 1, 1, 5)[i4]
            beside[t * 128 + i4 * 32, left * 16 + 4 + t * 2 + i] = 1
            beside[t * 128 + i4 * 32 + 31, right * 16 + t * 2 + i] = 1
    back = np.zeros((384, 384), np.float32)
    for e in range(12):
        for j in range(32):
            back[e * 32 + j, 12 * j + e] = 1
    packed = np.zeros((SELECTION_ROWS, 512), np.float32)
    for at, one in zip(SELECTION_AT, (pick, rim, ends, cols, side, rows, beside, back)):
        packed[at : at + one.shape[0], : one.shape[1]] = one
    return packed


def chosen(at, values):
    out = jnp.int32(values[3])
    for k in range(3):
        out = jnp.where(at == k, jnp.int32(values[k]), out)
    return out


FRAMES_OF = ((0, 1, 2, 3), (2, 4, 5, 6), (5, 6, 7, 9), (8, 9, 10, 11))
SLOTS_OF = (
    (((4, 0, 1), (1, 2, 3))),
    (((0, 4, 1), (4, 2, 3))),
    (((0, 1, 4), (2, 4, 3))),
    (((0, 1, 2), (2, 3, 4))),
)


def dot(a, b, dims=((1,), (0,))):
    return lax.dot_general(a, b, (dims, ((), ())), preferred_element_type=F32)


def kernel(
    video, tokens, weight, packed,
    vout, wout,
    sel,
    wv, vs, hv, he, hg, sb, sg, hs, qf, gx, ge, gbuf, qs, qw, sq, qr, rq, lm, pg, fs, ll, vg, mr,
    wg, cr, a1, xa, xb, xr1, xr2, xs1, xs2, a2, zr,
    load, send, recv,
):
    r = lax.axis_index("row")
    c = lax.axis_index("col")
    m = lax.axis_index("mp")
    y, core = r // 2, r % 2
    z, x = c // 4, c % 4

    pairs = [
        (video, vs.at[0:288]), (packed.at[0:96], sel.at[0:96]), (tokens, gx.at[:, 1:3]),
        (tokens, gbuf.at[:, 0]), (packed.at[96:1536], sel.at[96:1536]), (weight, wv),
    ]
    loads = [pltpu.make_async_copy(a, b, load.at[k]) for k, (a, b) in enumerate(pairs)]
    for one in loads:
        one.start()

    pick, rim, ends = sel.at[0:16, 0:384], sel.at[16:80, 0:288], sel.at[80:96, 0:128]
    cols, side, rows = sel.at[96:480], sel.at[480:512], sel.at[512:896, 0:384]
    beside, back = sel.at[896:1152, 0:128], sel.at[1152:1536, 0:384]

    hv[...] = jnp.zeros_like(hv)
    he[...] = jnp.zeros_like(he)
    hg[...] = jnp.zeros_like(hg)
    vs[288:384, :] = jnp.zeros((96, 384), BF16)
    for i4 in (0, 3):
        gx[:, i4] = jnp.zeros((2, 32, 512), BF16)
    lm[4] = jnp.zeros((16, 16, 256), BF16)

    barrier = pltpu.get_barrier_semaphore()
    up, down, lef, rig = r > 0, r < 7, c > 0, c < 15
    near = [
        (up, {"row": r - 1}), (down, {"row": r + 1}), (lef, {"col": c - 1}), (rig, {"col": c + 1}),
        (up & lef, {"row": r - 1, "col": c - 1}), (up & rig, {"row": r - 1, "col": c + 1}),
        (down & lef, {"row": r + 1, "col": c - 1}), (down & rig, {"row": r + 1, "col": c + 1}),
    ]
    yp, ym = {"row": (r + 2) % 8}, {"row": (r + 6) % 8}
    xp, xm = {"col": z * 4 + (x + 1) % 4}, {"col": z * 4 + (x + 3) % 4}
    other = {"row": y * 2 + 1 - core}
    zs = [{"col": ((z + d) % 4) * 4 + x} for d in (1, 2, 3)]
    partner = {"mp": 1 - m}

    def greet(to):
        pl.semaphore_signal(barrier, inc=1, device_id=to, device_id_type=MESH)

    for to in (yp, ym, xp, xm, other, *zs, partner):
        greet(to)
    for there, to in near:
        pl.when(there)(lambda to=to: greet(to))

    def one_if(p):
        return jnp.where(p, jnp.int32(1), jnp.int32(0))

    n_near = (1 + one_if(up) + one_if(down)) * (1 + one_if(lef) + one_if(rig)) - 1

    count = iter(range(N_SEMS))

    def remote(src, dst, to):
        k = next(count)
        return pltpu.make_async_remote_copy(
            src_ref=src, dst_ref=dst, send_sem=send.at[k], recv_sem=recv.at[k],
            device_id=to, device_id_type=MESH,
        )

    for k in range(3):
        loads[k].wait()
    vs[288:352, :] = dot(rim[...], vs[0:288, :]).astype(BF16)
    sb[...] = dot(pick[...], vs[...], ((1,), (1,))).astype(BF16)
    sg[...] = dot(ends[...], gx[:, 1:3].reshape(128, 512)).astype(BF16)
    loads[3].wait()

    pl.semaphore_wait(barrier, 9 + n_near)

    corner = (slice(None), slice(256, 384))
    halo = [
        (remote(vs.at[288:320], hv.at[0:32], {"row": r + 1}), down, up),
        (remote(vs.at[320:352], hv.at[32:64], {"row": r - 1}), up, down),
        (remote(sb, he.at[0], {"col": c + 1}), rig, lef),
        (remote(sb, he.at[1], {"col": c - 1}), lef, rig),
        (remote(sb.at[corner], he.at[2].at[corner], {"row": r + 1, "col": c + 1}), down & rig, up & lef),
        (remote(sb.at[corner], he.at[3].at[corner], {"row": r - 1, "col": c + 1}), up & rig, down & lef),
        (remote(sb.at[corner], he.at[4].at[corner], {"row": r + 1, "col": c - 1}), down & lef, up & rig),
        (remote(sb.at[corner], he.at[5].at[corner], {"row": r - 1, "col": c - 1}), up & lef, down & rig),
    ]
    for copy, sent, _ in halo:
        pl.when(sent)(lambda copy=copy: copy.start())
    g_p = remote(gbuf.at[:, 0], gbuf.at[:, 1], yp)
    g_m = remote(gbuf.at[:, 0], gbuf.at[:, 2], ym)
    g_p.start()
    g_m.start()
    g_in = remote(gx.at[:, 2 - core], gx.at[:, 3 * core], other)
    g_in.start()
    token_halo = [
        (remote(sg, hg.at[0], {"col": c + 1}), rig, lef),
        (remote(sg, hg.at[1], {"col": c - 1}), lef, rig),
        (remote(sg, hg.at[2], {"row": r + 1, "col": c + 1}), down & rig, up & lef),
        (remote(sg, hg.at[3], {"row": r - 1, "col": c + 1}), up & rig, down & lef),
        (remote(sg, hg.at[4], {"row": r + 1, "col": c - 1}), down & lef, up & rig),
        (remote(sg, hg.at[5], {"row": r - 1, "col": c - 1}), up & lef, down & rig),
    ]
    for copy, sent, _ in token_halo:
        pl.when(sent)(lambda copy=copy: copy.start())

    loads[4].wait()
    qf[...] = dot(vs[0:288, :], cols[...])

    for copy, _, got in halo:
        pl.when(got)(lambda copy=copy: copy.wait_recv())

    lane = lax.broadcasted_iota(jnp.int32, (16, 128), 1)
    for k, (a, b, d) in enumerate(((0, 2, 3), (1, 4, 5))):
        hs[16 * k : 16 * k + 16, 0:256] = he[a, :, 0:256]
        tile = jnp.where(
            lane < 32, he[a, :, 256:384].astype(F32),
            jnp.where(lane < 64, he[b, :, 256:384].astype(F32), he[d, :, 256:384].astype(F32)),
        )
        hs[16 * k : 16 * k + 16, 256:384] = tile.astype(BF16)
    from_side = dot(hs[...], side[...], ((0,), (0,)))
    qs[0:288, :] = (qf[...] + from_side[0:288]).astype(BF16)
    qs[288:384, :] = (dot(hv[...], cols[...]) + from_side[288:384]).astype(BF16)
    qw[...] = dot(rows[...], qs[...]).astype(BF16).reshape(12, 2, 16, 512)

    for d, to in ((2, 2), (0, 1), (1, 3)):
        for s in range(4):
            at = chosen((y + to) % 4, [f[s] for f in FRAMES_OF])
            sq[d, :, s] = qw[at]
    q_far_p = remote(sq.at[2, :, 0:2], rq.at[0], yp)
    q_far_m = remote(sq.at[2, :, 2:4], rq.at[1], ym)
    q_p = remote(sq.at[0], qr.at[1], yp)
    q_m = remote(sq.at[1], qr.at[2], ym)
    for one in (q_far_p, q_far_m, q_p, q_m):
        one.start()
    for s in range(4):
        at = chosen(y, [f[s] for f in FRAMES_OF])
        qr[0, :, s] = qw[at]

    g_p.wait_recv()
    gf_p = remote(gbuf.at[0, 1], gbuf.at[0, 3], yp)
    gf_p.start()
    g_m.wait_recv()
    gf_m = remote(gbuf.at[1, 2], gbuf.at[1, 3], ym)
    gf_m.start()
    g_out = remote(gbuf.at[:, 2 - core, core], gx.at[:, 3 - 3 * core], other)
    g_sent = ((core == 0) & (y < 3)) | ((core == 1) & (y > 0))
    g_got = ((core == 0) & (y > 0)) | ((core == 1) & (y < 3))
    pl.when(g_sent)(g_out.start)

    g_in.wait_recv()
    pl.when(g_got)(g_out.wait_recv)
    for copy, _, got in token_halo:
        pl.when(got)(lambda copy=copy: copy.wait_recv())
    loads[5].wait()

    ge[...] = dot(beside[...], hg[...].reshape(128, 512)).astype(BF16)

    def token_grads(first, last):
        @pl.loop(first, last)
        def _(k):
            at = pl.ds(pl.multiple_of(k * 256, 256), 256)
            for n, right in enumerate((gx[...].reshape(256, 512), ge[...])):
                block = dot(wv[at, :], right, ((1,), (1,)))
                pg[2 * n, at, :] = block[:, 0:128]
                pg[2 * n + 1, at, :] = block[:, 128:256]

    token_grads(0, 6)

    q_far_p.wait_recv()
    qf_p = remote(rq.at[0], qr.at[3, :, 0:2], yp)
    qf_p.start()
    q_far_m.wait_recv()
    qf_m = remote(rq.at[1], qr.at[3, :, 2:4], ym)
    qf_m.start()

    token_grads(6, 12)

    def frames(e, first):
        early = pg[first, pl.ds(e, 192, stride=16), :].reshape(12, 16, 128)
        late = pg[first + 1, pl.ds(e, 192, stride=16), :].reshape(12, 16, 128)
        out = []
        for ch in range(0, 12, 4):
            out += [
                early[ch + 1], early[ch + 2] + late[ch], early[ch + 3] + late[ch + 1], late[ch + 2],
            ]
        return jnp.stack(out)

    j = lax.broadcasted_iota(jnp.int32, (12, 16, 128), 2) % 32
    sub = lax.broadcasted_iota(jnp.int32, (12, 8, 128), 1)
    wrap = {0: (14, 0, 1), 1: (15, 0, 1), 10: (0, 31, 127), 11: (1, 31, 127)}
    for e in range(12):
        cell = frames(e + 2, 0)
        if e in wrap:
            far, at, by = wrap[e]
            cell = cell + jnp.where(j == at, frames(far, 2), pltpu.roll(frames(far, 0), by, 2))
        low, high = cell[:, 0:8], cell[:, 8:16]
        to_low = pltpu.roll(pltpu.roll(high, 32, 2), 4, 1)
        to_high = pltpu.roll(pltpu.roll(low, 96, 2), 4, 1)
        fs[e, :, 0:8] = low + jnp.where((sub == 2) | (sub == 3), to_low, 0.0)
        fs[e, :, 8:16] = high + jnp.where((sub == 4) | (sub == 5), to_high, 0.0)
    block = lax.broadcasted_iota(jnp.int32, (192, 128), 1) // 32
    for i in range(2):
        for k in range(3):
            row = None
            for q in range(4):
                part = fs[4 * k + q].reshape(192, 128)
                by = ((q - i - 1) * 32) % 128
                if by:
                    part = pltpu.roll(part, by, 1)
                row = part if row is None else jnp.where(block == q, part, row)
            upper = row.astype(BF16)
            ll[192 * i : 192 * i + 192, 128 * k : 128 * k + 128] = upper
            ll[384 + 192 * i : 576 + 192 * i, 128 * k : 128 * k + 128] = (row - upper.astype(F32)).astype(BF16)
    pixels = (dot(ll[0:384, :], back[...]) + dot(ll[384:768, :], back[...])).reshape(2, 12, 16, 384)
    for i in range(2):
        for cf in range(12):
            ch, f = cf // 4, cf % 4
            vg[f // 2, ch * 2 + f % 2, 12 * i : 12 * i + 12, :] = pixels[i, cf, 2:14, :]
    v_x = remote(vg.at[1 - m], mr, partner)
    v_x.start()

    for one in (q_p, q_m, qf_p, qf_m, gf_p, gf_m):
        one.wait_recv()

    block = lax.broadcasted_iota(jnp.int32, (64, 128), 1) // 32
    for k in range(4):
        for half in range(2):
            parts = [
                qr[2 * half + n // 2, n % 2, :, :, 128 * k : 128 * k + 128].astype(F32).reshape(64, 128)
                for n in range(4)
            ]
            for q in range(4):
                row = None
                for n in range(4):
                    by = ((n - q) * 32) % 128
                    part = pltpu.roll(parts[n], by, 1) if by else parts[n]
                    row = part if row is None else jnp.where(block == n, part, row)
                lm[0:4, 4 * k + q, :, 128 * half : 128 * half + 128] = row.astype(BF16).reshape(4, 16, 128)

    give = []
    for p in range(PIECES):
        for ca in range(3):
            total = None
            for t in range(2):
                at = chosen(y, [s[t][ca] for s in SLOTS_OF])
                right = gbuf[t, :, :, :, 128 * WIDE * p : 128 * WIDE * (p + 1)].reshape(256, 128 * WIDE)
                part = dot(lm[at].reshape(256, 256), right)
                total = part if total is None else total + part
            for e in range(16):
                for n in range(WIDE):
                    wg[WIDE * p + n, pl.ds(ca * 256 + e, 16, stride=16), :] = (
                        total[16 * e : 16 * e + 16, 128 * n : 128 * n + 128]
                    )
        tiles = slice(WIDE * p, WIDE * p + WIDE)
        give.append(remote(wg.at[tiles, pl.ds((1 - core) * 384, 384)], cr.at[tiles], other))
        give[p].start()

    x1, x2, x3 = (x + 1) % 4, (x + 2) % 4, (x + 3) % 4
    far_p, far_m, near_p, near_m, last_p, last_m = [], [], [], [], [], []
    for p in range(PIECES):
        tiles = slice(WIDE * p, WIDE * p + WIDE)
        give[p].wait_recv()
        for n in range(WIDE * p, WIDE * p + WIDE):
            for k in range(16):
                a1[n, k // 4, k % 4] = wg[n, pl.ds(core * 384 + 24 * k, 24), :] + cr[n, 24 * k : 24 * k + 24, :]
        far_p.append(remote(a1.at[tiles, 0:2, x2], xa.at[tiles], xp))
        far_m.append(remote(a1.at[tiles, 2:4, x2], xb.at[tiles], xm))
        far_p[p].start()
        far_m[p].start()
    for p in range(PIECES):
        tiles = slice(WIDE * p, WIDE * p + WIDE)
        near_p.append(remote(a1.at[tiles, 2:4, x1], xr1.at[tiles, 2:4], xp))
        near_m.append(remote(a1.at[tiles, 0:2, x3], xr2.at[tiles, 0:2], xm))
        near_p[p].start()
        near_m[p].start()

    for p in range(PIECES):
        tiles = slice(WIDE * p, WIDE * p + WIDE)
        far_p[p].wait_recv()
        xs1[tiles] = a1[tiles, 0:2, x1] + xa[tiles]
        last_p.append(remote(xs1.at[tiles], xr1.at[tiles, 0:2], xp))
        last_p[p].start()
        far_m[p].wait_recv()
        xs2[tiles] = a1[tiles, 2:4, x3] + xb[tiles]
        last_m.append(remote(xs2.at[tiles], xr2.at[tiles, 2:4], xm))
        last_m[p].start()

    z_out = []
    for p in range(PIECES):
        tiles = slice(WIDE * p, WIDE * p + WIDE)
        for one in (near_p, near_m, last_p, last_m):
            one[p].wait_recv()
        a2[tiles] = a1[tiles, :, x] + xr1[tiles] + xr2[tiles]
        z_out.append([remote(a2.at[tiles, (z + d + 1) % 4], zr.at[d, tiles], zs[d]) for d in (2, 1, 0)])
        for one in z_out[p]:
            one.start()

    v_x.wait_recv()
    vg[m] = vg[m] + mr[...]
    v_out = pltpu.make_async_copy(vg.at[m], vout, load.at[6])
    v_out.start()

    for p in range(PIECES):
        for one in z_out[p]:
            one.wait_recv()
        for n in range(WIDE * p, WIDE * p + WIDE):
            wout[:, 128 * n : 128 * n + 128] = (a2[n, z] + zr[0, n] + (zr[1, n] + zr[2, n])) * (1.0 / 128.0)

    v_out.wait()
    for copy, sent, _ in halo + token_halo:
        pl.when(sent)(lambda copy=copy: copy.wait_send())
    pl.when(g_sent)(g_out.wait_send)
    for one in (
        g_p, g_m, g_in, gf_p, gf_m, q_far_p, q_far_m, q_p, q_m, qf_p, qf_m, v_x,
        *give, *far_p, *far_m, *near_p, *near_m, *last_p, *last_m, *sum(z_out, []),
    ):
        one.wait_send()


def shards(video, grad_tokens, weight):
    packed = jnp.asarray(selections(), BF16)
    anywhere = pl.BlockSpec(memory_space=pltpu.HBM)
    in_vmem = pl.BlockSpec(memory_space=pltpu.VMEM)

    def v(*shape, kind=F32):
        return pltpu.VMEM(shape, kind)

    def b(*shape):
        return pltpu.VMEM(shape, BF16)

    video_grad, weight_grad = pl.pallas_call(
        kernel,
        out_shape=(
            jax.ShapeDtypeStruct((6, 24, 384), F32),
            jax.ShapeDtypeStruct((24, 512), F32),
        ),
        in_specs=[anywhere] * 4,
        out_specs=(pl.BlockSpec(memory_space=pl.ANY), in_vmem),
        scratch_shapes=[
            b(SELECTION_ROWS, 512),
            b(3072, 512), b(384, 384), b(96, 384), b(6, 16, 384), b(8, 16, 512), b(16, 384), b(16, 512), b(32, 384), v(288, 512),
            b(2, 4, 32, 512), b(256, 512), b(2, 4, 2, 32, 512), b(384, 512), b(12, 2, 16, 512),
            b(3, 2, 4, 16, 512), b(4, 2, 4, 16, 512), b(2, 2, 2, 16, 512), b(5, 16, 16, 256),
            v(4, 3072, 128), v(12, 12, 16, 128), b(768, 384), v(2, 6, 24, 384), v(6, 24, 384),
            v(4, 768, 128), v(4, 384, 128), v(4, 4, 4, 24, 128), v(4, 2, 24, 128), v(4, 2, 24, 128),
            v(4, 4, 24, 128), v(4, 4, 24, 128), v(4, 2, 24, 128), v(4, 2, 24, 128), v(4, 4, 24, 128),
            v(3, 4, 24, 128),
            pltpu.SemaphoreType.DMA((7,)),
            pltpu.SemaphoreType.DMA((N_SEMS,)),
            pltpu.SemaphoreType.DMA((N_SEMS,)),
        ],
        compiler_params=pltpu.CompilerParams(
            collective_id=0, has_side_effects=True, vmem_limit_bytes=VMEM_BYTES
        ),
        name="tubelet_backward",
    )(video.reshape(288, 384), grad_tokens, weight, packed)
    return video_grad.reshape(3, 2, 24, 384), weight_grad


def solution(mesh):
    return jax.shard_map(
        shards,
        mesh=mesh,
        in_specs=(P(None, None, "row", "col"), P(None, "row", "col", "mp"), P(None, "mp")),
        out_specs=(P(None, "mp", "row", "col"), P(("row", "col"), "mp")),
        check_vma=False,
    )
```

```python
import jax
import jax.numpy as jnp
import numpy as np
from jax import lax
from jax.experimental import pallas as pl
from jax.experimental.pallas import tpu as pltpu
from jax.sharding import PartitionSpec as P

MESH = pl.DeviceIdType.MESH
F32 = jnp.float32
BF16 = jnp.bfloat16
N_SEMS = 64
VMEM_BYTES = 56500000
PIECES = 2
WIDE = 4 // PIECES
CODED = WIDE * 48
SELECTION_AT = (0, 16, 80, 96, 480, 512, 896, 1152)
SELECTION_ROWS = 1536


def selections():
    cols = np.zeros((384, 512), np.float32)
    for e in range(16):
        for j in range(32):
            x = 12 * j + e - 2
            if 0 <= x < 384:
                cols[x, e * 32 + j] = 1
    side = np.zeros((32, 512), np.float32)
    side[2, 0] = side[3, 32] = 1
    side[16, 14 * 32 + 31] = side[17, 15 * 32 + 31] = 1
    rows = np.zeros((384, 384), np.float32)
    for cf in range(12):
        for i in range(2):
            for b in range(16):
                y = 12 * i + b - 2
                src = cf * 24 + y if 0 <= y < 24 else 288 + cf * 2 + y + 2 if y < 0 else 320 + cf * 2 + y - 24
                rows[cf * 32 + i * 16 + b, src] = 1
    pick = np.zeros((16, 384), np.float32)
    for k, x in enumerate((0, 1, 382, 383)):
        pick[k, x] = 1
    rim = np.zeros((64, 288), np.float32)
    for cf in range(12):
        for k in range(2):
            rim[cf * 2 + k, cf * 24 + 22 + k] = 1
            rim[32 + cf * 2 + k, cf * 24 + k] = 1
    ends = np.zeros((16, 128), np.float32)
    for ti in range(4):
        ends[ti, ti * 32] = 1
        ends[4 + ti, ti * 32 + 31] = 1
    beside = np.zeros((256, 128), np.float32)
    for t in range(2):
        for i4 in range(4):
            i = (1, 0, 1, 0)[i4]
            left = (2, 0, 0, 3)[i4]
            right = (4, 1, 1, 5)[i4]
            beside[t * 128 + i4 * 32, left * 16 + 4 + t * 2 + i] = 1
            beside[t * 128 + i4 * 32 + 31, right * 16 + t * 2 + i] = 1
    back = np.zeros((384, 384), np.float32)
    for e in range(12):
        for j in range(32):
            back[e * 32 + j, 12 * j + e] = 1
    packed = np.zeros((SELECTION_ROWS, 512), np.float32)
    for at, one in zip(SELECTION_AT, (pick, rim, ends, cols, side, rows, beside, back)):
        packed[at : at + one.shape[0], : one.shape[1]] = one
    return packed


def chosen(at, values):
    out = jnp.int32(values[3])
    for k in range(3):
        out = jnp.where(at == k, jnp.int32(values[k]), out)
    return out


FRAMES_OF = ((0, 1, 2, 3), (2, 4, 5, 6), (5, 6, 7, 9), (8, 9, 10, 11))
SLOTS_OF = (
    (((4, 0, 1), (1, 2, 3))),
    (((0, 4, 1), (4, 2, 3))),
    (((0, 1, 4), (2, 4, 3))),
    (((0, 1, 2), (2, 3, 4))),
)


def dot(a, b, dims=((1,), (0,))):
    return lax.dot_general(a, b, (dims, ((), ())), preferred_element_type=F32)


TOP = 2.0**15


def largest(x):
    top = jnp.abs(x).reshape(-1, x.shape[-1])
    top = jnp.max(jnp.max(top, axis=0, keepdims=True), axis=1, keepdims=True)
    return (jnp.maximum(top, 1e-25) * 1.01).astype(BF16).astype(F32)


def packed_rows(x):
    return x.reshape(-1, x.shape[-1])


def coded(x, top):
    t = packed_rows(x) * (TOP / top)
    t2 = t * t
    t4 = t2 * t2
    return (t4 * t2 * jnp.abs(t) * t).astype(BF16)


def decoded(code, top, shape):
    v = code.astype(F32)
    t = jnp.sqrt(jnp.sqrt(jnp.sqrt(jnp.abs(v)))) * (top * (1.0 / TOP))
    return jnp.where(v < 0, -t, t).reshape(shape)


def spread(top, lanes):
    return jnp.broadcast_to(top, (16, lanes)).astype(BF16)


def kernel(
    video, tokens, weight, packed,
    vout, wout,
    sel,
    wv, vs, hv, he, hg, sb, sg, hs, qf, gx, ge, gbuf, qs, qw, sq, qr, rq, lm, pg, fs, ll, vg, ms, mr,
    wg, cr, a1, fo, fi, no, ni, lo, li, a2, zr,
    load, send, recv,
):
    r = lax.axis_index("row")
    c = lax.axis_index("col")
    m = lax.axis_index("mp")
    y, core = r // 2, r % 2
    z, x = c // 4, c % 4

    pairs = [
        (video, vs.at[0:288]), (packed.at[0:96], sel.at[0:96]), (tokens, gx.at[:, 1:3]),
        (tokens, gbuf.at[:, 0]), (packed.at[96:1536], sel.at[96:1536]), (weight, wv),
    ]
    loads = [pltpu.make_async_copy(a, b, load.at[k]) for k, (a, b) in enumerate(pairs)]
    for one in loads:
        one.start()

    pick, rim, ends = sel.at[0:16, 0:384], sel.at[16:80, 0:288], sel.at[80:96, 0:128]
    cols, side, rows = sel.at[96:480], sel.at[480:512], sel.at[512:896, 0:384]
    beside, back = sel.at[896:1152, 0:128], sel.at[1152:1536, 0:384]

    hv[...] = jnp.zeros_like(hv)
    he[...] = jnp.zeros_like(he)
    hg[...] = jnp.zeros_like(hg)
    vs[288:384, :] = jnp.zeros((96, 384), BF16)
    for i4 in (0, 3):
        gx[:, i4] = jnp.zeros((2, 32, 512), BF16)
    lm[4] = jnp.zeros((16, 16, 256), BF16)

    barrier = pltpu.get_barrier_semaphore()
    up, down, lef, rig = r > 0, r < 7, c > 0, c < 15
    near = [
        (up, {"row": r - 1}), (down, {"row": r + 1}), (lef, {"col": c - 1}), (rig, {"col": c + 1}),
        (up & lef, {"row": r - 1, "col": c - 1}), (up & rig, {"row": r - 1, "col": c + 1}),
        (down & lef, {"row": r + 1, "col": c - 1}), (down & rig, {"row": r + 1, "col": c + 1}),
    ]
    yp, ym = {"row": (r + 2) % 8}, {"row": (r + 6) % 8}
    xp, xm = {"col": z * 4 + (x + 1) % 4}, {"col": z * 4 + (x + 3) % 4}
    other = {"row": y * 2 + 1 - core}
    zs = [{"col": ((z + d) % 4) * 4 + x} for d in (1, 2, 3)]
    partner = {"mp": 1 - m}

    def greet(to):
        pl.semaphore_signal(barrier, inc=1, device_id=to, device_id_type=MESH)

    for to in (yp, ym, xp, xm, other, *zs, partner):
        greet(to)
    for there, to in near:
        pl.when(there)(lambda to=to: greet(to))

    def one_if(p):
        return jnp.where(p, jnp.int32(1), jnp.int32(0))

    n_near = (1 + one_if(up) + one_if(down)) * (1 + one_if(lef) + one_if(rig)) - 1

    count = iter(range(N_SEMS))

    def remote(src, dst, to):
        k = next(count)
        return pltpu.make_async_remote_copy(
            src_ref=src, dst_ref=dst, send_sem=send.at[k], recv_sem=recv.at[k],
            device_id=to, device_id_type=MESH,
        )

    for k in range(3):
        loads[k].wait()
    vs[288:352, :] = dot(rim[...], vs[0:288, :]).astype(BF16)
    sb[...] = dot(pick[...], vs[...], ((1,), (1,))).astype(BF16)
    sg[...] = dot(ends[...], gx[:, 1:3].reshape(128, 512)).astype(BF16)
    loads[3].wait()

    pl.semaphore_wait(barrier, 9 + n_near)

    corner = (slice(None), slice(256, 384))
    halo = [
        (remote(vs.at[288:320], hv.at[0:32], {"row": r + 1}), down, up),
        (remote(vs.at[320:352], hv.at[32:64], {"row": r - 1}), up, down),
        (remote(sb, he.at[0], {"col": c + 1}), rig, lef),
        (remote(sb, he.at[1], {"col": c - 1}), lef, rig),
        (remote(sb.at[corner], he.at[2].at[corner], {"row": r + 1, "col": c + 1}), down & rig, up & lef),
        (remote(sb.at[corner], he.at[3].at[corner], {"row": r - 1, "col": c + 1}), up & rig, down & lef),
        (remote(sb.at[corner], he.at[4].at[corner], {"row": r + 1, "col": c - 1}), down & lef, up & rig),
        (remote(sb.at[corner], he.at[5].at[corner], {"row": r - 1, "col": c - 1}), up & lef, down & rig),
    ]
    for copy, sent, _ in halo:
        pl.when(sent)(lambda copy=copy: copy.start())
    g_p = remote(gbuf.at[:, 0], gbuf.at[:, 1], yp)
    g_m = remote(gbuf.at[:, 0], gbuf.at[:, 2], ym)
    g_p.start()
    g_m.start()
    g_in = remote(gx.at[:, 2 - core], gx.at[:, 3 * core], other)
    g_in.start()
    token_halo = [
        (remote(sg, hg.at[0], {"col": c + 1}), rig, lef),
        (remote(sg, hg.at[1], {"col": c - 1}), lef, rig),
        (remote(sg, hg.at[2], {"row": r + 1, "col": c + 1}), down & rig, up & lef),
        (remote(sg, hg.at[3], {"row": r - 1, "col": c + 1}), up & rig, down & lef),
        (remote(sg, hg.at[4], {"row": r + 1, "col": c - 1}), down & lef, up & rig),
        (remote(sg, hg.at[5], {"row": r - 1, "col": c - 1}), up & lef, down & rig),
    ]
    for copy, sent, _ in token_halo:
        pl.when(sent)(lambda copy=copy: copy.start())

    loads[4].wait()
    qf[...] = dot(vs[0:288, :], cols[...])

    for copy, _, got in halo:
        pl.when(got)(lambda copy=copy: copy.wait_recv())

    lane = lax.broadcasted_iota(jnp.int32, (16, 128), 1)
    for k, (a, b, d) in enumerate(((0, 2, 3), (1, 4, 5))):
        hs[16 * k : 16 * k + 16, 0:256] = he[a, :, 0:256]
        tile = jnp.where(
            lane < 32, he[a, :, 256:384].astype(F32),
            jnp.where(lane < 64, he[b, :, 256:384].astype(F32), he[d, :, 256:384].astype(F32)),
        )
        hs[16 * k : 16 * k + 16, 256:384] = tile.astype(BF16)
    from_side = dot(hs[...], side[...], ((0,), (0,)))
    qs[0:288, :] = (qf[...] + from_side[0:288]).astype(BF16)
    qs[288:384, :] = (dot(hv[...], cols[...]) + from_side[288:384]).astype(BF16)
    qw[...] = dot(rows[...], qs[...]).astype(BF16).reshape(12, 2, 16, 512)

    for d, to in ((2, 2), (0, 1), (1, 3)):
        for s in range(4):
            at = chosen((y + to) % 4, [f[s] for f in FRAMES_OF])
            sq[d, :, s] = qw[at]
    q_far_p = remote(sq.at[2, :, 0:2], rq.at[0], yp)
    q_far_m = remote(sq.at[2, :, 2:4], rq.at[1], ym)
    q_p = remote(sq.at[0], qr.at[1], yp)
    q_m = remote(sq.at[1], qr.at[2], ym)
    for one in (q_far_p, q_far_m, q_p, q_m):
        one.start()
    for s in range(4):
        at = chosen(y, [f[s] for f in FRAMES_OF])
        qr[0, :, s] = qw[at]

    g_p.wait_recv()
    gf_p = remote(gbuf.at[0, 1], gbuf.at[0, 3], yp)
    gf_p.start()
    g_m.wait_recv()
    gf_m = remote(gbuf.at[1, 2], gbuf.at[1, 3], ym)
    gf_m.start()
    g_out = remote(gbuf.at[:, 2 - core, core], gx.at[:, 3 - 3 * core], other)
    g_sent = ((core == 0) & (y < 3)) | ((core == 1) & (y > 0))
    g_got = ((core == 0) & (y > 0)) | ((core == 1) & (y < 3))
    pl.when(g_sent)(g_out.start)

    g_in.wait_recv()
    pl.when(g_got)(g_out.wait_recv)
    for copy, _, got in token_halo:
        pl.when(got)(lambda copy=copy: copy.wait_recv())
    loads[5].wait()

    ge[...] = dot(beside[...], hg[...].reshape(128, 512)).astype(BF16)

    def token_grads(first, last):
        @pl.loop(first, last)
        def _(k):
            at = pl.ds(pl.multiple_of(k * 256, 256), 256)
            for n, right in enumerate((gx[...].reshape(256, 512), ge[...])):
                block = dot(wv[at, :], right, ((1,), (1,)))
                pg[2 * n, at, :] = block[:, 0:128]
                pg[2 * n + 1, at, :] = block[:, 128:256]

    token_grads(0, 6)

    q_far_p.wait_recv()
    qf_p = remote(rq.at[0], qr.at[3, :, 0:2], yp)
    qf_p.start()
    q_far_m.wait_recv()
    qf_m = remote(rq.at[1], qr.at[3, :, 2:4], ym)
    qf_m.start()

    token_grads(6, 12)

    def frames(e, first):
        early = pg[first, pl.ds(e, 192, stride=16), :].reshape(12, 16, 128)
        late = pg[first + 1, pl.ds(e, 192, stride=16), :].reshape(12, 16, 128)
        out = []
        for ch in range(0, 12, 4):
            out += [
                early[ch + 1], early[ch + 2] + late[ch], early[ch + 3] + late[ch + 1], late[ch + 2],
            ]
        return jnp.stack(out)

    j = lax.broadcasted_iota(jnp.int32, (12, 16, 128), 2) % 32
    sub = lax.broadcasted_iota(jnp.int32, (12, 8, 128), 1)
    wrap = {0: (14, 0, 1), 1: (15, 0, 1), 10: (0, 31, 127), 11: (1, 31, 127)}
    for e in range(12):
        cell = frames(e + 2, 0)
        if e in wrap:
            far, at, by = wrap[e]
            cell = cell + jnp.where(j == at, frames(far, 2), pltpu.roll(frames(far, 0), by, 2))
        low, high = cell[:, 0:8], cell[:, 8:16]
        to_low = pltpu.roll(pltpu.roll(high, 32, 2), 4, 1)
        to_high = pltpu.roll(pltpu.roll(low, 96, 2), 4, 1)
        fs[e, :, 0:8] = low + jnp.where((sub == 2) | (sub == 3), to_low, 0.0)
        fs[e, :, 8:16] = high + jnp.where((sub == 4) | (sub == 5), to_high, 0.0)
    block = lax.broadcasted_iota(jnp.int32, (192, 128), 1) // 32
    for i in range(2):
        for k in range(3):
            row = None
            for q in range(4):
                part = fs[4 * k + q].reshape(192, 128)
                by = ((q - i - 1) * 32) % 128
                if by:
                    part = pltpu.roll(part, by, 1)
                row = part if row is None else jnp.where(block == q, part, row)
            upper = row.astype(BF16)
            ll[192 * i : 192 * i + 192, 128 * k : 128 * k + 128] = upper
            ll[384 + 192 * i : 576 + 192 * i, 128 * k : 128 * k + 128] = (row - upper.astype(F32)).astype(BF16)
    pixels = (dot(ll[0:384, :], back[...]) + dot(ll[384:768, :], back[...])).reshape(2, 12, 16, 384)
    for i in range(2):
        for cf in range(12):
            ch, f = cf // 4, cf % 4
            vg[f // 2, ch * 2 + f % 2, 12 * i : 12 * i + 12, :] = pixels[i, cf, 2:14, :]
    top = largest(vg[1 - m])
    ms[0:16] = spread(top, 384)
    ms[16:160] = coded(vg[1 - m], top)
    v_x = remote(ms, mr, partner)
    v_x.start()

    for one in (q_p, q_m, qf_p, qf_m, gf_p, gf_m):
        one.wait_recv()

    block = lax.broadcasted_iota(jnp.int32, (64, 128), 1) // 32
    for k in range(4):
        for half in range(2):
            parts = [
                qr[2 * half + n // 2, n % 2, :, :, 128 * k : 128 * k + 128].astype(F32).reshape(64, 128)
                for n in range(4)
            ]
            for q in range(4):
                row = None
                for n in range(4):
                    by = ((n - q) * 32) % 128
                    part = pltpu.roll(parts[n], by, 1) if by else parts[n]
                    row = part if row is None else jnp.where(block == n, part, row)
                lm[0:4, 4 * k + q, :, 128 * half : 128 * half + 128] = row.astype(BF16).reshape(4, 16, 128)

    give = []
    for p in range(PIECES):
        for ca in range(3):
            total = None
            for t in range(2):
                at = chosen(y, [s[t][ca] for s in SLOTS_OF])
                right = gbuf[t, :, :, :, 128 * WIDE * p : 128 * WIDE * (p + 1)].reshape(256, 128 * WIDE)
                part = dot(lm[at].reshape(256, 256), right)
                total = part if total is None else total + part
            for e in range(16):
                for n in range(WIDE):
                    wg[WIDE * p + n, pl.ds(ca * 256 + e, 16, stride=16), :] = (
                        total[16 * e : 16 * e + 16, 128 * n : 128 * n + 128]
                    )
        tiles = slice(WIDE * p, WIDE * p + WIDE)
        give.append(remote(wg.at[tiles, pl.ds((1 - core) * 384, 384)], cr.at[tiles], other))
        give[p].start()

    x1, x2, x3 = (x + 1) % 4, (x + 2) % 4, (x + 3) % 4
    far, near, last, tops = [], [], [], []
    halves = (slice(0, 2), slice(2, 4))
    ring = (xp, xm)
    beyond = (x1, x3)
    block = (WIDE, 2, 24, 128)
    for p in range(PIECES):
        tiles = slice(WIDE * p, WIDE * p + WIDE)
        give[p].wait_recv()
        for n in range(WIDE * p, WIDE * p + WIDE):
            for k in range(16):
                a1[n, k // 4, k % 4] = wg[n, pl.ds(core * 384 + 24 * k, 24), :] + cr[n, 24 * k : 24 * k + 24, :]
        tops.append(largest(a1[tiles]))
        for d in range(2):
            fo[d, p, 0:16] = spread(tops[p], 128)
            fo[d, p, 16:] = coded(a1[tiles, halves[d], x2], tops[p])
            far.append(remote(fo.at[d, p], fi.at[d, p], ring[d]))
            far[-1].start()
    for p in range(PIECES):
        tiles = slice(WIDE * p, WIDE * p + WIDE)
        for d in range(2):
            no[d, p] = coded(a1[tiles, halves[1 - d], beyond[d]], tops[p])
            near.append(remote(no.at[d, p], ni.at[d, p], ring[d]))
            near[-1].start()

    for p in range(PIECES):
        tiles = slice(WIDE * p, WIDE * p + WIDE)
        for d in range(2):
            far[2 * p + d].wait_recv()
            top = fi[d, p, 0:16].astype(F32)[0:1]
            total = a1[tiles, halves[d], beyond[d]] + decoded(fi[d, p, 16:], top, block)
            top = ((top[:, 0:1] + tops[p]) * 1.01).astype(BF16).astype(F32)
            lo[d, p, 0:16] = spread(top, 128)
            lo[d, p, 16:] = coded(total, top)
            last.append(remote(lo.at[d, p], li.at[d, p], ring[d]))
            last[-1].start()

    z_out = []
    for p in range(PIECES):
        tiles = slice(WIDE * p, WIDE * p + WIDE)
        for d in range(2):
            near[2 * p + d].wait_recv()
            top = fi[d, p, 0:16].astype(F32)[0:1]
            a1[tiles, halves[1 - d], x] = a1[tiles, halves[1 - d], x] + decoded(ni[d, p], top, block)
        for d in range(2):
            last[2 * p + d].wait_recv()
            top = li[d, p, 0:16].astype(F32)[0:1]
            a2[tiles, halves[d]] = a1[tiles, halves[d], x] + decoded(li[d, p, 16:], top, block)
        z_out.append([remote(a2.at[tiles, (z + d + 1) % 4], zr.at[d, tiles], zs[d]) for d in (2, 1, 0)])
        for one in z_out[p]:
            one.start()

    v_x.wait_recv()
    vg[m] = vg[m] + decoded(mr[16:160], mr[0:16].astype(F32)[0:1], (6, 24, 384))
    v_out = pltpu.make_async_copy(vg.at[m], vout, load.at[6])
    v_out.start()

    for p in range(PIECES):
        for one in z_out[p]:
            one.wait_recv()
        for n in range(WIDE * p, WIDE * p + WIDE):
            wout[:, 128 * n : 128 * n + 128] = (a2[n, z] + zr[0, n] + (zr[1, n] + zr[2, n])) * (1.0 / 128.0)

    v_out.wait()
    for copy, sent, _ in halo + token_halo:
        pl.when(sent)(lambda copy=copy: copy.wait_send())
    pl.when(g_sent)(g_out.wait_send)
    for one in (
        g_p, g_m, g_in, gf_p, gf_m, q_far_p, q_far_m, q_p, q_m, qf_p, qf_m, v_x,
        *give, *far, *near, *last, *sum(z_out, []),
    ):
        one.wait_send()


def shards(video, grad_tokens, weight):
    packed = jnp.asarray(selections(), BF16)
    anywhere = pl.BlockSpec(memory_space=pltpu.HBM)
    in_vmem = pl.BlockSpec(memory_space=pltpu.VMEM)

    def v(*shape, kind=F32):
        return pltpu.VMEM(shape, kind)

    def b(*shape):
        return pltpu.VMEM(shape, BF16)

    video_grad, weight_grad = pl.pallas_call(
        kernel,
        out_shape=(
            jax.ShapeDtypeStruct((6, 24, 384), F32),
            jax.ShapeDtypeStruct((24, 512), F32),
        ),
        in_specs=[anywhere] * 4,
        out_specs=(pl.BlockSpec(memory_space=pl.ANY), in_vmem),
        scratch_shapes=[
            b(SELECTION_ROWS, 512),
            b(3072, 512), b(384, 384), b(96, 384), b(6, 16, 384), b(8, 16, 512), b(16, 384), b(16, 512), b(32, 384), v(288, 512),
            b(2, 4, 32, 512), b(256, 512), b(2, 4, 2, 32, 512), b(384, 512), b(12, 2, 16, 512),
            b(3, 2, 4, 16, 512), b(4, 2, 4, 16, 512), b(2, 2, 2, 16, 512), b(5, 16, 16, 256),
            v(4, 3072, 128), v(12, 12, 16, 128), b(768, 384), v(2, 6, 24, 384), b(160, 384), b(160, 384),
            v(4, 768, 128), v(4, 384, 128), v(4, 4, 4, 24, 128),
            *[b(2, PIECES, rows, 128) for rows in (CODED + 16, CODED + 16, CODED, CODED, CODED + 16, CODED + 16)],
            v(4, 4, 24, 128),
            v(3, 4, 24, 128),
            pltpu.SemaphoreType.DMA((7,)),
            pltpu.SemaphoreType.DMA((N_SEMS,)),
            pltpu.SemaphoreType.DMA((N_SEMS,)),
        ],
        compiler_params=pltpu.CompilerParams(
            collective_id=0, has_side_effects=True, vmem_limit_bytes=VMEM_BYTES
        ),
        name="tubelet_backward",
    )(video.reshape(288, 384), grad_tokens, weight, packed)
    return video_grad.reshape(3, 2, 24, 384), weight_grad


def solution(mesh):
    return jax.shard_map(
        shards,
        mesh=mesh,
        in_specs=(P(None, None, "row", "col"), P(None, "row", "col", "mp"), P(None, "mp")),
        out_specs=(P(None, "mp", "row", "col"), P(("row", "col"), "mp")),
        check_vma=False,
    )
```

```python
import jax
import jax.numpy as jnp
import numpy as np
from jax import lax
from jax.experimental import pallas as pl
from jax.experimental.pallas import tpu as pltpu
from jax.sharding import PartitionSpec as P

MESH = pl.DeviceIdType.MESH
F32 = jnp.float32
BF16 = jnp.bfloat16
N_SEMS = 80
FRAMES_OF = ((0, 1, 2, 3), (2, 4, 5, 6), (5, 6, 7, 9), (8, 9, 10, 11))
VMEM_BYTES = 56500000
PIECES = 2
WIDE = 4 // PIECES
CODED = WIDE * 48
SELECTION_AT = (0, 16, 80, 96, 480, 496, 880, 1008, 1136, 1200, 1456)
SELECTION_ROWS = 1840


def selections():
    cols = np.zeros((384, 512), np.float32)
    for e in range(16):
        for j in range(32):
            x = 12 * j + e - 2
            if 0 <= x < 384:
                cols[x, e * 32 + j] = 1
    side = np.zeros((16, 512), np.float32)
    side[2, 0] = side[3, 32] = 1
    side[0, 14 * 32 + 31] = side[1, 15 * 32 + 31] = 1
    rim_of = np.zeros((64, 64), np.float32)
    places = np.zeros((384, 512), np.float32)
    for at in range(4):
        for s, cf in enumerate(FRAMES_OF[at]):
            for k in range(24):
                places[cf * 24 + k, at * 128 + s * 32 + k] = 1
            for k in range(4):
                far = (k // 2) * 32 + cf * 2 + k % 2
                rim_of[at * 16 + s * 4 + k, far] = 1
                places[288 + far, at * 128 + s * 32 + 24 + k] = 1
    rows = np.zeros((128, 128), np.float32)
    rows_far = np.zeros((128, 16), np.float32)
    for i in range(2):
        for s in range(4):
            for b in range(16):
                y = 12 * i + b - 2
                k = y + 2 if y < 0 else y - 22
                rows[i * 64 + s * 16 + b, s * 32 + (y if 0 <= y < 24 else 24 + k)] = 1
                if not 0 <= y < 24:
                    rows_far[i * 64 + s * 16 + b, s * 4 + k] = 1
    pick = np.zeros((16, 384), np.float32)
    for k, x in enumerate((0, 1, 382, 383)):
        pick[k, x] = 1
    rim = np.zeros((64, 288), np.float32)
    for cf in range(12):
        for k in range(2):
            rim[cf * 2 + k, cf * 24 + 22 + k] = 1
            rim[32 + cf * 2 + k, cf * 24 + k] = 1
    ends = np.zeros((16, 128), np.float32)
    for ti in range(4):
        ends[ti, ti * 32] = 1
        ends[4 + ti, ti * 32 + 31] = 1
    beside = np.zeros((256, 128), np.float32)
    for t in range(2):
        for i4 in range(4):
            i = (1, 0, 1, 0)[i4]
            left = (2, 0, 0, 3)[i4]
            right = (4, 1, 1, 5)[i4]
            beside[t * 128 + i4 * 32, left * 16 + 4 + t * 2 + i] = 1
            beside[t * 128 + i4 * 32 + 31, right * 16 + t * 2 + i] = 1
    back = np.zeros((384, 384), np.float32)
    for e in range(12):
        for j in range(32):
            back[e * 32 + j, 12 * j + e] = 1
    packed = np.zeros((SELECTION_ROWS, 512), np.float32)
    for at, one in zip(SELECTION_AT, (pick, rim, ends, cols, side, places, rows, rows_far, rim_of, beside, back)):
        packed[at : at + one.shape[0], : one.shape[1]] = one
    return packed


def chosen(at, values):
    out = jnp.int32(values[3])
    for k in range(3):
        out = jnp.where(at == k, jnp.int32(values[k]), out)
    return out


SLOTS_OF = (
    (((4, 0, 1), (1, 2, 3))),
    (((0, 4, 1), (4, 2, 3))),
    (((0, 1, 4), (2, 4, 3))),
    (((0, 1, 2), (2, 3, 4))),
)


def dot(a, b, dims=((1,), (0,))):
    return lax.dot_general(a, b, (dims, ((), ())), preferred_element_type=F32)


TOP = 2.0**15


def largest(x):
    top = jnp.abs(x).reshape(-1, x.shape[-1])
    top = jnp.max(jnp.max(top, axis=0, keepdims=True), axis=1, keepdims=True)
    return (jnp.maximum(top, 1e-25) * 1.01).astype(BF16).astype(F32)


def packed_rows(x):
    return x.reshape(-1, x.shape[-1])


def coded(x, top):
    t = packed_rows(x) * (TOP / top)
    t2 = t * t
    t4 = t2 * t2
    return (t4 * t2 * jnp.abs(t) * t).astype(BF16)


def decoded(code, top, shape):
    v = code.astype(F32)
    t = jnp.sqrt(jnp.sqrt(jnp.sqrt(jnp.abs(v)))) * (top * (1.0 / TOP))
    return jnp.where(v < 0, -t, t).reshape(shape)


def spread(top, lanes):
    return jnp.broadcast_to(top, (16, lanes)).astype(BF16)


def kernel(
    video, frames_h, tokens, weight, packed,
    vout, wout,
    sel,
    wv, vs, v3, rv, rq, hv, he, hg, sb, sg, hs, ex, er, gx, ge, gbuf, qr, lm, pg, fs, ll, vg, ms, mr,
    wg, cr, a1, fo, fi, no, ni, lo, li, a2, zr,
    load, send, recv,
):
    r = lax.axis_index("row")
    c = lax.axis_index("col")
    m = lax.axis_index("mp")
    y, core = r // 2, r % 2
    z, x = c // 4, c % 4

    pairs = [
        (video, vs.at[0:288]), (packed.at[0:96], sel.at[0:96]), (tokens, gx.at[:, 1:3]),
        (tokens, gbuf.at[:, 0]), (frames_h, v3), (packed.at[96:SELECTION_ROWS], sel.at[96:SELECTION_ROWS]),
        (weight, wv),
    ]
    for s in range(4):
        pairs.append((frames_h.at[chosen(y, [f[s] for f in FRAMES_OF])], rv.at[0, s, 0:24]))
    loads = [pltpu.make_async_copy(a, b, load.at[k]) for k, (a, b) in enumerate(pairs)]
    for one in loads:
        one.start()

    pick, rim, ends = sel.at[0:16, 0:384], sel.at[16:80, 0:288], sel.at[80:96, 0:128]
    cols, side, places = sel.at[96:480], sel.at[480:496], sel.at[496:880]
    rows, rows_far, rim_of = sel.at[880:1008, 0:128], sel.at[1008:1136, 0:16], sel.at[1136:1200, 0:64]
    beside, back = sel.at[1200:1456, 0:128], sel.at[1456:1840, 0:384]

    hv[...] = jnp.zeros_like(hv)
    he[...] = jnp.zeros_like(he)
    hg[...] = jnp.zeros_like(hg)
    vs[288:384, :] = jnp.zeros((96, 384), BF16)
    for i4 in (0, 3):
        gx[:, i4] = jnp.zeros((2, 32, 512), BF16)
    rv[:, :, 24:32] = jnp.zeros((4, 4, 8, 384), BF16)
    lm[4] = jnp.zeros((16, 16, 256), BF16)

    barrier = pltpu.get_barrier_semaphore()
    up, down, lef, rig = r > 0, r < 7, c > 0, c < 15
    near = [
        (up, {"row": r - 1}), (down, {"row": r + 1}), (lef, {"col": c - 1}), (rig, {"col": c + 1}),
        (up & lef, {"row": r - 1, "col": c - 1}), (up & rig, {"row": r - 1, "col": c + 1}),
        (down & lef, {"row": r + 1, "col": c - 1}), (down & rig, {"row": r + 1, "col": c + 1}),
    ]
    yp, ym = {"row": (r + 2) % 8}, {"row": (r + 6) % 8}
    xp, xm = {"col": z * 4 + (x + 1) % 4}, {"col": z * 4 + (x + 3) % 4}
    other = {"row": y * 2 + 1 - core}
    zs = [{"col": ((z + d) % 4) * 4 + x} for d in (1, 2, 3)]
    partner = {"mp": 1 - m}

    def greet(to):
        pl.semaphore_signal(barrier, inc=1, device_id=to, device_id_type=MESH)

    for to in (yp, ym, {"row": (r + 4) % 8}, xp, xm, other, *zs, partner):
        greet(to)
    for there, to in near:
        pl.when(there)(lambda to=to: greet(to))

    def one_if(p):
        return jnp.where(p, jnp.int32(1), jnp.int32(0))

    n_near = (1 + one_if(up) + one_if(down)) * (1 + one_if(lef) + one_if(rig)) - 1

    count = iter(range(N_SEMS))

    def remote(src, dst, to):
        k = next(count)
        return pltpu.make_async_remote_copy(
            src_ref=src, dst_ref=dst, send_sem=send.at[k], recv_sem=recv.at[k],
            device_id=to, device_id_type=MESH,
        )

    for k in range(3):
        loads[k].wait()
    vs[288:352, :] = dot(rim[...], vs[0:288, :]).astype(BF16)
    sb[...] = dot(pick[...], vs[...], ((1,), (1,))).astype(BF16)
    sg[...] = dot(ends[...], gx[:, 1:3].reshape(128, 512)).astype(BF16)
    loads[3].wait()
    loads[4].wait()

    pl.semaphore_wait(barrier, 10 + n_near)

    corner = (slice(None), slice(256, 384))
    halo = [
        (remote(vs.at[288:320], hv.at[0:32], {"row": r + 1}), down, up),
        (remote(vs.at[320:352], hv.at[32:64], {"row": r - 1}), up, down),
        (remote(sb, he.at[0], {"col": c + 1}), rig, lef),
        (remote(sb, he.at[1], {"col": c - 1}), lef, rig),
        (remote(sb.at[corner], he.at[2].at[corner], {"row": r + 1, "col": c + 1}), down & rig, up & lef),
        (remote(sb.at[corner], he.at[3].at[corner], {"row": r - 1, "col": c + 1}), up & rig, down & lef),
        (remote(sb.at[corner], he.at[4].at[corner], {"row": r + 1, "col": c - 1}), down & lef, up & rig),
        (remote(sb.at[corner], he.at[5].at[corner], {"row": r - 1, "col": c - 1}), up & lef, down & rig),
    ]
    for copy, sent, _ in halo:
        pl.when(sent)(lambda copy=copy: copy.start())

    def slice_of(to, s):
        return v3.at[chosen((y + to) % 4, [f[s] for f in FRAMES_OF])]

    v_far_p = [remote(slice_of(2, s), rq.at[0, s], yp) for s in (0, 1)]
    v_far_m = [remote(slice_of(2, s + 2), rq.at[1, s], ym) for s in (0, 1)]
    g_p = remote(gbuf.at[:, 0], gbuf.at[:, 1], yp)
    g_m = remote(gbuf.at[:, 0], gbuf.at[:, 2], ym)
    v_p = [remote(slice_of(1, s), rv.at[1, s, 0:24], yp) for s in range(4)]
    v_m = [remote(slice_of(3, s), rv.at[2, s, 0:24], ym) for s in range(4)]
    for one in (*v_far_p, *v_far_m, g_p, g_m, *v_p, *v_m):
        one.start()
    g_in = remote(gx.at[:, 2 - core], gx.at[:, 3 * core], other)
    g_in.start()
    token_halo = [
        (remote(sg, hg.at[0], {"col": c + 1}), rig, lef),
        (remote(sg, hg.at[1], {"col": c - 1}), lef, rig),
        (remote(sg, hg.at[2], {"row": r + 1, "col": c + 1}), down & rig, up & lef),
        (remote(sg, hg.at[3], {"row": r - 1, "col": c + 1}), up & rig, down & lef),
        (remote(sg, hg.at[4], {"row": r + 1, "col": c - 1}), down & lef, up & rig),
        (remote(sg, hg.at[5], {"row": r - 1, "col": c - 1}), up & lef, down & rig),
    ]
    for copy, sent, _ in token_halo:
        pl.when(sent)(lambda copy=copy: copy.start())

    loads[5].wait()
    for copy, _, got in halo:
        pl.when(got)(lambda copy=copy: copy.wait_recv())

    sub = lax.broadcasted_iota(jnp.int32, (16, 128), 0)
    lane = lax.broadcasted_iota(jnp.int32, (16, 128), 1)
    for n in range(3):
        tile = slice(128 * n, 128 * n + 128)

        def edge(beside_, above, below):
            out = he[beside_, :, tile].astype(F32)
            if n == 2:
                out = jnp.where(
                    lane < 32, out,
                    jnp.where(lane < 64, he[above, :, tile].astype(F32), he[below, :, tile].astype(F32)),
                )
            return out

        hs[:, tile] = jnp.where(sub < 2, edge(1, 4, 5), edge(0, 2, 3)).astype(BF16)
    rim_rows = dot(rim_of[...], hv[...]).astype(BF16)
    rim_cols = dot(hs[...], places[...]).astype(BF16)
    for at in range(4):
        ex[at, :, 0:384] = rim_rows[16 * at : 16 * at + 16]
        ex[at, :, 384:512] = rim_cols[:, 128 * at : 128 * at + 128]
    e_far = remote(ex.at[(y + 2) % 4], er.at[3], {"row": (r + 4) % 8})
    e_p = remote(ex.at[(y + 1) % 4], er.at[1], yp)
    e_m = remote(ex.at[(y + 3) % 4], er.at[2], ym)
    for one in (e_far, e_p, e_m):
        one.start()
    er[0] = ex[y]

    for one in v_far_p:
        one.wait_recv()
    vf_p = remote(rq.at[0], rv.at[3, 0:2, 0:24], yp)
    vf_p.start()
    for one in v_far_m:
        one.wait_recv()
    vf_m = remote(rq.at[1], rv.at[3, 2:4, 0:24], ym)
    vf_m.start()
    g_p.wait_recv()
    gf_p = remote(gbuf.at[0, 1], gbuf.at[0, 3], yp)
    gf_p.start()
    g_m.wait_recv()
    gf_m = remote(gbuf.at[1, 2], gbuf.at[1, 3], ym)
    gf_m.start()
    g_out = remote(gbuf.at[:, 2 - core, core], gx.at[:, 3 - 3 * core], other)
    g_sent = ((core == 0) & (y < 3)) | ((core == 1) & (y > 0))
    g_got = ((core == 0) & (y > 0)) | ((core == 1) & (y < 3))
    pl.when(g_sent)(g_out.start)

    g_in.wait_recv()
    pl.when(g_got)(g_out.wait_recv)
    for copy, _, got in token_halo:
        pl.when(got)(lambda copy=copy: copy.wait_recv())
    loads[6].wait()

    ge[...] = dot(beside[...], hg[...].reshape(128, 512)).astype(BF16)

    def token_grads(first, last):
        @pl.loop(first, last)
        def _(k):
            at = pl.ds(pl.multiple_of(k * 256, 256), 256)
            for n, right in enumerate((gx[...].reshape(256, 512), ge[...])):
                block = dot(wv[at, :], right, ((1,), (1,)))
                pg[2 * n, at, :] = block[:, 0:128]
                pg[2 * n + 1, at, :] = block[:, 128:256]

    token_grads(0, 12)

    def frames(e, first):
        early = pg[first, pl.ds(e, 192, stride=16), :].reshape(12, 16, 128)
        late = pg[first + 1, pl.ds(e, 192, stride=16), :].reshape(12, 16, 128)
        out = []
        for ch in range(0, 12, 4):
            out += [
                early[ch + 1], early[ch + 2] + late[ch], early[ch + 3] + late[ch + 1], late[ch + 2],
            ]
        return jnp.stack(out)

    j = lax.broadcasted_iota(jnp.int32, (12, 16, 128), 2) % 32
    sub = lax.broadcasted_iota(jnp.int32, (12, 8, 128), 1)
    wrap = {0: (14, 0, 1), 1: (15, 0, 1), 10: (0, 31, 127), 11: (1, 31, 127)}
    for e in range(12):
        cell = frames(e + 2, 0)
        if e in wrap:
            far, at, by = wrap[e]
            cell = cell + jnp.where(j == at, frames(far, 2), pltpu.roll(frames(far, 0), by, 2))
        low, high = cell[:, 0:8], cell[:, 8:16]
        to_low = pltpu.roll(pltpu.roll(high, 32, 2), 4, 1)
        to_high = pltpu.roll(pltpu.roll(low, 96, 2), 4, 1)
        fs[e, :, 0:8] = low + jnp.where((sub == 2) | (sub == 3), to_low, 0.0)
        fs[e, :, 8:16] = high + jnp.where((sub == 4) | (sub == 5), to_high, 0.0)
    block = lax.broadcasted_iota(jnp.int32, (192, 128), 1) // 32
    for i in range(2):
        for k in range(3):
            row = None
            for q in range(4):
                part = fs[4 * k + q].reshape(192, 128)
                by = ((q - i - 1) * 32) % 128
                if by:
                    part = pltpu.roll(part, by, 1)
                row = part if row is None else jnp.where(block == q, part, row)
            upper = row.astype(BF16)
            ll[192 * i : 192 * i + 192, 128 * k : 128 * k + 128] = upper
            ll[384 + 192 * i : 576 + 192 * i, 128 * k : 128 * k + 128] = (row - upper.astype(F32)).astype(BF16)
    pixels = (dot(ll[0:384, :], back[...]) + dot(ll[384:768, :], back[...])).reshape(2, 12, 16, 384)
    for i in range(2):
        for cf in range(12):
            ch, f = cf // 4, cf % 4
            vg[f // 2, ch * 2 + f % 2, 12 * i : 12 * i + 12, :] = pixels[i, cf, 2:14, :]
    top = largest(vg[1 - m])
    ms[0:16] = spread(top, 384)
    ms[16:160] = coded(vg[1 - m], top)
    v_x = remote(ms, mr, partner)
    v_x.start()

    def unfold(n):
        at = dot(rv[n].reshape(128, 384), cols[...])
        at = (at + dot(er[n, :, 384:512], side[...], ((0,), (0,)))).astype(BF16)
        far = dot(er[n, :, 0:384], cols[...]).astype(BF16)
        qr[n] = (dot(rows[...], at) + dot(rows_far[...], far)).astype(BF16).reshape(2, 4, 16, 512)

    block = lax.broadcasted_iota(jnp.int32, (64, 128), 1) // 32

    def merge(half):
        for k in range(4):
            parts = [
                qr[2 * half + n // 2, n % 2, :, :, 128 * k : 128 * k + 128].astype(F32).reshape(64, 128)
                for n in range(4)
            ]
            for q in range(4):
                row = None
                for n in range(4):
                    by = ((n - q) * 32) % 128
                    part = pltpu.roll(parts[n], by, 1) if by else parts[n]
                    row = part if row is None else jnp.where(block == n, part, row)
                lm[0:4, 4 * k + q, :, 128 * half : 128 * half + 128] = row.astype(BF16).reshape(4, 16, 128)

    for k in range(7, 11):
        loads[k].wait()
    for one in (*v_p, *v_m, e_p, e_m):
        one.wait_recv()
    for n in range(3):
        unfold(n)
    merge(0)

    for one in (vf_p, vf_m, e_far, gf_p, gf_m):
        one.wait_recv()

    unfold(3)
    merge(1)

    give = []
    for p in range(PIECES):
        for ca in range(3):
            total = None
            for t in range(2):
                at = chosen(y, [s[t][ca] for s in SLOTS_OF])
                right = gbuf[t, :, :, :, 128 * WIDE * p : 128 * WIDE * (p + 1)].reshape(256, 128 * WIDE)
                part = dot(lm[at].reshape(256, 256), right)
                total = part if total is None else total + part
            for e in range(16):
                for n in range(WIDE):
                    wg[WIDE * p + n, pl.ds(ca * 256 + e, 16, stride=16), :] = (
                        total[16 * e : 16 * e + 16, 128 * n : 128 * n + 128]
                    )
        tiles = slice(WIDE * p, WIDE * p + WIDE)
        give.append(remote(wg.at[tiles, pl.ds((1 - core) * 384, 384)], cr.at[tiles], other))
        give[p].start()

    x1, x2, x3 = (x + 1) % 4, (x + 2) % 4, (x + 3) % 4
    far, near, last, tops = [], [], [], []
    halves = (slice(0, 2), slice(2, 4))
    ring = (xp, xm)
    beyond = (x1, x3)
    block = (WIDE, 2, 24, 128)
    for p in range(PIECES):
        tiles = slice(WIDE * p, WIDE * p + WIDE)
        give[p].wait_recv()
        for n in range(WIDE * p, WIDE * p + WIDE):
            for k in range(16):
                a1[n, k // 4, k % 4] = wg[n, pl.ds(core * 384 + 24 * k, 24), :] + cr[n, 24 * k : 24 * k + 24, :]
        tops.append(largest(a1[tiles]))
        for d in range(2):
            fo[d, p, 0:16] = spread(tops[p], 128)
            fo[d, p, 16:] = coded(a1[tiles, halves[d], x2], tops[p])
            far.append(remote(fo.at[d, p], fi.at[d, p], ring[d]))
            far[-1].start()
    for p in range(PIECES):
        tiles = slice(WIDE * p, WIDE * p + WIDE)
        for d in range(2):
            no[d, p] = coded(a1[tiles, halves[1 - d], beyond[d]], tops[p])
            near.append(remote(no.at[d, p], ni.at[d, p], ring[d]))
            near[-1].start()

    for p in range(PIECES):
        tiles = slice(WIDE * p, WIDE * p + WIDE)
        for d in range(2):
            far[2 * p + d].wait_recv()
            top = fi[d, p, 0:16].astype(F32)[0:1]
            total = a1[tiles, halves[d], beyond[d]] + decoded(fi[d, p, 16:], top, block)
            top = ((top[:, 0:1] + tops[p]) * 1.01).astype(BF16).astype(F32)
            lo[d, p, 0:16] = spread(top, 128)
            lo[d, p, 16:] = coded(total, top)
            last.append(remote(lo.at[d, p], li.at[d, p], ring[d]))
            last[-1].start()

    z_out = []
    for p in range(PIECES):
        tiles = slice(WIDE * p, WIDE * p + WIDE)
        for d in range(2):
            near[2 * p + d].wait_recv()
            top = fi[d, p, 0:16].astype(F32)[0:1]
            a1[tiles, halves[1 - d], x] = a1[tiles, halves[1 - d], x] + decoded(ni[d, p], top, block)
        for d in range(2):
            last[2 * p + d].wait_recv()
            top = li[d, p, 0:16].astype(F32)[0:1]
            a2[tiles, halves[d]] = a1[tiles, halves[d], x] + decoded(li[d, p, 16:], top, block)
        z_out.append([remote(a2.at[tiles, (z + d + 1) % 4], zr.at[d, tiles], zs[d]) for d in (2, 1, 0)])
        for one in z_out[p]:
            one.start()

    v_x.wait_recv()
    vg[m] = vg[m] + decoded(mr[16:160], mr[0:16].astype(F32)[0:1], (6, 24, 384))
    v_out = pltpu.make_async_copy(vg.at[m], vout, load.at[11])
    v_out.start()

    for p in range(PIECES):
        for one in z_out[p]:
            one.wait_recv()
        for n in range(WIDE * p, WIDE * p + WIDE):
            wout[:, 128 * n : 128 * n + 128] = (a2[n, z] + zr[0, n] + (zr[1, n] + zr[2, n])) * (1.0 / 128.0)

    v_out.wait()
    for copy, sent, _ in halo + token_halo:
        pl.when(sent)(lambda copy=copy: copy.wait_send())
    pl.when(g_sent)(g_out.wait_send)
    for one in (
        g_p, g_m, g_in, gf_p, gf_m, *v_far_p, *v_far_m, *v_p, *v_m, vf_p, vf_m, e_p, e_m, e_far, v_x,
        *give, *far, *near, *last, *sum(z_out, []),
    ):
        one.wait_send()


def shards(video, grad_tokens, weight):
    packed = jnp.asarray(selections(), BF16)
    anywhere = pl.BlockSpec(memory_space=pltpu.HBM)
    in_vmem = pl.BlockSpec(memory_space=pltpu.VMEM)

    def v(*shape, kind=F32):
        return pltpu.VMEM(shape, kind)

    def b(*shape):
        return pltpu.VMEM(shape, BF16)

    video_grad, weight_grad = pl.pallas_call(
        kernel,
        out_shape=(
            jax.ShapeDtypeStruct((6, 24, 384), F32),
            jax.ShapeDtypeStruct((24, 512), F32),
        ),
        in_specs=[anywhere] * 5,
        out_specs=(pl.BlockSpec(memory_space=pl.ANY), in_vmem),
        scratch_shapes=[
            b(SELECTION_ROWS, 512),
            b(3072, 512), b(384, 384), b(12, 24, 384), b(4, 4, 32, 384), b(2, 2, 24, 384), b(64, 384),
            b(6, 16, 384), b(8, 16, 512), b(16, 384), b(16, 512), b(16, 384), b(4, 16, 512), b(4, 16, 512),
            b(2, 4, 32, 512), b(256, 512), b(2, 4, 2, 32, 512),
            b(4, 2, 4, 16, 512), b(5, 16, 16, 256),
            v(4, 3072, 128), v(12, 12, 16, 128), b(768, 384), v(2, 6, 24, 384), b(160, 384), b(160, 384),
            v(4, 768, 128), v(4, 384, 128), v(4, 4, 4, 24, 128),
            *[b(2, PIECES, rows, 128) for rows in (CODED + 16, CODED + 16, CODED, CODED, CODED + 16, CODED + 16)],
            v(4, 4, 24, 128),
            v(3, 4, 24, 128),
            pltpu.SemaphoreType.DMA((12,)),
            pltpu.SemaphoreType.DMA((N_SEMS,)),
            pltpu.SemaphoreType.DMA((N_SEMS,)),
        ],
        compiler_params=pltpu.CompilerParams(
            collective_id=0, has_side_effects=True, vmem_limit_bytes=VMEM_BYTES
        ),
        name="tubelet_backward",
    )(video.reshape(288, 384), video.reshape(12, 24, 384), grad_tokens, weight, packed)
    return video_grad.reshape(3, 2, 24, 384), weight_grad


def solution(mesh):
    return jax.shard_map(
        shards,
        mesh=mesh,
        in_specs=(P(None, None, "row", "col"), P(None, "row", "col", "mp"), P(None, "mp")),
        out_specs=(P(None, "mp", "row", "col"), P(("row", "col"), "mp")),
        check_vma=False,
    )
```

```python
import jax
import jax.numpy as jnp
import numpy as np
from jax import lax
from jax.experimental import pallas as pl
from jax.experimental.pallas import tpu as pltpu
from jax.sharding import PartitionSpec as P

MESH = pl.DeviceIdType.MESH
F32 = jnp.float32
BF16 = jnp.bfloat16
N_SEMS = 80
FRAMES_OF = ((0, 1, 2, 3), (2, 4, 5, 6), (5, 6, 7, 9), (8, 9, 10, 11))
VMEM_BYTES = 56500000
PIECES = 2
WIDE = 4 // PIECES
CODED = WIDE * 48
SELECTION_AT = (0, 16, 80, 96, 480, 496, 880, 1008, 1136, 1200, 1328)
SELECTION_ROWS = 1712


def selections():
    cols = np.zeros((384, 512), np.float32)
    for e in range(16):
        for j in range(32):
            x = 12 * j + e - 2
            if 0 <= x < 384:
                cols[x, e * 32 + j] = 1
    side = np.zeros((16, 512), np.float32)
    side[2, 0] = side[3, 32] = 1
    side[0, 14 * 32 + 31] = side[1, 15 * 32 + 31] = 1
    rim_of = np.zeros((64, 64), np.float32)
    places = np.zeros((384, 512), np.float32)
    for at in range(4):
        for s, cf in enumerate(FRAMES_OF[at]):
            for k in range(24):
                places[cf * 24 + k, at * 128 + s * 32 + k] = 1
            for k in range(4):
                far = (k // 2) * 32 + cf * 2 + k % 2
                rim_of[at * 16 + s * 4 + k, far] = 1
                places[288 + far, at * 128 + s * 32 + 24 + k] = 1
    rows = np.zeros((128, 128), np.float32)
    rows_far = np.zeros((128, 16), np.float32)
    for i in range(2):
        for s in range(4):
            for b in range(16):
                y = 12 * i + b - 2
                k = y + 2 if y < 0 else y - 22
                rows[i * 64 + s * 16 + b, s * 32 + (y if 0 <= y < 24 else 24 + k)] = 1
                if not 0 <= y < 24:
                    rows_far[i * 64 + s * 16 + b, s * 4 + k] = 1
    pick = np.zeros((16, 384), np.float32)
    for k, x in enumerate((0, 1, 382, 383)):
        pick[k, x] = 1
    rim = np.zeros((64, 288), np.float32)
    for cf in range(12):
        for k in range(2):
            rim[cf * 2 + k, cf * 24 + 22 + k] = 1
            rim[32 + cf * 2 + k, cf * 24 + k] = 1
    ends = np.zeros((16, 128), np.float32)
    for ti in range(4):
        ends[ti, ti * 32] = 1
        ends[4 + ti, ti * 32 + 31] = 1
    beside = np.zeros((128, 128), np.float32)
    for t in range(2):
        for n in range(4):
            i = (0, 1, 0, 1)[n]
            left = (0, 0, 3, 2)[n]
            right = (1, 1, 5, 4)[n]
            beside[n * 32 + 16 * t, left * 16 + 4 + t * 2 + i] = 1
            beside[n * 32 + 31 - 16 * t, right * 16 + t * 2 + i] = 1
    back = np.zeros((384, 384), np.float32)
    for e in range(12):
        for j in range(32):
            back[e * 32 + j, 12 * j + e] = 1
    packed = np.zeros((SELECTION_ROWS, 512), np.float32)
    for at, one in zip(SELECTION_AT, (pick, rim, ends, cols, side, places, rows, rows_far, rim_of, beside, back)):
        packed[at : at + one.shape[0], : one.shape[1]] = one
    return packed


def chosen(at, values):
    out = jnp.int32(values[3])
    for k in range(3):
        out = jnp.where(at == k, jnp.int32(values[k]), out)
    return out


SLOTS_OF = (
    (((4, 0, 1), (1, 2, 3))),
    (((0, 4, 1), (4, 2, 3))),
    (((0, 1, 4), (2, 4, 3))),
    (((0, 1, 2), (2, 3, 4))),
)


def dot(a, b, dims=((1,), (0,))):
    return lax.dot_general(a, b, (dims, ((), ())), preferred_element_type=F32)


TOP = 2.0**15


def largest(x):
    top = jnp.abs(x).reshape(-1, x.shape[-1])
    top = jnp.max(jnp.max(top, axis=0, keepdims=True), axis=1, keepdims=True)
    return (jnp.maximum(top, 1e-25) * 1.01).astype(BF16).astype(F32)


def packed_rows(x):
    return x.reshape(-1, x.shape[-1])


def coded(x, top):
    t = packed_rows(x) * (TOP / top)
    t2 = t * t
    t4 = t2 * t2
    return (t4 * t2 * jnp.abs(t) * t).astype(BF16)


def decoded(code, top, shape):
    v = code.astype(F32)
    t = jnp.sqrt(jnp.sqrt(jnp.sqrt(jnp.abs(v)))) * (top * (1.0 / TOP))
    return jnp.where(v < 0, -t, t).reshape(shape)


def spread(top, lanes):
    return jnp.broadcast_to(top, (16, lanes)).astype(BF16)


def kernel(
    video, frames_h, tokens, weight, packed,
    vout, wout,
    sel,
    wv, vs, v3, rv, rq, hv, he, hg, sb, sg, hs, ex, er, gx, gh, gbuf, qr, lm, pg, fs, ll, vg, ms, mr,
    wg, cr, a1, fo, fi, no, ni, lo, li, a2, zr,
    load, send, recv,
):
    r = lax.axis_index("row")
    c = lax.axis_index("col")
    m = lax.axis_index("mp")
    y, core = r // 2, r % 2
    z, x = c // 4, c % 4

    pairs = [
        (video, vs.at[0:288]), (packed.at[0:96], sel.at[0:96]), (tokens, gx.at[:, 0:2]),
        (tokens, gbuf.at[:, 0]), (frames_h, v3), (packed.at[96:SELECTION_ROWS], sel.at[96:SELECTION_ROWS]),
        (weight, wv),
    ]
    for s in range(4):
        pairs.append((frames_h.at[chosen(y, [f[s] for f in FRAMES_OF])], rv.at[0, s, 0:24]))
    loads = [pltpu.make_async_copy(a, b, load.at[k]) for k, (a, b) in enumerate(pairs)]
    for one in loads:
        one.start()

    pick, rim, ends = sel.at[0:16, 0:384], sel.at[16:80, 0:288], sel.at[80:96, 0:128]
    cols, side, places = sel.at[96:480], sel.at[480:496], sel.at[496:880]
    rows, rows_far, rim_of = sel.at[880:1008, 0:128], sel.at[1008:1136, 0:16], sel.at[1136:1200, 0:64]
    beside, back = sel.at[1200:1328, 0:128], sel.at[1328:1712, 0:384]

    hv[...] = jnp.zeros_like(hv)
    he[...] = jnp.zeros_like(he)
    hg[...] = jnp.zeros_like(hg)
    vs[288:384, :] = jnp.zeros((96, 384), BF16)
    gx[:, 2:4] = jnp.zeros((2, 2, 32, 512), BF16)
    rv[:, :, 24:32] = jnp.zeros((4, 4, 8, 384), BF16)
    lm[4] = jnp.zeros((16, 16, 256), BF16)

    barrier = pltpu.get_barrier_semaphore()
    up, down, lef, rig = r > 0, r < 7, c > 0, c < 15
    near = [
        (up, {"row": r - 1}), (down, {"row": r + 1}), (lef, {"col": c - 1}), (rig, {"col": c + 1}),
        (up & lef, {"row": r - 1, "col": c - 1}), (up & rig, {"row": r - 1, "col": c + 1}),
        (down & lef, {"row": r + 1, "col": c - 1}), (down & rig, {"row": r + 1, "col": c + 1}),
    ]
    yp, ym = {"row": (r + 2) % 8}, {"row": (r + 6) % 8}
    xp, xm = {"col": z * 4 + (x + 1) % 4}, {"col": z * 4 + (x + 3) % 4}
    other = {"row": y * 2 + 1 - core}
    zs = [{"col": ((z + d) % 4) * 4 + x} for d in (1, 2, 3)]
    partner = {"mp": 1 - m}

    def greet(to):
        pl.semaphore_signal(barrier, inc=1, device_id=to, device_id_type=MESH)

    for to in (yp, ym, {"row": (r + 4) % 8}, xp, xm, other, *zs, partner):
        greet(to)
    for there, to in near:
        pl.when(there)(lambda to=to: greet(to))

    def one_if(p):
        return jnp.where(p, jnp.int32(1), jnp.int32(0))

    n_near = (1 + one_if(up) + one_if(down)) * (1 + one_if(lef) + one_if(rig)) - 1

    count = iter(range(N_SEMS))

    def remote(src, dst, to):
        k = next(count)
        return pltpu.make_async_remote_copy(
            src_ref=src, dst_ref=dst, send_sem=send.at[k], recv_sem=recv.at[k],
            device_id=to, device_id_type=MESH,
        )

    for k in range(3):
        loads[k].wait()
    vs[288:352, :] = dot(rim[...], vs[0:288, :]).astype(BF16)
    sb[...] = dot(pick[...], vs[...], ((1,), (1,))).astype(BF16)
    sg[...] = dot(ends[...], gx[:, 0:2].reshape(128, 512)).astype(BF16)
    loads[3].wait()
    loads[4].wait()

    pl.semaphore_wait(barrier, 10 + n_near)

    corner = (slice(None), slice(256, 384))
    halo = [
        (remote(vs.at[288:320], hv.at[0:32], {"row": r + 1}), down, up),
        (remote(vs.at[320:352], hv.at[32:64], {"row": r - 1}), up, down),
        (remote(sb, he.at[0], {"col": c + 1}), rig, lef),
        (remote(sb, he.at[1], {"col": c - 1}), lef, rig),
        (remote(sb.at[corner], he.at[2].at[corner], {"row": r + 1, "col": c + 1}), down & rig, up & lef),
        (remote(sb.at[corner], he.at[3].at[corner], {"row": r - 1, "col": c + 1}), up & rig, down & lef),
        (remote(sb.at[corner], he.at[4].at[corner], {"row": r + 1, "col": c - 1}), down & lef, up & rig),
        (remote(sb.at[corner], he.at[5].at[corner], {"row": r - 1, "col": c - 1}), up & lef, down & rig),
    ]
    for copy, sent, _ in halo:
        pl.when(sent)(lambda copy=copy: copy.start())

    def slice_of(to, s):
        return v3.at[chosen((y + to) % 4, [f[s] for f in FRAMES_OF])]

    v_far_p = [remote(slice_of(2, s), rq.at[0, s], yp) for s in (0, 1)]
    v_far_m = [remote(slice_of(2, s + 2), rq.at[1, s], ym) for s in (0, 1)]
    g_p = remote(gbuf.at[:, 0], gbuf.at[:, 1], yp)
    g_m = remote(gbuf.at[:, 0], gbuf.at[:, 2], ym)
    v_p = [remote(slice_of(1, s), rv.at[1, s, 0:24], yp) for s in range(4)]
    v_m = [remote(slice_of(3, s), rv.at[2, s, 0:24], ym) for s in range(4)]
    for one in (g_p, g_m, *v_far_p, *v_far_m, *v_p, *v_m):
        one.start()
    g_in = remote(gx.at[:, 1 - core], gx.at[:, 3 - core], other)
    g_in.start()
    token_halo = [
        (remote(sg, hg.at[0], {"col": c + 1}), rig, lef),
        (remote(sg, hg.at[1], {"col": c - 1}), lef, rig),
        (remote(sg, hg.at[2], {"row": r + 1, "col": c + 1}), down & rig, up & lef),
        (remote(sg, hg.at[3], {"row": r - 1, "col": c + 1}), up & rig, down & lef),
        (remote(sg, hg.at[4], {"row": r + 1, "col": c - 1}), down & lef, up & rig),
        (remote(sg, hg.at[5], {"row": r - 1, "col": c - 1}), up & lef, down & rig),
    ]
    for copy, sent, _ in token_halo:
        pl.when(sent)(lambda copy=copy: copy.start())

    loads[6].wait()

    @pl.loop(0, 12)
    def _(k):
        at = pl.ds(pl.multiple_of(k * 256, 256), 256)
        pg[0, at, :] = dot(wv[at, :], gx[:, 0:2].reshape(128, 512), ((1,), (1,)))

    loads[5].wait()
    for copy, _, got in halo:
        pl.when(got)(lambda copy=copy: copy.wait_recv())

    sub = lax.broadcasted_iota(jnp.int32, (16, 128), 0)
    lane = lax.broadcasted_iota(jnp.int32, (16, 128), 1)
    for n in range(3):
        tile = slice(128 * n, 128 * n + 128)

        def edge(beside_, above, below):
            out = he[beside_, :, tile].astype(F32)
            if n == 2:
                out = jnp.where(
                    lane < 32, out,
                    jnp.where(lane < 64, he[above, :, tile].astype(F32), he[below, :, tile].astype(F32)),
                )
            return out

        hs[:, tile] = jnp.where(sub < 2, edge(1, 4, 5), edge(0, 2, 3)).astype(BF16)
    rim_rows = dot(rim_of[...], hv[...]).astype(BF16)
    rim_cols = dot(hs[...], places[...]).astype(BF16)
    for at in range(4):
        ex[at, :, 0:384] = rim_rows[16 * at : 16 * at + 16]
        ex[at, :, 384:512] = rim_cols[:, 128 * at : 128 * at + 128]
    e_far = remote(ex.at[(y + 2) % 4], er.at[3], {"row": (r + 4) % 8})
    e_p = remote(ex.at[(y + 1) % 4], er.at[1], yp)
    e_m = remote(ex.at[(y + 3) % 4], er.at[2], ym)
    for one in (e_far, e_p, e_m):
        one.start()
    er[0] = ex[y]

    def unfold(n):
        at = dot(rv[n].reshape(128, 384), cols[...])
        at = (at + dot(er[n, :, 384:512], side[...], ((0,), (0,)))).astype(BF16)
        far = dot(er[n, :, 0:384], cols[...]).astype(BF16)
        qr[n] = (dot(rows[...], at) + dot(rows_far[...], far)).astype(BF16).reshape(2, 4, 16, 512)

    block = lax.broadcasted_iota(jnp.int32, (64, 128), 1) // 32

    def merge(half):
        for k in range(4):
            parts = [
                qr[2 * half + n // 2, n % 2, :, :, 128 * k : 128 * k + 128].astype(F32).reshape(64, 128)
                for n in range(4)
            ]
            for q in range(4):
                row = None
                for n in range(4):
                    by = ((n - q) * 32) % 128
                    part = pltpu.roll(parts[n], by, 1) if by else parts[n]
                    row = part if row is None else jnp.where(block == n, part, row)
                lm[0:4, 4 * k + q, :, 128 * half : 128 * half + 128] = row.astype(BF16).reshape(4, 16, 128)

    for k in range(7, 11):
        loads[k].wait()
    unfold(0)

    g_p.wait_recv()
    gf_p = remote(gbuf.at[0, 1], gbuf.at[0, 3], yp)
    gf_p.start()
    g_m.wait_recv()
    gf_m = remote(gbuf.at[1, 2], gbuf.at[1, 3], ym)
    gf_m.start()
    g_out = remote(gbuf.at[:, 2 - core, core], gx.at[:, 2 + core], other)
    g_sent = ((core == 0) & (y < 3)) | ((core == 1) & (y > 0))
    g_got = ((core == 0) & (y > 0)) | ((core == 1) & (y < 3))
    pl.when(g_sent)(g_out.start)

    for one in v_far_p:
        one.wait_recv()
    vf_p = remote(rq.at[0], rv.at[3, 0:2, 0:24], yp)
    vf_p.start()
    for one in v_far_m:
        one.wait_recv()
    vf_m = remote(rq.at[1], rv.at[3, 2:4, 0:24], ym)
    vf_m.start()

    g_in.wait_recv()
    pl.when(g_got)(g_out.wait_recv)
    for copy, _, got in token_halo:
        pl.when(got)(lambda copy=copy: copy.wait_recv())

    gh[0:128] = gx[:, 2:4].reshape(128, 512)
    gh[128:256] = dot(beside[...], hg[...].reshape(128, 512)).astype(BF16)

    @pl.loop(0, 12)
    def _(k):
        at = pl.ds(pl.multiple_of(k * 256, 256), 256)
        out = dot(wv[at, :], gh[...], ((1,), (1,)))
        pg[1, at, :] = out[:, 0:128]
        pg[2, at, :] = out[:, 128:256]

    for one in (*v_p, *v_m, e_p, e_m):
        one.wait_recv()
    unfold(1)
    unfold(2)
    merge(0)

    first = lax.broadcasted_iota(jnp.int32, (12, 16, 128), 2) < 64

    def summed(early, late):
        out = []
        for ch in range(0, 12, 4):
            out += [
                early[ch + 1], early[ch + 2] + late[ch], early[ch + 3] + late[ch + 1], late[ch + 2],
            ]
        return jnp.stack(out)

    def rows_of(n, e):
        return pg[n, pl.ds(e, 192, stride=16), :].reshape(12, 16, 128)

    def frames(e):
        own, around = rows_of(0, e), rows_of(1, e)
        return summed(
            jnp.where(first, own, pltpu.roll(around, 64, 2)), jnp.where(first, pltpu.roll(own, 64, 2), around)
        )

    def frames_beside(e):
        both = rows_of(2, e)
        return summed(both, pltpu.roll(both, 16 if e < 8 else 112, 2))

    j = lax.broadcasted_iota(jnp.int32, (12, 16, 128), 2) % 32
    sub = lax.broadcasted_iota(jnp.int32, (12, 8, 128), 1)
    wrap = {0: (14, 0, 1), 1: (15, 0, 1), 10: (0, 31, 127), 11: (1, 31, 127)}
    for e in range(12):
        cell = frames(e + 2)
        if e in wrap:
            far, at, by = wrap[e]
            cell = cell + jnp.where(j == at, frames_beside(far), pltpu.roll(frames(far), by, 2))
        low, high = cell[:, 0:8], cell[:, 8:16]
        to_low = pltpu.roll(pltpu.roll(high, 32, 2), 4, 1)
        to_high = pltpu.roll(pltpu.roll(low, 96, 2), 4, 1)
        fs[e, :, 0:8] = low + jnp.where((sub == 2) | (sub == 3), to_low, 0.0)
        fs[e, :, 8:16] = high + jnp.where((sub == 4) | (sub == 5), to_high, 0.0)
    for one in (vf_p, vf_m, e_far, gf_p, gf_m):
        one.wait_recv()

    unfold(3)
    merge(1)

    give = []
    for p in range(PIECES):
        for ca in range(3):
            total = None
            for t in range(2):
                at = chosen(y, [s[t][ca] for s in SLOTS_OF])
                right = gbuf[t, :, :, :, 128 * WIDE * p : 128 * WIDE * (p + 1)].reshape(256, 128 * WIDE)
                part = dot(lm[at].reshape(256, 256), right)
                total = part if total is None else total + part
            for e in range(16):
                for n in range(WIDE):
                    wg[WIDE * p + n, pl.ds(ca * 256 + e, 16, stride=16), :] = (
                        total[16 * e : 16 * e + 16, 128 * n : 128 * n + 128]
                    )
        tiles = slice(WIDE * p, WIDE * p + WIDE)
        give.append(remote(wg.at[tiles, pl.ds((1 - core) * 384, 384)], cr.at[tiles], other))
        give[p].start()

    block = lax.broadcasted_iota(jnp.int32, (192, 128), 1) // 32
    for i in range(2):
        for k in range(3):
            row = None
            for q in range(4):
                part = fs[4 * k + q].reshape(192, 128)
                by = ((q - i) * 32) % 128
                if by:
                    part = pltpu.roll(part, by, 1)
                row = part if row is None else jnp.where(block == q, part, row)
            upper = row.astype(BF16)
            ll[192 * i : 192 * i + 192, 128 * k : 128 * k + 128] = upper
            ll[384 + 192 * i : 576 + 192 * i, 128 * k : 128 * k + 128] = (row - upper.astype(F32)).astype(BF16)
    pixels = (dot(ll[0:384, :], back[...]) + dot(ll[384:768, :], back[...])).reshape(2, 12, 16, 384)
    for i in range(2):
        for cf in range(12):
            ch, f = cf // 4, cf % 4
            vg[f // 2, ch * 2 + f % 2, 12 * i : 12 * i + 12, :] = pixels[i, cf, 2:14, :]
    top = largest(vg[1 - m])
    ms[0:16] = spread(top, 384)
    ms[16:160] = coded(vg[1 - m], top)
    v_x = remote(ms, mr, partner)
    v_x.start()

    x1, x2, x3 = (x + 1) % 4, (x + 2) % 4, (x + 3) % 4
    far, near, last, tops = [], [], [], []
    halves = (slice(0, 2), slice(2, 4))
    ring = (xp, xm)
    beyond = (x1, x3)
    block = (WIDE, 2, 24, 128)
    for p in range(PIECES):
        tiles = slice(WIDE * p, WIDE * p + WIDE)
        give[p].wait_recv()
        for n in range(WIDE * p, WIDE * p + WIDE):
            for k in range(16):
                a1[n, k // 4, k % 4] = wg[n, pl.ds(core * 384 + 24 * k, 24), :] + cr[n, 24 * k : 24 * k + 24, :]
        tops.append(largest(a1[tiles]))
        for d in range(2):
            fo[d, p, 0:16] = spread(tops[p], 128)
            fo[d, p, 16:] = coded(a1[tiles, halves[d], x2], tops[p])
            far.append(remote(fo.at[d, p], fi.at[d, p], ring[d]))
            far[-1].start()
    for p in range(PIECES):
        tiles = slice(WIDE * p, WIDE * p + WIDE)
        for d in range(2):
            no[d, p] = coded(a1[tiles, halves[1 - d], beyond[d]], tops[p])
            near.append(remote(no.at[d, p], ni.at[d, p], ring[d]))
            near[-1].start()

    for p in range(PIECES):
        tiles = slice(WIDE * p, WIDE * p + WIDE)
        for d in range(2):
            far[2 * p + d].wait_recv()
            top = fi[d, p, 0:16].astype(F32)[0:1]
            total = a1[tiles, halves[d], beyond[d]] + decoded(fi[d, p, 16:], top, block)
            top = ((top[:, 0:1] + tops[p]) * 1.01).astype(BF16).astype(F32)
            lo[d, p, 0:16] = spread(top, 128)
            lo[d, p, 16:] = coded(total, top)
            last.append(remote(lo.at[d, p], li.at[d, p], ring[d]))
            last[-1].start()

    z_out = []
    for p in range(PIECES):
        tiles = slice(WIDE * p, WIDE * p + WIDE)
        for d in range(2):
            near[2 * p + d].wait_recv()
            top = fi[d, p, 0:16].astype(F32)[0:1]
            a1[tiles, halves[1 - d], x] = a1[tiles, halves[1 - d], x] + decoded(ni[d, p], top, block)
        for d in range(2):
            last[2 * p + d].wait_recv()
            top = li[d, p, 0:16].astype(F32)[0:1]
            a2[tiles, halves[d]] = a1[tiles, halves[d], x] + decoded(li[d, p, 16:], top, block)
        z_out.append([remote(a2.at[tiles, (z + d + 1) % 4], zr.at[d, tiles], zs[d]) for d in (2, 1, 0)])
        for one in z_out[p]:
            one.start()

    v_x.wait_recv()
    vg[m] = vg[m] + decoded(mr[16:160], mr[0:16].astype(F32)[0:1], (6, 24, 384))
    v_out = pltpu.make_async_copy(vg.at[m], vout, load.at[11])
    v_out.start()

    for p in range(PIECES):
        for one in z_out[p]:
            one.wait_recv()
        for n in range(WIDE * p, WIDE * p + WIDE):
            wout[:, 128 * n : 128 * n + 128] = (a2[n, z] + zr[0, n] + (zr[1, n] + zr[2, n])) * (1.0 / 128.0)

    v_out.wait()
    for copy, sent, _ in halo + token_halo:
        pl.when(sent)(lambda copy=copy: copy.wait_send())
    pl.when(g_sent)(g_out.wait_send)
    for one in (
        g_p, g_m, g_in, gf_p, gf_m, *v_far_p, *v_far_m, *v_p, *v_m, vf_p, vf_m, e_p, e_m, e_far, v_x,
        *give, *far, *near, *last, *sum(z_out, []),
    ):
        one.wait_send()


def shards(video, grad_tokens, weight):
    packed = jnp.asarray(selections(), BF16)
    anywhere = pl.BlockSpec(memory_space=pltpu.HBM)
    in_vmem = pl.BlockSpec(memory_space=pltpu.VMEM)

    def v(*shape, kind=F32):
        return pltpu.VMEM(shape, kind)

    def b(*shape):
        return pltpu.VMEM(shape, BF16)

    video_grad, weight_grad = pl.pallas_call(
        kernel,
        out_shape=(
            jax.ShapeDtypeStruct((6, 24, 384), F32),
            jax.ShapeDtypeStruct((24, 512), F32),
        ),
        in_specs=[anywhere] * 5,
        out_specs=(pl.BlockSpec(memory_space=pl.ANY), in_vmem),
        scratch_shapes=[
            b(SELECTION_ROWS, 512),
            b(3072, 512), b(384, 384), b(12, 24, 384), b(4, 4, 32, 384), b(2, 2, 24, 384), b(64, 384),
            b(6, 16, 384), b(8, 16, 512), b(16, 384), b(16, 512), b(16, 384), b(4, 16, 512), b(4, 16, 512),
            b(2, 4, 32, 512), b(256, 512), b(2, 4, 2, 32, 512),
            b(4, 2, 4, 16, 512), b(5, 16, 16, 256),
            v(3, 3072, 128), v(12, 12, 16, 128), b(768, 384), v(2, 6, 24, 384), b(160, 384), b(160, 384),
            v(4, 768, 128), v(4, 384, 128), v(4, 4, 4, 24, 128),
            *[b(2, PIECES, rows, 128) for rows in (CODED + 16, CODED + 16, CODED, CODED, CODED + 16, CODED + 16)],
            v(4, 4, 24, 128),
            v(3, 4, 24, 128),
            pltpu.SemaphoreType.DMA((12,)),
            pltpu.SemaphoreType.DMA((N_SEMS,)),
            pltpu.SemaphoreType.DMA((N_SEMS,)),
        ],
        compiler_params=pltpu.CompilerParams(
            collective_id=0, has_side_effects=True, vmem_limit_bytes=VMEM_BYTES
        ),
        name="tubelet_backward",
    )(video.reshape(288, 384), video.reshape(12, 24, 384), grad_tokens, weight, packed)
    return video_grad.reshape(3, 2, 24, 384), weight_grad


def solution(mesh):
    return jax.shard_map(
        shards,
        mesh=mesh,
        in_specs=(P(None, None, "row", "col"), P(None, "row", "col", "mp"), P(None, "mp")),
        out_specs=(P(None, "mp", "row", "col"), P(("row", "col"), "mp")),
        check_vma=False,
    )
```

```python
import jax
import jax.numpy as jnp
import numpy as np
from jax import lax
from jax.experimental import pallas as pl
from jax.experimental.pallas import tpu as pltpu
from jax.sharding import PartitionSpec as P

MESH = pl.DeviceIdType.MESH
F32 = jnp.float32
BF16 = jnp.bfloat16
N_SEMS = 80
TALL = 1536
FRAMES_OF = ((0, 1, 2, 3), (2, 4, 5, 6), (5, 6, 7, 9), (8, 9, 10, 11))
VMEM_BYTES = 56500000
PIECES = 2
WIDE = 4 // PIECES
CODED = WIDE * 48
SELECTION_AT = (0, 16, 80, 96, 480, 496, 880, 1008, 1072, 1200)
SELECTION_ROWS = 1584


def selections():
    cols = np.zeros((384, 512), np.float32)
    for e in range(16):
        for j in range(32):
            x = 12 * j + e - 2
            if 0 <= x < 384:
                cols[x, e * 32 + j] = 1
    side = np.zeros((16, 512), np.float32)
    side[2, 0] = side[3, 32] = 1
    side[0, 14 * 32 + 31] = side[1, 15 * 32 + 31] = 1
    rim_of = np.zeros((64, 64), np.float32)
    places = np.zeros((384, 512), np.float32)
    for at in range(4):
        for s, cf in enumerate(FRAMES_OF[at]):
            for k in range(24):
                places[cf * 24 + k, at * 128 + s * 32 + k] = 1
            for k in range(4):
                far = (k // 2) * 32 + cf * 2 + k % 2
                rim_of[at * 16 + s * 4 + k, far] = 1
                places[288 + far, at * 128 + s * 32 + 24 + k] = 1
    rows = np.zeros((128, 144), np.float32)
    for i in range(2):
        for s in range(4):
            for b in range(16):
                y = 12 * i + b - 2
                k = y + 2 if y < 0 else y - 22
                rows[i * 64 + s * 16 + b, s * 32 + (y if 0 <= y < 24 else 24 + k)] = 1
                if not 0 <= y < 24:
                    rows[i * 64 + s * 16 + b, 128 + s * 4 + k] = 1
    pick = np.zeros((16, 384), np.float32)
    for k, x in enumerate((0, 1, 382, 383)):
        pick[k, x] = 1
    rim = np.zeros((64, 288), np.float32)
    for cf in range(12):
        for k in range(2):
            rim[cf * 2 + k, cf * 24 + 22 + k] = 1
            rim[32 + cf * 2 + k, cf * 24 + k] = 1
    ends = np.zeros((16, 128), np.float32)
    for ti in range(4):
        ends[ti, ti * 32] = 1
        ends[4 + ti, ti * 32 + 31] = 1
    beside = np.zeros((128, 128), np.float32)
    for t in range(2):
        for n in range(4):
            i = (0, 1, 0, 1)[n]
            left = (0, 0, 3, 2)[n]
            right = (1, 1, 5, 4)[n]
            beside[n * 32 + 16 * t, left * 16 + 4 + t * 2 + i] = 1
            beside[n * 32 + 31 - 16 * t, right * 16 + t * 2 + i] = 1
    back = np.zeros((384, 384), np.float32)
    for e in range(12):
        for j in range(32):
            back[e * 32 + j, 12 * j + e] = 1
    packed = np.zeros((SELECTION_ROWS, 512), np.float32)
    for at, one in zip(SELECTION_AT, (pick, rim, ends, cols, side, places, rows, rim_of, beside, back)):
        packed[at : at + one.shape[0], : one.shape[1]] = one
    return packed


def chosen(at, values):
    out = jnp.int32(values[3])
    for k in range(3):
        out = jnp.where(at == k, jnp.int32(values[k]), out)
    return out


SLOTS_OF = (
    (((4, 0, 1), (1, 2, 3))),
    (((0, 4, 1), (4, 2, 3))),
    (((0, 1, 4), (2, 4, 3))),
    (((0, 1, 2), (2, 3, 4))),
)


def dot(a, b, dims=((1,), (0,))):
    return lax.dot_general(a, b, (dims, ((), ())), preferred_element_type=F32)


TOP = 2.0**15


def largest(x):
    top = jnp.abs(x).reshape(-1, x.shape[-1])
    top = jnp.max(jnp.max(top, axis=0, keepdims=True), axis=1, keepdims=True)
    return (jnp.maximum(top, 1e-25) * 1.01).astype(BF16).astype(F32)


def packed_rows(x):
    return x.reshape(-1, x.shape[-1])


def coded(x, top):
    t = packed_rows(x) * (TOP / top)
    t2 = t * t
    t4 = t2 * t2
    return (t4 * t2 * jnp.abs(t) * t).astype(BF16)


def decoded(code, top, shape):
    v = code.astype(F32)
    t = jnp.sqrt(jnp.sqrt(jnp.sqrt(jnp.abs(v)))) * (top * (1.0 / TOP))
    return jnp.where(v < 0, -t, t).reshape(shape)


def spread(top, lanes):
    return jnp.broadcast_to(top, (16, lanes)).astype(BF16)


def kernel(
    video, frames_h, tokens, weight, packed,
    vout, wout,
    sel,
    wv, vs, v3, rv, rq, hv, he, hg, sb, sg, hs, ex, er, gx, gh, gbuf, qs, qr, lm, pg, fs, ll, vg, ms, mr,
    wg, cr, a1, fo, fi, no, ni, lo, li, a2, zr,
    load, send, recv,
):
    r = lax.axis_index("row")
    c = lax.axis_index("col")
    m = lax.axis_index("mp")
    y, core = r // 2, r % 2
    z, x = c // 4, c % 4

    pairs = [
        (video, vs.at[0:288]), (packed.at[0:96], sel.at[0:96]), (tokens, gx.at[:, 0:2]),
        (tokens, gbuf.at[:, 0]), (frames_h, v3), (packed.at[96:SELECTION_ROWS], sel.at[96:SELECTION_ROWS]),
        (weight, wv),
    ]
    for s in range(4):
        pairs.append((frames_h.at[chosen(y, [f[s] for f in FRAMES_OF])], rv.at[0, s, 0:24]))
    loads = [pltpu.make_async_copy(a, b, load.at[k]) for k, (a, b) in enumerate(pairs)]
    for one in loads:
        one.start()

    pick, rim, ends = sel.at[0:16, 0:384], sel.at[16:80, 0:288], sel.at[80:96, 0:128]
    cols, side, places = sel.at[96:480], sel.at[480:496], sel.at[496:880]
    rows, rim_of = sel.at[880:1008, 0:144], sel.at[1008:1072, 0:64]
    beside, back = sel.at[1072:1200, 0:128], sel.at[1200:1584, 0:384]

    hv[...] = jnp.zeros_like(hv)
    he[...] = jnp.zeros_like(he)
    hg[...] = jnp.zeros_like(hg)
    vs[288:384, :] = jnp.zeros((96, 384), BF16)
    gx[:, 2:4] = jnp.zeros((2, 2, 32, 512), BF16)
    rv[:, :, 24:32] = jnp.zeros((4, 4, 8, 384), BF16)
    lm[4] = jnp.zeros((16, 16, 256), BF16)

    barrier = pltpu.get_barrier_semaphore()
    up, down, lef, rig = r > 0, r < 7, c > 0, c < 15
    near = [
        (up, {"row": r - 1}), (down, {"row": r + 1}), (lef, {"col": c - 1}), (rig, {"col": c + 1}),
        (up & lef, {"row": r - 1, "col": c - 1}), (up & rig, {"row": r - 1, "col": c + 1}),
        (down & lef, {"row": r + 1, "col": c - 1}), (down & rig, {"row": r + 1, "col": c + 1}),
    ]
    yp, ym = {"row": (r + 2) % 8}, {"row": (r + 6) % 8}
    xp, xm = {"col": z * 4 + (x + 1) % 4}, {"col": z * 4 + (x + 3) % 4}
    other = {"row": y * 2 + 1 - core}
    zs = [{"col": ((z + d) % 4) * 4 + x} for d in (1, 2, 3)]
    partner = {"mp": 1 - m}

    def greet(to):
        pl.semaphore_signal(barrier, inc=1, device_id=to, device_id_type=MESH)

    for to in (yp, ym, {"row": (r + 4) % 8}, xp, xm, other, *zs, partner):
        greet(to)
    for there, to in near:
        pl.when(there)(lambda to=to: greet(to))

    def one_if(p):
        return jnp.where(p, jnp.int32(1), jnp.int32(0))

    n_near = (1 + one_if(up) + one_if(down)) * (1 + one_if(lef) + one_if(rig)) - 1

    count = iter(range(N_SEMS))

    def remote(src, dst, to):
        k = next(count)
        return pltpu.make_async_remote_copy(
            src_ref=src, dst_ref=dst, send_sem=send.at[k], recv_sem=recv.at[k],
            device_id=to, device_id_type=MESH,
        )

    for k in range(3):
        loads[k].wait()
    vs[288:352, :] = dot(rim[...], vs[0:288, :]).astype(BF16)
    sb[...] = dot(pick[...], vs[...], ((1,), (1,))).astype(BF16)
    sg[...] = dot(ends[...], gx[:, 0:2].reshape(128, 512)).astype(BF16)
    loads[3].wait()
    loads[4].wait()

    pl.semaphore_wait(barrier, 10 + n_near)

    corner = (slice(None), slice(256, 384))
    halo = [
        (remote(vs.at[288:320], hv.at[0:32], {"row": r + 1}), down, up),
        (remote(vs.at[320:352], hv.at[32:64], {"row": r - 1}), up, down),
        (remote(sb, he.at[0], {"col": c + 1}), rig, lef),
        (remote(sb, he.at[1], {"col": c - 1}), lef, rig),
        (remote(sb.at[corner], he.at[2].at[corner], {"row": r + 1, "col": c + 1}), down & rig, up & lef),
        (remote(sb.at[corner], he.at[3].at[corner], {"row": r - 1, "col": c + 1}), up & rig, down & lef),
        (remote(sb.at[corner], he.at[4].at[corner], {"row": r + 1, "col": c - 1}), down & lef, up & rig),
        (remote(sb.at[corner], he.at[5].at[corner], {"row": r - 1, "col": c - 1}), up & lef, down & rig),
    ]
    for copy, sent, _ in halo:
        pl.when(sent)(lambda copy=copy: copy.start())

    def slice_of(to, s):
        return v3.at[chosen((y + to) % 4, [f[s] for f in FRAMES_OF])]

    v_far_p = [remote(slice_of(2, s), rq.at[0, s], yp) for s in (0, 1)]
    v_far_m = [remote(slice_of(2, s + 2), rq.at[1, s], ym) for s in (0, 1)]
    g_p = remote(gbuf.at[:, 0], gbuf.at[:, 1], yp)
    g_m = remote(gbuf.at[:, 0], gbuf.at[:, 2], ym)
    v_p = [remote(slice_of(1, s), rv.at[1, s, 0:24], yp) for s in range(4)]
    v_m = [remote(slice_of(3, s), rv.at[2, s, 0:24], ym) for s in range(4)]
    for one in (g_p, g_m, *v_far_p, *v_far_m, *v_p, *v_m):
        one.start()
    g_in = remote(gx.at[:, 1 - core], gx.at[:, 3 - core], other)
    g_in.start()
    token_halo = [
        (remote(sg, hg.at[0], {"col": c + 1}), rig, lef),
        (remote(sg, hg.at[1], {"col": c - 1}), lef, rig),
        (remote(sg, hg.at[2], {"row": r + 1, "col": c + 1}), down & rig, up & lef),
        (remote(sg, hg.at[3], {"row": r - 1, "col": c + 1}), up & rig, down & lef),
        (remote(sg, hg.at[4], {"row": r + 1, "col": c - 1}), down & lef, up & rig),
        (remote(sg, hg.at[5], {"row": r - 1, "col": c - 1}), up & lef, down & rig),
    ]
    for copy, sent, _ in token_halo:
        pl.when(sent)(lambda copy=copy: copy.start())

    loads[6].wait()

    @pl.loop(0, 3072 // TALL)
    def _(k):
        at = pl.ds(pl.multiple_of(k * TALL, TALL), TALL)
        out = dot(wv[at, :], gx[:, 0:2].reshape(128, 512), ((1,), (1,)))
        pg[0, at, 0:64] = out[:, 0:64]
        pg[1, at, 0:64] = pltpu.roll(out, 64, 1)[:, 0:64]

    loads[5].wait()
    for copy, _, got in halo:
        pl.when(got)(lambda copy=copy: copy.wait_recv())

    sub = lax.broadcasted_iota(jnp.int32, (16, 128), 0)
    lane = lax.broadcasted_iota(jnp.int32, (16, 128), 1)
    for n in range(3):
        tile = slice(128 * n, 128 * n + 128)

        def edge(beside_, above, below):
            out = he[beside_, :, tile].astype(F32)
            if n == 2:
                out = jnp.where(
                    lane < 32, out,
                    jnp.where(lane < 64, he[above, :, tile].astype(F32), he[below, :, tile].astype(F32)),
                )
            return out

        hs[:, tile] = jnp.where(sub < 2, edge(1, 4, 5), edge(0, 2, 3)).astype(BF16)
    rim_rows = dot(rim_of[...], hv[...]).astype(BF16)
    rim_cols = dot(hs[...], places[...]).astype(BF16)
    for at in range(4):
        ex[at, :, 0:384] = rim_rows[16 * at : 16 * at + 16]
        ex[at, :, 384:512] = rim_cols[:, 128 * at : 128 * at + 128]
    e_far = remote(ex.at[(y + 2) % 4], er.at[3], {"row": (r + 4) % 8})
    e_p = remote(ex.at[(y + 1) % 4], er.at[1], yp)
    e_m = remote(ex.at[(y + 3) % 4], er.at[2], ym)
    for one in (e_far, e_p, e_m):
        one.start()
    er[0] = ex[y]

    def unfold(*sources):
        pixels = []
        for n in sources:
            pixels += [rv[n].reshape(128, 384), er[n, :, 0:384]]
        at = dot(jnp.concatenate(pixels, axis=0), cols[...])
        for k, n in enumerate(sources):
            from_side = dot(er[n, :, 384:512], side[...], ((0,), (0,)))
            qs[0:128] = (at[144 * k : 144 * k + 128] + from_side).astype(BF16)
            qs[128:144] = at[144 * k + 128 : 144 * k + 144].astype(BF16)
            qr[n] = dot(rows[...], qs[...]).astype(BF16).reshape(2, 4, 16, 512)

    block = lax.broadcasted_iota(jnp.int32, (64, 128), 1) // 32

    def merge(half):
        for k in range(4):
            parts = [
                qr[2 * half + n // 2, n % 2, :, :, 128 * k : 128 * k + 128].astype(F32).reshape(64, 128)
                for n in range(4)
            ]
            for q in range(4):
                row = None
                for n in range(4):
                    by = ((n - q) * 32) % 128
                    part = pltpu.roll(parts[n], by, 1) if by else parts[n]
                    row = part if row is None else jnp.where(block == n, part, row)
                lm[0:4, 4 * k + q, :, 128 * half : 128 * half + 128] = row.astype(BF16).reshape(4, 16, 128)

    for k in range(7, 11):
        loads[k].wait()
    unfold(0)

    g_p.wait_recv()
    gf_p = remote(gbuf.at[0, 1], gbuf.at[0, 3], yp)
    gf_p.start()
    g_m.wait_recv()
    gf_m = remote(gbuf.at[1, 2], gbuf.at[1, 3], ym)
    gf_m.start()
    g_out = remote(gbuf.at[:, 2 - core, core], gx.at[:, 2 + core], other)
    g_sent = ((core == 0) & (y < 3)) | ((core == 1) & (y > 0))
    g_got = ((core == 0) & (y > 0)) | ((core == 1) & (y < 3))
    pl.when(g_sent)(g_out.start)

    for one in v_far_p:
        one.wait_recv()
    vf_p = remote(rq.at[0], rv.at[3, 0:2, 0:24], yp)
    vf_p.start()
    for one in v_far_m:
        one.wait_recv()
    vf_m = remote(rq.at[1], rv.at[3, 2:4, 0:24], ym)
    vf_m.start()

    g_in.wait_recv()
    pl.when(g_got)(g_out.wait_recv)
    for copy, _, got in token_halo:
        pl.when(got)(lambda copy=copy: copy.wait_recv())

    gh[0:128] = gx[:, 2:4].reshape(128, 512)
    gh[128:256] = dot(beside[...], hg[...].reshape(128, 512)).astype(BF16)

    @pl.loop(0, 3072 // TALL)
    def _(k):
        at = pl.ds(pl.multiple_of(k * TALL, TALL), TALL)
        out = dot(wv[at, :], gh[...], ((1,), (1,)))
        pg[0, at, 64:128] = pltpu.roll(out[:, 0:128], 64, 1)[:, 64:128]
        pg[1, at, 64:128] = out[:, 64:128]
        pg[2, at, :] = out[:, 128:256]

    for one in (*v_p, *v_m, e_p, e_m):
        one.wait_recv()
    unfold(1, 2)
    merge(0)

    def summed(early, late):
        out = []
        for ch in range(0, 12, 4):
            out += [
                early[ch + 1], early[ch + 2] + late[ch], early[ch + 3] + late[ch + 1], late[ch + 2],
            ]
        return jnp.stack(out)

    def rows_of(n, e):
        return pg[n, pl.ds(e, 192, stride=16), :].reshape(12, 16, 128)

    def frames(e):
        return summed(rows_of(0, e), rows_of(1, e))

    def frames_beside(e):
        both = rows_of(2, e)
        return summed(both, pltpu.roll(both, 16 if e < 8 else 112, 2))

    j = lax.broadcasted_iota(jnp.int32, (12, 16, 128), 2) % 32
    sub = lax.broadcasted_iota(jnp.int32, (12, 8, 128), 1)
    wrap = {0: (14, 0, 1), 1: (15, 0, 1), 10: (0, 31, 127), 11: (1, 31, 127)}
    for e in range(12):
        cell = frames(e + 2)
        if e in wrap:
            far, at, by = wrap[e]
            cell = cell + jnp.where(j == at, frames_beside(far), pltpu.roll(frames(far), by, 2))
        low, high = cell[:, 0:8], cell[:, 8:16]
        to_low = pltpu.roll(pltpu.roll(high, 32, 2), 4, 1)
        to_high = pltpu.roll(pltpu.roll(low, 96, 2), 4, 1)
        fs[e, :, 0:8] = low + jnp.where((sub == 2) | (sub == 3), to_low, 0.0)
        fs[e, :, 8:16] = high + jnp.where((sub == 4) | (sub == 5), to_high, 0.0)
    for one in (vf_p, vf_m, e_far, gf_p, gf_m):
        one.wait_recv()

    unfold(3)
    merge(1)

    give = []
    for p in range(PIECES):
        for ca in range(3):
            total = None
            for t in range(2):
                at = chosen(y, [s[t][ca] for s in SLOTS_OF])
                right = gbuf[t, :, :, :, 128 * WIDE * p : 128 * WIDE * (p + 1)].reshape(256, 128 * WIDE)
                part = dot(lm[at].reshape(256, 256), right)
                total = part if total is None else total + part
            for e in range(16):
                for n in range(WIDE):
                    wg[WIDE * p + n, pl.ds(ca * 256 + e, 16, stride=16), :] = (
                        total[16 * e : 16 * e + 16, 128 * n : 128 * n + 128]
                    )
        tiles = slice(WIDE * p, WIDE * p + WIDE)
        give.append(remote(wg.at[tiles, pl.ds((1 - core) * 384, 384)], cr.at[tiles], other))
        give[p].start()

    block = lax.broadcasted_iota(jnp.int32, (192, 128), 1) // 32
    for i in range(2):
        for k in range(3):
            row = None
            for q in range(4):
                part = fs[4 * k + q].reshape(192, 128)
                by = ((q - i) * 32) % 128
                if by:
                    part = pltpu.roll(part, by, 1)
                row = part if row is None else jnp.where(block == q, part, row)
            upper = row.astype(BF16)
            ll[192 * i : 192 * i + 192, 128 * k : 128 * k + 128] = upper
            ll[384 + 192 * i : 576 + 192 * i, 128 * k : 128 * k + 128] = (row - upper.astype(F32)).astype(BF16)
    pixels = dot(ll[...], back[...])
    pixels = (pixels[0:384] + pixels[384:768]).reshape(2, 12, 16, 384)
    for i in range(2):
        for cf in range(12):
            ch, f = cf // 4, cf % 4
            vg[f // 2, ch * 2 + f % 2, 12 * i : 12 * i + 12, :] = pixels[i, cf, 2:14, :]
    top = largest(vg[1 - m])
    ms[0:16] = spread(top, 384)
    ms[16:160] = coded(vg[1 - m], top)
    v_x = remote(ms, mr, partner)
    v_x.start()

    x1, x2, x3 = (x + 1) % 4, (x + 2) % 4, (x + 3) % 4
    far, near, last, tops = [], [], [], []
    halves = (slice(0, 2), slice(2, 4))
    ring = (xp, xm)
    beyond = (x1, x3)
    block = (WIDE, 2, 24, 128)
    for p in range(PIECES):
        tiles = slice(WIDE * p, WIDE * p + WIDE)
        give[p].wait_recv()
        for n in range(WIDE * p, WIDE * p + WIDE):
            for k in range(16):
                a1[n, k // 4, k % 4] = wg[n, pl.ds(core * 384 + 24 * k, 24), :] + cr[n, 24 * k : 24 * k + 24, :]
        tops.append(largest(a1[tiles]))
        for d in range(2):
            fo[d, p, 0:16] = spread(tops[p], 128)
            fo[d, p, 16:] = coded(a1[tiles, halves[d], x2], tops[p])
            far.append(remote(fo.at[d, p], fi.at[d, p], ring[d]))
            far[-1].start()
    for p in range(PIECES):
        tiles = slice(WIDE * p, WIDE * p + WIDE)
        for d in range(2):
            no[d, p] = coded(a1[tiles, halves[1 - d], beyond[d]], tops[p])
            near.append(remote(no.at[d, p], ni.at[d, p], ring[d]))
            near[-1].start()

    for p in range(PIECES):
        tiles = slice(WIDE * p, WIDE * p + WIDE)
        for d in range(2):
            far[2 * p + d].wait_recv()
            top = fi[d, p, 0:16].astype(F32)[0:1]
            total = a1[tiles, halves[d], beyond[d]] + decoded(fi[d, p, 16:], top, block)
            top = ((top[:, 0:1] + tops[p]) * 1.01).astype(BF16).astype(F32)
            lo[d, p, 0:16] = spread(top, 128)
            lo[d, p, 16:] = coded(total, top)
            last.append(remote(lo.at[d, p], li.at[d, p], ring[d]))
            last[-1].start()

    z_out = []
    for p in range(PIECES):
        tiles = slice(WIDE * p, WIDE * p + WIDE)
        for d in range(2):
            near[2 * p + d].wait_recv()
            top = fi[d, p, 0:16].astype(F32)[0:1]
            a1[tiles, halves[1 - d], x] = a1[tiles, halves[1 - d], x] + decoded(ni[d, p], top, block)
        for d in range(2):
            last[2 * p + d].wait_recv()
            top = li[d, p, 0:16].astype(F32)[0:1]
            a2[tiles, halves[d]] = a1[tiles, halves[d], x] + decoded(li[d, p, 16:], top, block)
        z_out.append([remote(a2.at[tiles, (z + d + 1) % 4], zr.at[d, tiles], zs[d]) for d in (2, 1, 0)])
        for one in z_out[p]:
            one.start()

    v_x.wait_recv()
    vg[m] = vg[m] + decoded(mr[16:160], mr[0:16].astype(F32)[0:1], (6, 24, 384))
    v_out = pltpu.make_async_copy(vg.at[m], vout, load.at[11])
    v_out.start()

    for p in range(PIECES):
        for one in z_out[p]:
            one.wait_recv()
        for n in range(WIDE * p, WIDE * p + WIDE):
            wout[:, 128 * n : 128 * n + 128] = (a2[n, z] + zr[0, n] + (zr[1, n] + zr[2, n])) * (1.0 / 128.0)

    v_out.wait()
    for copy, sent, _ in halo + token_halo:
        pl.when(sent)(lambda copy=copy: copy.wait_send())
    pl.when(g_sent)(g_out.wait_send)
    for one in (
        g_p, g_m, g_in, gf_p, gf_m, *v_far_p, *v_far_m, *v_p, *v_m, vf_p, vf_m, e_p, e_m, e_far, v_x,
        *give, *far, *near, *last, *sum(z_out, []),
    ):
        one.wait_send()


def shards(video, grad_tokens, weight):
    packed = jnp.asarray(selections(), BF16)
    anywhere = pl.BlockSpec(memory_space=pltpu.HBM)
    in_vmem = pl.BlockSpec(memory_space=pltpu.VMEM)

    def v(*shape, kind=F32):
        return pltpu.VMEM(shape, kind)

    def b(*shape):
        return pltpu.VMEM(shape, BF16)

    video_grad, weight_grad = pl.pallas_call(
        kernel,
        out_shape=(
            jax.ShapeDtypeStruct((6, 24, 384), F32),
            jax.ShapeDtypeStruct((24, 512), F32),
        ),
        in_specs=[anywhere] * 5,
        out_specs=(pl.BlockSpec(memory_space=pl.ANY), in_vmem),
        scratch_shapes=[
            b(SELECTION_ROWS, 512),
            b(3072, 512), b(384, 384), b(12, 24, 384), b(4, 4, 32, 384), b(2, 2, 24, 384), b(64, 384),
            b(6, 16, 384), b(8, 16, 512), b(16, 384), b(16, 512), b(16, 384), b(4, 16, 512), b(4, 16, 512),
            b(2, 4, 32, 512), b(256, 512), b(2, 4, 2, 32, 512), b(144, 512),
            b(4, 2, 4, 16, 512), b(5, 16, 16, 256),
            v(3, 3072, 128), v(12, 12, 16, 128), b(768, 384), v(2, 6, 24, 384), b(160, 384), b(160, 384),
            v(4, 768, 128), v(4, 384, 128), v(4, 4, 4, 24, 128),
            *[b(2, PIECES, rows, 128) for rows in (CODED + 16, CODED + 16, CODED, CODED, CODED + 16, CODED + 16)],
            v(4, 4, 24, 128),
            v(3, 4, 24, 128),
            pltpu.SemaphoreType.DMA((12,)),
            pltpu.SemaphoreType.DMA((N_SEMS,)),
            pltpu.SemaphoreType.DMA((N_SEMS,)),
        ],
        compiler_params=pltpu.CompilerParams(
            collective_id=0, has_side_effects=True, vmem_limit_bytes=VMEM_BYTES
        ),
        name="tubelet_backward",
    )(video.reshape(288, 384), video.reshape(12, 24, 384), grad_tokens, weight, packed)
    return video_grad.reshape(3, 2, 24, 384), weight_grad


def solution(mesh):
    return jax.shard_map(
        shards,
        mesh=mesh,
        in_specs=(P(None, None, "row", "col"), P(None, "row", "col", "mp"), P(None, "mp")),
        out_specs=(P(None, "mp", "row", "col"), P(("row", "col"), "mp")),
        check_vma=False,
    )
```

```python
import jax
import jax.numpy as jnp
import numpy as np
from jax import lax
from jax.experimental import pallas as pl
from jax.experimental.pallas import tpu as pltpu
from jax.sharding import PartitionSpec as P

MESH = pl.DeviceIdType.MESH
F32 = jnp.float32
BF16 = jnp.bfloat16
N_SEMS = 80
TALL = 1536
FRAMES_OF = ((0, 1, 2, 3), (2, 4, 5, 6), (5, 6, 7, 9), (8, 9, 10, 11))
VMEM_BYTES = 56500000
PIECES = 2
WIDE = 4 // PIECES
CODED = WIDE * 48
SELECTION_AT = (0, 16, 80, 96, 480, 496, 880, 1008, 1072, 1200)
SELECTION_ROWS = 1584


def selections():
    cols = np.zeros((384, 512), np.float32)
    for e in range(16):
        for j in range(32):
            x = 12 * j + e - 2
            if 0 <= x < 384:
                cols[x, e * 32 + j] = 1
    side = np.zeros((16, 512), np.float32)
    side[2, 0] = side[3, 32] = 1
    side[0, 14 * 32 + 31] = side[1, 15 * 32 + 31] = 1
    rim_of = np.zeros((64, 64), np.float32)
    places = np.zeros((384, 512), np.float32)
    for at in range(4):
        for s, cf in enumerate(FRAMES_OF[at]):
            for k in range(24):
                places[cf * 24 + k, at * 128 + s * 32 + k] = 1
            for k in range(4):
                far = (k // 2) * 32 + cf * 2 + k % 2
                rim_of[at * 16 + s * 4 + k, far] = 1
                places[288 + far, at * 128 + s * 32 + 24 + k] = 1
    rows = np.zeros((128, 144), np.float32)
    for i in range(2):
        for s in range(4):
            for b in range(16):
                y = 12 * i + b - 2
                k = y + 2 if y < 0 else y - 22
                rows[i * 64 + s * 16 + b, s * 32 + (y if 0 <= y < 24 else 24 + k)] = 1
                if not 0 <= y < 24:
                    rows[i * 64 + s * 16 + b, 128 + s * 4 + k] = 1
    pick = np.zeros((16, 384), np.float32)
    for k, x in enumerate((0, 1, 382, 383)):
        pick[k, x] = 1
    rim = np.zeros((64, 288), np.float32)
    for cf in range(12):
        for k in range(2):
            rim[cf * 2 + k, cf * 24 + 22 + k] = 1
            rim[32 + cf * 2 + k, cf * 24 + k] = 1
    ends = np.zeros((16, 128), np.float32)
    for ti in range(4):
        ends[ti, ti * 32] = 1
        ends[4 + ti, ti * 32 + 31] = 1
    beside = np.zeros((128, 128), np.float32)
    for t in range(2):
        for n in range(4):
            i = (0, 1, 0, 1)[n]
            left = (0, 0, 3, 2)[n]
            right = (1, 1, 5, 4)[n]
            beside[n * 32 + 16 * t, left * 16 + 4 + t * 2 + i] = 1
            beside[n * 32 + 31 - 16 * t, right * 16 + t * 2 + i] = 1
    back = np.zeros((384, 384), np.float32)
    for e in range(12):
        for j in range(32):
            back[e * 32 + j, 12 * j + e] = 1
    packed = np.zeros((SELECTION_ROWS, 512), np.float32)
    for at, one in zip(SELECTION_AT, (pick, rim, ends, cols, side, places, rows, rim_of, beside, back)):
        packed[at : at + one.shape[0], : one.shape[1]] = one
    return packed


def chosen(at, values):
    out = jnp.int32(values[3])
    for k in range(3):
        out = jnp.where(at == k, jnp.int32(values[k]), out)
    return out


SLOTS_OF = (
    (((4, 0, 1), (1, 2, 3))),
    (((0, 4, 1), (4, 2, 3))),
    (((0, 1, 4), (2, 4, 3))),
    (((0, 1, 2), (2, 3, 4))),
)


def dot(a, b, dims=((1,), (0,))):
    return lax.dot_general(a, b, (dims, ((), ())), preferred_element_type=F32)


TOP = 2.0**15


def largest(x):
    top = jnp.abs(x).reshape(-1, x.shape[-1])
    top = jnp.max(jnp.max(top, axis=0, keepdims=True), axis=1, keepdims=True)
    return (jnp.maximum(top, 1e-25) * 1.01).astype(BF16).astype(F32)


def packed_rows(x):
    return x.reshape(-1, x.shape[-1])


def coded(x, top):
    t = packed_rows(x) * (TOP / top)
    t2 = t * t
    t4 = t2 * t2
    return (t4 * t2 * jnp.abs(t) * t).astype(BF16)


def decoded(code, top, shape):
    v = code.astype(F32)
    t = jnp.sqrt(jnp.sqrt(jnp.sqrt(jnp.abs(v)))) * (top * (1.0 / TOP))
    return jnp.where(v < 0, -t, t).reshape(shape)


def spread(top, lanes):
    return jnp.broadcast_to(top, (16, lanes)).astype(BF16)


def kernel(
    video, frames_h, tokens, weight, packed,
    vout, wout,
    sel,
    wv, vs, v3, rv, rq, hv, he, hg, sb, sg, hs, ex, er, gx, gh, gbuf, qs, qr, lm, pg, fs, ll, vg, ms, mr,
    wg, cr, a1, fo, fi, no, ni, lo, li, a2, zr,
    load, send, recv,
):
    r = lax.axis_index("row")
    c = lax.axis_index("col")
    m = lax.axis_index("mp")
    y, core = r // 2, r % 2
    z, x = c // 4, c % 4

    pairs = [
        (video, vs.at[0:288]), (packed.at[0:96], sel.at[0:96]), (tokens, gx.at[:, 0:2]),
        (tokens, gbuf.at[:, 0]), (frames_h, v3), (packed.at[96:SELECTION_ROWS], sel.at[96:SELECTION_ROWS]),
        (weight, wv),
    ]
    for s in range(4):
        pairs.append((frames_h.at[chosen(y, [f[s] for f in FRAMES_OF])], rv.at[0, s, 0:24]))
    loads = [pltpu.make_async_copy(a, b, load.at[k]) for k, (a, b) in enumerate(pairs)]
    for one in loads:
        one.start()

    pick, rim, ends = sel.at[0:16, 0:384], sel.at[16:80, 0:288], sel.at[80:96, 0:128]
    cols, side, places = sel.at[96:480], sel.at[480:496], sel.at[496:880]
    rows, rim_of = sel.at[880:1008, 0:144], sel.at[1008:1072, 0:64]
    beside, back = sel.at[1072:1200, 0:128], sel.at[1200:1584, 0:384]

    hv[...] = jnp.zeros_like(hv)
    he[...] = jnp.zeros_like(he)
    hg[...] = jnp.zeros_like(hg)
    vs[288:384, :] = jnp.zeros((96, 384), BF16)
    gx[:, 2:4] = jnp.zeros((2, 2, 32, 512), BF16)
    rv[:, :, 24:32] = jnp.zeros((4, 4, 8, 384), BF16)
    lm[4] = jnp.zeros((16, 16, 256), BF16)

    barrier = pltpu.get_barrier_semaphore()
    up, down, lef, rig = r > 0, r < 7, c > 0, c < 15
    near = [
        (up, {"row": r - 1}), (down, {"row": r + 1}), (lef, {"col": c - 1}), (rig, {"col": c + 1}),
        (up & lef, {"row": r - 1, "col": c - 1}), (up & rig, {"row": r - 1, "col": c + 1}),
        (down & lef, {"row": r + 1, "col": c - 1}), (down & rig, {"row": r + 1, "col": c + 1}),
    ]
    yp, ym = {"row": (r + 2) % 8}, {"row": (r + 6) % 8}
    xp, xm = {"col": z * 4 + (x + 1) % 4}, {"col": z * 4 + (x + 3) % 4}
    other = {"row": y * 2 + 1 - core}
    zs = [{"col": ((z + d) % 4) * 4 + x} for d in (1, 2, 3)]
    partner = {"mp": 1 - m}

    def greet(to):
        pl.semaphore_signal(barrier, inc=1, device_id=to, device_id_type=MESH)

    for to in (yp, ym, {"row": (r + 4) % 8}, xp, xm, other, *zs, partner):
        greet(to)
    for there, to in near:
        pl.when(there)(lambda to=to: greet(to))

    def one_if(p):
        return jnp.where(p, jnp.int32(1), jnp.int32(0))

    n_near = (1 + one_if(up) + one_if(down)) * (1 + one_if(lef) + one_if(rig)) - 1

    count = iter(range(N_SEMS))

    def remote(src, dst, to):
        k = next(count)
        return pltpu.make_async_remote_copy(
            src_ref=src, dst_ref=dst, send_sem=send.at[k], recv_sem=recv.at[k],
            device_id=to, device_id_type=MESH,
        )

    for k in range(3):
        loads[k].wait()
    vs[288:352, :] = dot(rim[...], vs[0:288, :]).astype(BF16)
    sb[...] = dot(pick[...], vs[...], ((1,), (1,))).astype(BF16)
    sg[...] = dot(ends[...], gx[:, 0:2].reshape(128, 512)).astype(BF16)
    loads[3].wait()
    loads[4].wait()

    pl.semaphore_wait(barrier, 10 + n_near)

    corner = (slice(None), slice(256, 384))
    halo = [
        (remote(vs.at[288:320], hv.at[0:32], {"row": r + 1}), down, up),
        (remote(vs.at[320:352], hv.at[32:64], {"row": r - 1}), up, down),
        (remote(sb, he.at[0], {"col": c + 1}), rig, lef),
        (remote(sb, he.at[1], {"col": c - 1}), lef, rig),
        (remote(sb.at[corner], he.at[2].at[corner], {"row": r + 1, "col": c + 1}), down & rig, up & lef),
        (remote(sb.at[corner], he.at[3].at[corner], {"row": r - 1, "col": c + 1}), up & rig, down & lef),
        (remote(sb.at[corner], he.at[4].at[corner], {"row": r + 1, "col": c - 1}), down & lef, up & rig),
        (remote(sb.at[corner], he.at[5].at[corner], {"row": r - 1, "col": c - 1}), up & lef, down & rig),
    ]
    for copy, sent, _ in halo:
        pl.when(sent)(lambda copy=copy: copy.start())

    g_sent = ((core == 1) & down) | ((core == 0) & up)
    g_got = ((core == 0) & up) | ((core == 1) & down)
    g_out = remote(gx.at[:, core], gx.at[:, 2 + core], {"row": r + 2 * core - 1})

    def slice_of(to, s):
        return v3.at[chosen((y + to) % 4, [f[s] for f in FRAMES_OF])]

    v_far_p = [remote(slice_of(2, s), rq.at[0, s], yp) for s in (0, 1)]
    v_far_m = [remote(slice_of(2, s + 2), rq.at[1, s], ym) for s in (0, 1)]
    g_p = [remote(gbuf.at[t, 0], gbuf.at[t, 1], yp) for t in (0, 1)]
    g_m = [remote(gbuf.at[t, 0], gbuf.at[t, 2], ym) for t in (1, 0)]
    v_p = [remote(slice_of(1, s), rv.at[1, s, 0:24], yp) for s in range(4)]
    v_m = [remote(slice_of(3, s), rv.at[2, s, 0:24], ym) for s in range(4)]
    for one in (g_p[0], g_m[0]):
        one.start()
    pl.when(g_sent)(g_out.start)
    for one in (*v_far_p, *v_far_m, g_p[1], g_m[1], *v_p, *v_m):
        one.start()
    g_in = remote(gx.at[:, 1 - core], gx.at[:, 3 - core], other)
    g_in.start()
    token_halo = [
        (remote(sg, hg.at[0], {"col": c + 1}), rig, lef),
        (remote(sg, hg.at[1], {"col": c - 1}), lef, rig),
        (remote(sg, hg.at[2], {"row": r + 1, "col": c + 1}), down & rig, up & lef),
        (remote(sg, hg.at[3], {"row": r - 1, "col": c + 1}), up & rig, down & lef),
        (remote(sg, hg.at[4], {"row": r + 1, "col": c - 1}), down & lef, up & rig),
        (remote(sg, hg.at[5], {"row": r - 1, "col": c - 1}), up & lef, down & rig),
    ]
    for copy, sent, _ in token_halo:
        pl.when(sent)(lambda copy=copy: copy.start())

    loads[6].wait()

    @pl.loop(0, 3072 // TALL)
    def _(k):
        at = pl.ds(pl.multiple_of(k * TALL, TALL), TALL)
        out = dot(wv[at, :], gx[:, 0:2].reshape(128, 512), ((1,), (1,)))
        pg[0, at, 0:64] = out[:, 0:64]
        pg[1, at, 0:64] = pltpu.roll(out, 64, 1)[:, 0:64]

    loads[5].wait()
    for copy, _, got in halo:
        pl.when(got)(lambda copy=copy: copy.wait_recv())

    sub = lax.broadcasted_iota(jnp.int32, (16, 128), 0)
    lane = lax.broadcasted_iota(jnp.int32, (16, 128), 1)
    for n in range(3):
        tile = slice(128 * n, 128 * n + 128)

        def edge(beside_, above, below):
            out = he[beside_, :, tile].astype(F32)
            if n == 2:
                out = jnp.where(
                    lane < 32, out,
                    jnp.where(lane < 64, he[above, :, tile].astype(F32), he[below, :, tile].astype(F32)),
                )
            return out

        hs[:, tile] = jnp.where(sub < 2, edge(1, 4, 5), edge(0, 2, 3)).astype(BF16)
    rim_rows = dot(rim_of[...], hv[...]).astype(BF16)
    rim_cols = dot(hs[...], places[...]).astype(BF16)
    for at in range(4):
        ex[at, :, 0:384] = rim_rows[16 * at : 16 * at + 16]
        ex[at, :, 384:512] = rim_cols[:, 128 * at : 128 * at + 128]
    e_far = remote(ex.at[(y + 2) % 4], er.at[3], {"row": (r + 4) % 8})
    e_p = remote(ex.at[(y + 1) % 4], er.at[1], yp)
    e_m = remote(ex.at[(y + 3) % 4], er.at[2], ym)
    for one in (e_far, e_p, e_m):
        one.start()
    er[0] = ex[y]

    def unfold(*sources):
        pixels = []
        for n in sources:
            pixels += [rv[n].reshape(128, 384), er[n, :, 0:384]]
        at = dot(jnp.concatenate(pixels, axis=0), cols[...])
        for k, n in enumerate(sources):
            from_side = dot(er[n, :, 384:512], side[...], ((0,), (0,)))
            qs[0:128] = (at[144 * k : 144 * k + 128] + from_side).astype(BF16)
            qs[128:144] = at[144 * k + 128 : 144 * k + 144].astype(BF16)
            qr[n] = dot(rows[...], qs[...]).astype(BF16).reshape(2, 4, 16, 512)

    block = lax.broadcasted_iota(jnp.int32, (64, 128), 1) // 32

    def merge(half):
        for k in range(4):
            parts = [
                qr[2 * half + n // 2, n % 2, :, :, 128 * k : 128 * k + 128].astype(F32).reshape(64, 128)
                for n in range(4)
            ]
            for q in range(4):
                row = None
                for n in range(4):
                    by = ((n - q) * 32) % 128
                    part = pltpu.roll(parts[n], by, 1) if by else parts[n]
                    row = part if row is None else jnp.where(block == n, part, row)
                lm[0:4, 4 * k + q, :, 128 * half : 128 * half + 128] = row.astype(BF16).reshape(4, 16, 128)

    for k in range(7, 11):
        loads[k].wait()
    unfold(0)

    g_in.wait_recv()
    pl.when(g_got)(g_out.wait_recv)
    for copy, _, got in token_halo:
        pl.when(got)(lambda copy=copy: copy.wait_recv())

    gh[0:128] = gx[:, 2:4].reshape(128, 512)
    gh[128:256] = dot(beside[...], hg[...].reshape(128, 512)).astype(BF16)

    @pl.loop(0, 3072 // TALL)
    def _(k):
        at = pl.ds(pl.multiple_of(k * TALL, TALL), TALL)
        out = dot(wv[at, :], gh[...], ((1,), (1,)))
        pg[0, at, 64:128] = pltpu.roll(out[:, 0:128], 64, 1)[:, 64:128]
        pg[1, at, 64:128] = out[:, 64:128]
        pg[2, at, :] = out[:, 128:256]

    g_p[0].wait_recv()
    gf_p = remote(gbuf.at[0, 1], gbuf.at[0, 3], yp)
    gf_p.start()
    g_m[0].wait_recv()
    gf_m = remote(gbuf.at[1, 2], gbuf.at[1, 3], ym)
    gf_m.start()

    for one in v_far_p:
        one.wait_recv()
    vf_p = remote(rq.at[0], rv.at[3, 0:2, 0:24], yp)
    vf_p.start()
    for one in v_far_m:
        one.wait_recv()
    vf_m = remote(rq.at[1], rv.at[3, 2:4, 0:24], ym)
    vf_m.start()

    def summed(early, late):
        out = []
        for ch in range(0, 12, 4):
            out += [
                early[ch + 1], early[ch + 2] + late[ch], early[ch + 3] + late[ch + 1], late[ch + 2],
            ]
        return jnp.stack(out)

    def rows_of(n, e):
        return pg[n, pl.ds(e, 192, stride=16), :].reshape(12, 16, 128)

    def frames(e):
        return summed(rows_of(0, e), rows_of(1, e))

    def frames_beside(e):
        both = rows_of(2, e)
        return summed(both, pltpu.roll(both, 16 if e < 8 else 112, 2))

    j = lax.broadcasted_iota(jnp.int32, (12, 16, 128), 2) % 32
    sub = lax.broadcasted_iota(jnp.int32, (12, 8, 128), 1)
    wrap = {0: (14, 0, 1), 1: (15, 0, 1), 10: (0, 31, 127), 11: (1, 31, 127)}
    for e in range(12):
        cell = frames(e + 2)
        if e in wrap:
            far, at, by = wrap[e]
            cell = cell + jnp.where(j == at, frames_beside(far), pltpu.roll(frames(far), by, 2))
        low, high = cell[:, 0:8], cell[:, 8:16]
        to_low = pltpu.roll(pltpu.roll(high, 32, 2), 4, 1)
        to_high = pltpu.roll(pltpu.roll(low, 96, 2), 4, 1)
        fs[e, :, 0:8] = low + jnp.where((sub == 2) | (sub == 3), to_low, 0.0)
        fs[e, :, 8:16] = high + jnp.where((sub == 4) | (sub == 5), to_high, 0.0)
    quarter = lax.broadcasted_iota(jnp.int32, (192, 128), 1) // 32
    for i in range(2):
        for k in range(3):
            row = None
            for q in range(4):
                part = fs[4 * k + q].reshape(192, 128)
                by = ((q - i) * 32) % 128
                if by:
                    part = pltpu.roll(part, by, 1)
                row = part if row is None else jnp.where(quarter == q, part, row)
            upper = row.astype(BF16)
            ll[192 * i : 192 * i + 192, 128 * k : 128 * k + 128] = upper
            ll[384 + 192 * i : 576 + 192 * i, 128 * k : 128 * k + 128] = (row - upper.astype(F32)).astype(BF16)
    pixels = dot(ll[...], back[...])
    pixels = (pixels[0:384] + pixels[384:768]).reshape(2, 12, 16, 384)
    for i in range(2):
        for cf in range(12):
            ch, f = cf // 4, cf % 4
            vg[f // 2, ch * 2 + f % 2, 12 * i : 12 * i + 12, :] = pixels[i, cf, 2:14, :]
    top = largest(vg[1 - m])
    ms[0:16] = spread(top, 384)
    ms[16:160] = coded(vg[1 - m], top)
    v_x = remote(ms, mr, partner)
    v_x.start()

    for one in (*v_p, *v_m, e_p, e_m):
        one.wait_recv()
    unfold(1, 2)
    merge(0)

    for one in (vf_p, vf_m, e_far, g_p[1], g_m[1], gf_p, gf_m):
        one.wait_recv()

    unfold(3)
    merge(1)

    give = []
    for p in range(PIECES):
        for ca in range(3):
            total = None
            for t in range(2):
                at = chosen(y, [s[t][ca] for s in SLOTS_OF])
                right = gbuf[t, :, :, :, 128 * WIDE * p : 128 * WIDE * (p + 1)].reshape(256, 128 * WIDE)
                part = dot(lm[at].reshape(256, 256), right)
                total = part if total is None else total + part
            for e in range(16):
                for n in range(WIDE):
                    wg[WIDE * p + n, pl.ds(ca * 256 + e, 16, stride=16), :] = (
                        total[16 * e : 16 * e + 16, 128 * n : 128 * n + 128]
                    )
        tiles = slice(WIDE * p, WIDE * p + WIDE)
        give.append(remote(wg.at[tiles, pl.ds((1 - core) * 384, 384)], cr.at[tiles], other))
        give[p].start()

    x1, x2, x3 = (x + 1) % 4, (x + 2) % 4, (x + 3) % 4
    far, near, last, tops = [], [], [], []
    halves = (slice(0, 2), slice(2, 4))
    ring = (xp, xm)
    beyond = (x1, x3)
    block = (WIDE, 2, 24, 128)
    for p in range(PIECES):
        tiles = slice(WIDE * p, WIDE * p + WIDE)
        give[p].wait_recv()
        for n in range(WIDE * p, WIDE * p + WIDE):
            for k in range(16):
                a1[n, k // 4, k % 4] = wg[n, pl.ds(core * 384 + 24 * k, 24), :] + cr[n, 24 * k : 24 * k + 24, :]
        tops.append(largest(a1[tiles]))
        for d in range(2):
            fo[d, p, 0:16] = spread(tops[p], 128)
            fo[d, p, 16:] = coded(a1[tiles, halves[d], x2], tops[p])
            far.append(remote(fo.at[d, p], fi.at[d, p], ring[d]))
            far[-1].start()
    for p in range(PIECES):
        tiles = slice(WIDE * p, WIDE * p + WIDE)
        for d in range(2):
            no[d, p] = coded(a1[tiles, halves[1 - d], beyond[d]], tops[p])
            near.append(remote(no.at[d, p], ni.at[d, p], ring[d]))
            near[-1].start()

    for p in range(PIECES):
        tiles = slice(WIDE * p, WIDE * p + WIDE)
        for d in range(2):
            far[2 * p + d].wait_recv()
            top = fi[d, p, 0:16].astype(F32)[0:1]
            total = a1[tiles, halves[d], beyond[d]] + decoded(fi[d, p, 16:], top, block)
            top = ((top[:, 0:1] + tops[p]) * 1.01).astype(BF16).astype(F32)
            lo[d, p, 0:16] = spread(top, 128)
            lo[d, p, 16:] = coded(total, top)
            last.append(remote(lo.at[d, p], li.at[d, p], ring[d]))
            last[-1].start()

    z_out = []
    for p in range(PIECES):
        tiles = slice(WIDE * p, WIDE * p + WIDE)
        for d in range(2):
            near[2 * p + d].wait_recv()
            top = fi[d, p, 0:16].astype(F32)[0:1]
            a1[tiles, halves[1 - d], x] = a1[tiles, halves[1 - d], x] + decoded(ni[d, p], top, block)
        for d in range(2):
            last[2 * p + d].wait_recv()
            top = li[d, p, 0:16].astype(F32)[0:1]
            a2[tiles, halves[d]] = a1[tiles, halves[d], x] + decoded(li[d, p, 16:], top, block)
        z_out.append([remote(a2.at[tiles, (z + d + 1) % 4], zr.at[d, tiles], zs[d]) for d in (2, 1, 0)])
        for one in z_out[p]:
            one.start()

    v_x.wait_recv()
    vg[m] = vg[m] + decoded(mr[16:160], mr[0:16].astype(F32)[0:1], (6, 24, 384))
    v_out = pltpu.make_async_copy(vg.at[m], vout, load.at[11])
    v_out.start()

    for p in range(PIECES):
        for one in z_out[p]:
            one.wait_recv()
        for n in range(WIDE * p, WIDE * p + WIDE):
            wout[:, 128 * n : 128 * n + 128] = (a2[n, z] + zr[0, n] + (zr[1, n] + zr[2, n])) * (1.0 / 128.0)

    v_out.wait()
    for copy, sent, _ in halo + token_halo:
        pl.when(sent)(lambda copy=copy: copy.wait_send())
    pl.when(g_sent)(g_out.wait_send)
    for one in (
        *g_p, *g_m, g_in, gf_p, gf_m, *v_far_p, *v_far_m, *v_p, *v_m, vf_p, vf_m, e_p, e_m, e_far, v_x,
        *give, *far, *near, *last, *sum(z_out, []),
    ):
        one.wait_send()


def shards(video, grad_tokens, weight):
    packed = jnp.asarray(selections(), BF16)
    anywhere = pl.BlockSpec(memory_space=pltpu.HBM)
    in_vmem = pl.BlockSpec(memory_space=pltpu.VMEM)

    def v(*shape, kind=F32):
        return pltpu.VMEM(shape, kind)

    def b(*shape):
        return pltpu.VMEM(shape, BF16)

    video_grad, weight_grad = pl.pallas_call(
        kernel,
        out_shape=(
            jax.ShapeDtypeStruct((6, 24, 384), F32),
            jax.ShapeDtypeStruct((24, 512), F32),
        ),
        in_specs=[anywhere] * 5,
        out_specs=(pl.BlockSpec(memory_space=pl.ANY), in_vmem),
        scratch_shapes=[
            b(SELECTION_ROWS, 512),
            b(3072, 512), b(384, 384), b(12, 24, 384), b(4, 4, 32, 384), b(2, 2, 24, 384), b(64, 384),
            b(6, 16, 384), b(8, 16, 512), b(16, 384), b(16, 512), b(16, 384), b(4, 16, 512), b(4, 16, 512),
            b(2, 4, 32, 512), b(256, 512), b(2, 4, 2, 32, 512), b(144, 512),
            b(4, 2, 4, 16, 512), b(5, 16, 16, 256),
            v(3, 3072, 128), v(12, 12, 16, 128), b(768, 384), v(2, 6, 24, 384), b(160, 384), b(160, 384),
            v(4, 768, 128), v(4, 384, 128), v(4, 4, 4, 24, 128),
            *[b(2, PIECES, rows, 128) for rows in (CODED + 16, CODED + 16, CODED, CODED, CODED + 16, CODED + 16)],
            v(4, 4, 24, 128),
            v(3, 4, 24, 128),
            pltpu.SemaphoreType.DMA((12,)),
            pltpu.SemaphoreType.DMA((N_SEMS,)),
            pltpu.SemaphoreType.DMA((N_SEMS,)),
        ],
        compiler_params=pltpu.CompilerParams(
            collective_id=0, has_side_effects=True, vmem_limit_bytes=VMEM_BYTES
        ),
        name="tubelet_backward",
    )(video.reshape(288, 384), video.reshape(12, 24, 384), grad_tokens, weight, packed)
    return video_grad.reshape(3, 2, 24, 384), weight_grad


def solution(mesh):
    return jax.shard_map(
        shards,
        mesh=mesh,
        in_specs=(P(None, None, "row", "col"), P(None, "row", "col", "mp"), P(None, "mp")),
        out_specs=(P(None, "mp", "row", "col"), P(("row", "col"), "mp")),
        check_vma=False,
    )
```

```python
import jax
import jax.numpy as jnp
import numpy as np
from jax import lax
from jax.experimental import pallas as pl
from jax.experimental.pallas import tpu as pltpu
from jax.sharding import PartitionSpec as P

MESH = pl.DeviceIdType.MESH
F32 = jnp.float32
BF16 = jnp.bfloat16
N_SEMS = 80
TALL = 1536
FRAMES_OF = ((0, 1, 2, 3), (2, 4, 5, 6), (5, 6, 7, 9), (8, 9, 10, 11))
VMEM_BYTES = 56500000
PIECES = 2
WIDE = 4 // PIECES
CODED = WIDE * 48
SELECTION_AT = (0, 16, 80, 96, 480, 496, 880, 1008, 1072, 1200)
SELECTION_ROWS = 1584


def selections():
    cols = np.zeros((384, 512), np.float32)
    for e in range(16):
        for j in range(32):
            x = 12 * j + e - 2
            if 0 <= x < 384:
                cols[x, e * 32 + j] = 1
    side = np.zeros((16, 512), np.float32)
    side[2, 0] = side[3, 32] = 1
    side[0, 14 * 32 + 31] = side[1, 15 * 32 + 31] = 1
    rim_of = np.zeros((64, 64), np.float32)
    places = np.zeros((384, 512), np.float32)
    for at in range(4):
        for s, cf in enumerate(FRAMES_OF[at]):
            for k in range(24):
                places[cf * 24 + k, at * 128 + s * 32 + k] = 1
            for k in range(4):
                far = (k // 2) * 32 + cf * 2 + k % 2
                rim_of[at * 16 + s * 4 + k, far] = 1
                places[288 + far, at * 128 + s * 32 + 24 + k] = 1
    rows = np.zeros((128, 144), np.float32)
    for i in range(2):
        for s in range(4):
            for b in range(16):
                y = 12 * i + b - 2
                k = y + 2 if y < 0 else y - 22
                rows[i * 64 + s * 16 + b, s * 32 + (y if 0 <= y < 24 else 24 + k)] = 1
                if not 0 <= y < 24:
                    rows[i * 64 + s * 16 + b, 128 + s * 4 + k] = 1
    pick = np.zeros((16, 384), np.float32)
    for k, x in enumerate((0, 1, 382, 383)):
        pick[k, x] = 1
    rim = np.zeros((64, 288), np.float32)
    for cf in range(12):
        for k in range(2):
            rim[cf * 2 + k, cf * 24 + 22 + k] = 1
            rim[32 + cf * 2 + k, cf * 24 + k] = 1
    ends = np.zeros((16, 128), np.float32)
    for ti in range(4):
        ends[ti, ti * 32] = 1
        ends[4 + ti, ti * 32 + 31] = 1
    beside = np.zeros((128, 128), np.float32)
    for t in range(2):
        for n in range(4):
            i = (0, 1, 0, 1)[n]
            left = (0, 0, 3, 2)[n]
            right = (1, 1, 5, 4)[n]
            beside[n * 32 + 16 * t, left * 16 + 4 + t * 2 + i] = 1
            beside[n * 32 + 31 - 16 * t, right * 16 + t * 2 + i] = 1
    back = np.zeros((384, 384), np.float32)
    for e in range(12):
        for j in range(32):
            back[e * 32 + j, 12 * j + e] = 1
    packed = np.zeros((SELECTION_ROWS, 512), np.float32)
    for at, one in zip(SELECTION_AT, (pick, rim, ends, cols, side, places, rows, rim_of, beside, back)):
        packed[at : at + one.shape[0], : one.shape[1]] = one
    return packed


def chosen(at, values):
    out = jnp.int32(values[3])
    for k in range(3):
        out = jnp.where(at == k, jnp.int32(values[k]), out)
    return out


SLOTS_OF = (
    (((4, 0, 1), (1, 2, 3))),
    (((0, 4, 1), (4, 2, 3))),
    (((0, 1, 4), (2, 4, 3))),
    (((0, 1, 2), (2, 3, 4))),
)


def dot(a, b, dims=((1,), (0,))):
    return lax.dot_general(a, b, (dims, ((), ())), preferred_element_type=F32)


TOP = 2.0**15


def largest(x):
    top = jnp.abs(x).reshape(-1, x.shape[-1])
    top = jnp.max(jnp.max(top, axis=0, keepdims=True), axis=1, keepdims=True)
    return (jnp.maximum(top, 1e-25) * 1.01).astype(BF16).astype(F32)


def packed_rows(x):
    return x.reshape(-1, x.shape[-1])


def coded(x, top):
    t = packed_rows(x) * (TOP / top)
    t2 = t * t
    t4 = t2 * t2
    return (t4 * t2 * jnp.abs(t) * t).astype(BF16)


def decoded(code, top, shape):
    v = code.astype(F32)
    t = jnp.sqrt(jnp.sqrt(jnp.sqrt(jnp.abs(v)))) * (top * (1.0 / TOP))
    return jnp.where(v < 0, -t, t).reshape(shape)


def spread(top, lanes):
    return jnp.broadcast_to(top, (16, lanes)).astype(BF16)


def kernel(
    video, frames_h, tokens, weight, packed,
    vout, wout,
    sel,
    wv, vs, v3, rv, rq, hv, he, hg, sb, sg, hs, ex, er, gx, gh, gbuf, qs, qr, lm, pg, fs, ll, vg, ms, mr,
    wg, cr, a1, fo, fi, no, ni, lo, li, a2, zr,
    load, send, recv,
):
    r = lax.axis_index("row")
    c = lax.axis_index("col")
    m = lax.axis_index("mp")
    y, core = r // 2, r % 2
    z, x = c // 4, c % 4

    pairs = [
        (video, vs.at[0:288]), (packed.at[0:96], sel.at[0:96]), (tokens, gx.at[:, 0:2]),
        (tokens, gbuf.at[:, 0]), (frames_h, v3), (packed.at[96:SELECTION_ROWS], sel.at[96:SELECTION_ROWS]),
        (weight, wv),
    ]
    for s in range(4):
        pairs.append((frames_h.at[chosen(y, [f[s] for f in FRAMES_OF])], rv.at[0, s, 0:24]))
    loads = [pltpu.make_async_copy(a, b, load.at[k]) for k, (a, b) in enumerate(pairs)]
    for one in loads:
        one.start()

    pick, rim, ends = sel.at[0:16, 0:384], sel.at[16:80, 0:288], sel.at[80:96, 0:128]
    cols, side, places = sel.at[96:480], sel.at[480:496], sel.at[496:880]
    rows, rim_of = sel.at[880:1008, 0:144], sel.at[1008:1072, 0:64]
    beside, back = sel.at[1072:1200, 0:128], sel.at[1200:1584, 0:384]

    hv[...] = jnp.zeros_like(hv)
    he[...] = jnp.zeros_like(he)
    hg[...] = jnp.zeros_like(hg)
    vs[288:384, :] = jnp.zeros((96, 384), BF16)
    gx[:, 2:4] = jnp.zeros((2, 2, 32, 512), BF16)
    rv[:, :, 24:32] = jnp.zeros((4, 4, 8, 384), BF16)
    lm[4] = jnp.zeros((16, 16, 256), BF16)

    barrier = pltpu.get_barrier_semaphore()
    up, down, lef, rig = r > 0, r < 7, c > 0, c < 15
    near = [
        (up, {"row": r - 1}), (down, {"row": r + 1}), (lef, {"col": c - 1}), (rig, {"col": c + 1}),
        (up & lef, {"row": r - 1, "col": c - 1}), (up & rig, {"row": r - 1, "col": c + 1}),
        (down & lef, {"row": r + 1, "col": c - 1}), (down & rig, {"row": r + 1, "col": c + 1}),
    ]
    yp, ym = {"row": (r + 2) % 8}, {"row": (r + 6) % 8}
    xp, xm = {"col": z * 4 + (x + 1) % 4}, {"col": z * 4 + (x + 3) % 4}
    other = {"row": y * 2 + 1 - core}
    zs = [{"col": ((z + d) % 4) * 4 + x} for d in (1, 2, 3)]
    partner = {"mp": 1 - m}

    def greet(to):
        pl.semaphore_signal(barrier, inc=1, device_id=to, device_id_type=MESH)

    for to in (partner, *zs[::-1]):
        greet(to)
    for there, to in near[::-1]:
        pl.when(there)(lambda to=to: greet(to))
    for to in ({"row": (r + 4) % 8}, yp, ym, xp, xm, other):
        greet(to)

    def one_if(p):
        return jnp.where(p, jnp.int32(1), jnp.int32(0))

    n_near = (1 + one_if(up) + one_if(down)) * (1 + one_if(lef) + one_if(rig)) - 1

    count = iter(range(N_SEMS))

    def remote(src, dst, to):
        k = next(count)
        return pltpu.make_async_remote_copy(
            src_ref=src, dst_ref=dst, send_sem=send.at[k], recv_sem=recv.at[k],
            device_id=to, device_id_type=MESH,
        )

    for k in range(3):
        loads[k].wait()
    vs[288:352, :] = dot(rim[...], vs[0:288, :]).astype(BF16)
    sb[...] = dot(pick[...], vs[...], ((1,), (1,))).astype(BF16)
    sg[...] = dot(ends[...], gx[:, 0:2].reshape(128, 512)).astype(BF16)
    loads[3].wait()
    loads[4].wait()

    pl.semaphore_wait(barrier, 10 + n_near)

    corner = (slice(None), slice(256, 384))
    halo = [
        (remote(vs.at[288:320], hv.at[0:32], {"row": r + 1}), down, up),
        (remote(vs.at[320:352], hv.at[32:64], {"row": r - 1}), up, down),
        (remote(sb, he.at[0], {"col": c + 1}), rig, lef),
        (remote(sb, he.at[1], {"col": c - 1}), lef, rig),
        (remote(sb.at[corner], he.at[2].at[corner], {"row": r + 1, "col": c + 1}), down & rig, up & lef),
        (remote(sb.at[corner], he.at[3].at[corner], {"row": r - 1, "col": c + 1}), up & rig, down & lef),
        (remote(sb.at[corner], he.at[4].at[corner], {"row": r + 1, "col": c - 1}), down & lef, up & rig),
        (remote(sb.at[corner], he.at[5].at[corner], {"row": r - 1, "col": c - 1}), up & lef, down & rig),
    ]
    for copy, sent, _ in halo:
        pl.when(sent)(lambda copy=copy: copy.start())

    g_sent = ((core == 1) & down) | ((core == 0) & up)
    g_got = ((core == 0) & up) | ((core == 1) & down)
    g_out = remote(gx.at[:, core], gx.at[:, 2 + core], {"row": r + 2 * core - 1})

    def slice_of(to, s):
        return v3.at[chosen((y + to) % 4, [f[s] for f in FRAMES_OF])]

    v_far_p = [remote(slice_of(2, s), rq.at[0, s], yp) for s in (0, 1)]
    v_far_m = [remote(slice_of(2, s + 2), rq.at[1, s], ym) for s in (0, 1)]
    g_p = [remote(gbuf.at[t, 0], gbuf.at[t, 1], yp) for t in (0, 1)]
    g_m = [remote(gbuf.at[t, 0], gbuf.at[t, 2], ym) for t in (1, 0)]
    v_p = [remote(slice_of(1, s), rv.at[1, s, 0:24], yp) for s in range(4)]
    v_m = [remote(slice_of(3, s), rv.at[2, s, 0:24], ym) for s in range(4)]
    for one in (g_p[0], g_m[0]):
        one.start()
    pl.when(g_sent)(g_out.start)
    for one in (*v_far_p, *v_far_m, g_p[1], g_m[1], *v_p, *v_m):
        one.start()
    g_in = remote(gx.at[:, 1 - core], gx.at[:, 3 - core], other)
    g_in.start()
    token_halo = [
        (remote(sg, hg.at[0], {"col": c + 1}), rig, lef),
        (remote(sg, hg.at[1], {"col": c - 1}), lef, rig),
        (remote(sg, hg.at[2], {"row": r + 1, "col": c + 1}), down & rig, up & lef),
        (remote(sg, hg.at[3], {"row": r - 1, "col": c + 1}), up & rig, down & lef),
        (remote(sg, hg.at[4], {"row": r + 1, "col": c - 1}), down & lef, up & rig),
        (remote(sg, hg.at[5], {"row": r - 1, "col": c - 1}), up & lef, down & rig),
    ]
    for copy, sent, _ in token_halo:
        pl.when(sent)(lambda copy=copy: copy.start())

    loads[6].wait()

    @pl.loop(0, 3072 // TALL)
    def _(k):
        at = pl.ds(pl.multiple_of(k * TALL, TALL), TALL)
        out = dot(wv[at, :], gx[:, 0:2].reshape(128, 512), ((1,), (1,)))
        pg[0, at, 0:64] = out[:, 0:64]
        pg[1, at, 0:64] = pltpu.roll(out, 64, 1)[:, 0:64]

    loads[5].wait()
    for copy, _, got in halo:
        pl.when(got)(lambda copy=copy: copy.wait_recv())

    sub = lax.broadcasted_iota(jnp.int32, (16, 128), 0)
    lane = lax.broadcasted_iota(jnp.int32, (16, 128), 1)
    for n in range(3):
        tile = slice(128 * n, 128 * n + 128)

        def edge(beside_, above, below):
            out = he[beside_, :, tile].astype(F32)
            if n == 2:
                out = jnp.where(
                    lane < 32, out,
                    jnp.where(lane < 64, he[above, :, tile].astype(F32), he[below, :, tile].astype(F32)),
                )
            return out

        hs[:, tile] = jnp.where(sub < 2, edge(1, 4, 5), edge(0, 2, 3)).astype(BF16)
    rim_rows = dot(rim_of[...], hv[...]).astype(BF16)
    rim_cols = dot(hs[...], places[...]).astype(BF16)
    for at in range(4):
        ex[at, :, 0:384] = rim_rows[16 * at : 16 * at + 16]
        ex[at, :, 384:512] = rim_cols[:, 128 * at : 128 * at + 128]
    e_far = remote(ex.at[(y + 2) % 4], er.at[3], {"row": (r + 4) % 8})
    e_p = remote(ex.at[(y + 1) % 4], er.at[1], yp)
    e_m = remote(ex.at[(y + 3) % 4], er.at[2], ym)
    for one in (e_far, e_p, e_m):
        one.start()
    er[0] = ex[y]

    def unfold(*sources):
        pixels = []
        for n in sources:
            pixels += [rv[n].reshape(128, 384), er[n, :, 0:384]]
        at = dot(jnp.concatenate(pixels, axis=0), cols[...])
        for k, n in enumerate(sources):
            from_side = dot(er[n, :, 384:512], side[...], ((0,), (0,)))
            qs[0:128] = (at[144 * k : 144 * k + 128] + from_side).astype(BF16)
            qs[128:144] = at[144 * k + 128 : 144 * k + 144].astype(BF16)
            qr[n] = dot(rows[...], qs[...]).astype(BF16).reshape(2, 4, 16, 512)

    block = lax.broadcasted_iota(jnp.int32, (64, 128), 1) // 32

    def merge(half):
        for k in range(4):
            parts = [
                qr[2 * half + n // 2, n % 2, :, :, 128 * k : 128 * k + 128].astype(F32).reshape(64, 128)
                for n in range(4)
            ]
            for q in range(4):
                row = None
                for n in range(4):
                    by = ((n - q) * 32) % 128
                    part = pltpu.roll(parts[n], by, 1) if by else parts[n]
                    row = part if row is None else jnp.where(block == n, part, row)
                lm[0:4, 4 * k + q, :, 128 * half : 128 * half + 128] = row.astype(BF16).reshape(4, 16, 128)

    for k in range(7, 11):
        loads[k].wait()
    unfold(0)

    g_in.wait_recv()
    pl.when(g_got)(g_out.wait_recv)
    for copy, _, got in token_halo:
        pl.when(got)(lambda copy=copy: copy.wait_recv())

    gh[0:128] = gx[:, 2:4].reshape(128, 512)
    gh[128:256] = dot(beside[...], hg[...].reshape(128, 512)).astype(BF16)

    @pl.loop(0, 3072 // TALL)
    def _(k):
        at = pl.ds(pl.multiple_of(k * TALL, TALL), TALL)
        out = dot(wv[at, :], gh[...], ((1,), (1,)))
        pg[0, at, 64:128] = pltpu.roll(out[:, 0:128], 64, 1)[:, 64:128]
        pg[1, at, 64:128] = out[:, 64:128]
        pg[2, at, :] = out[:, 128:256]

    g_p[0].wait_recv()
    gf_p = remote(gbuf.at[0, 1], gbuf.at[0, 3], yp)
    gf_p.start()
    g_m[0].wait_recv()
    gf_m = remote(gbuf.at[1, 2], gbuf.at[1, 3], ym)
    gf_m.start()

    for one in v_far_p:
        one.wait_recv()
    vf_p = remote(rq.at[0], rv.at[3, 0:2, 0:24], yp)
    vf_p.start()
    for one in v_far_m:
        one.wait_recv()
    vf_m = remote(rq.at[1], rv.at[3, 2:4, 0:24], ym)
    vf_m.start()

    def summed(early, late):
        out = []
        for ch in range(0, 12, 4):
            out += [
                early[ch + 1], early[ch + 2] + late[ch], early[ch + 3] + late[ch + 1], late[ch + 2],
            ]
        return jnp.stack(out)

    def rows_of(n, e):
        return pg[n, pl.ds(e, 192, stride=16), :].reshape(12, 16, 128)

    def frames(e):
        return summed(rows_of(0, e), rows_of(1, e))

    def frames_beside(e):
        both = rows_of(2, e)
        return summed(both, pltpu.roll(both, 16 if e < 8 else 112, 2))

    j = lax.broadcasted_iota(jnp.int32, (12, 16, 128), 2) % 32
    sub = lax.broadcasted_iota(jnp.int32, (12, 8, 128), 1)
    wrap = {0: (14, 0, 1), 1: (15, 0, 1), 10: (0, 31, 127), 11: (1, 31, 127)}
    for e in range(12):
        cell = frames(e + 2)
        if e in wrap:
            far, at, by = wrap[e]
            cell = cell + jnp.where(j == at, frames_beside(far), pltpu.roll(frames(far), by, 2))
        low, high = cell[:, 0:8], cell[:, 8:16]
        to_low = pltpu.roll(pltpu.roll(high, 32, 2), 4, 1)
        to_high = pltpu.roll(pltpu.roll(low, 96, 2), 4, 1)
        fs[e, :, 0:8] = low + jnp.where((sub == 2) | (sub == 3), to_low, 0.0)
        fs[e, :, 8:16] = high + jnp.where((sub == 4) | (sub == 5), to_high, 0.0)
    quarter = lax.broadcasted_iota(jnp.int32, (192, 128), 1) // 32
    for i in range(2):
        for k in range(3):
            row = None
            for q in range(4):
                part = fs[4 * k + q].reshape(192, 128)
                by = ((q - i) * 32) % 128
                if by:
                    part = pltpu.roll(part, by, 1)
                row = part if row is None else jnp.where(quarter == q, part, row)
            upper = row.astype(BF16)
            ll[192 * i : 192 * i + 192, 128 * k : 128 * k + 128] = upper
            ll[384 + 192 * i : 576 + 192 * i, 128 * k : 128 * k + 128] = (row - upper.astype(F32)).astype(BF16)
    pixels = dot(ll[...], back[...])
    pixels = (pixels[0:384] + pixels[384:768]).reshape(2, 12, 16, 384)
    for i in range(2):
        for cf in range(12):
            ch, f = cf // 4, cf % 4
            vg[f // 2, ch * 2 + f % 2, 12 * i : 12 * i + 12, :] = pixels[i, cf, 2:14, :]
    top = largest(vg[1 - m])
    ms[0:16] = spread(top, 384)
    ms[16:160] = coded(vg[1 - m], top)
    v_x = remote(ms, mr, partner)
    v_x.start()

    for one in (*v_p, *v_m, e_p, e_m):
        one.wait_recv()
    unfold(1, 2)
    merge(0)

    for one in (vf_p, vf_m, e_far, g_p[1], g_m[1], gf_p, gf_m):
        one.wait_recv()

    unfold(3)
    merge(1)

    give = []
    for p in range(PIECES):
        for ca in range(3):
            total = None
            for t in range(2):
                at = chosen(y, [s[t][ca] for s in SLOTS_OF])
                right = gbuf[t, :, :, :, 128 * WIDE * p : 128 * WIDE * (p + 1)].reshape(256, 128 * WIDE)
                part = dot(lm[at].reshape(256, 256), right)
                total = part if total is None else total + part
            for e in range(16):
                for n in range(WIDE):
                    wg[WIDE * p + n, pl.ds(ca * 256 + e, 16, stride=16), :] = (
                        total[16 * e : 16 * e + 16, 128 * n : 128 * n + 128]
                    )
        tiles = slice(WIDE * p, WIDE * p + WIDE)
        give.append(remote(wg.at[tiles, pl.ds((1 - core) * 384, 384)], cr.at[tiles], other))
        give[p].start()

    x1, x2, x3 = (x + 1) % 4, (x + 2) % 4, (x + 3) % 4
    far, near, last, tops = [], [], [], []
    halves = (slice(0, 2), slice(2, 4))
    ring = (xp, xm)
    beyond = (x1, x3)
    block = (WIDE, 2, 24, 128)
    for p in range(PIECES):
        tiles = slice(WIDE * p, WIDE * p + WIDE)
        give[p].wait_recv()
        for n in range(WIDE * p, WIDE * p + WIDE):
            for k in range(16):
                a1[n, k // 4, k % 4] = wg[n, pl.ds(core * 384 + 24 * k, 24), :] + cr[n, 24 * k : 24 * k + 24, :]
        tops.append(largest(a1[tiles]))
        for d in range(2):
            fo[d, p, 0:16] = spread(tops[p], 128)
            fo[d, p, 16:] = coded(a1[tiles, halves[d], x2], tops[p])
            far.append(remote(fo.at[d, p], fi.at[d, p], ring[d]))
            far[-1].start()
    for p in range(PIECES):
        tiles = slice(WIDE * p, WIDE * p + WIDE)
        for d in range(2):
            no[d, p] = coded(a1[tiles, halves[1 - d], beyond[d]], tops[p])
            near.append(remote(no.at[d, p], ni.at[d, p], ring[d]))
            near[-1].start()

    for p in range(PIECES):
        tiles = slice(WIDE * p, WIDE * p + WIDE)
        for d in range(2):
            far[2 * p + d].wait_recv()
            top = fi[d, p, 0:16].astype(F32)[0:1]
            total = a1[tiles, halves[d], beyond[d]] + decoded(fi[d, p, 16:], top, block)
            top = ((top[:, 0:1] + tops[p]) * 1.01).astype(BF16).astype(F32)
            lo[d, p, 0:16] = spread(top, 128)
            lo[d, p, 16:] = coded(total, top)
            last.append(remote(lo.at[d, p], li.at[d, p], ring[d]))
            last[-1].start()

    z_out = []
    for p in range(PIECES):
        tiles = slice(WIDE * p, WIDE * p + WIDE)
        for d in range(2):
            near[2 * p + d].wait_recv()
            top = fi[d, p, 0:16].astype(F32)[0:1]
            a1[tiles, halves[1 - d], x] = a1[tiles, halves[1 - d], x] + decoded(ni[d, p], top, block)
        for d in range(2):
            last[2 * p + d].wait_recv()
            top = li[d, p, 0:16].astype(F32)[0:1]
            a2[tiles, halves[d]] = a1[tiles, halves[d], x] + decoded(li[d, p, 16:], top, block)
        z_out.append([remote(a2.at[tiles, (z + d + 1) % 4], zr.at[d, tiles], zs[d]) for d in (2, 1, 0)])
        for one in z_out[p]:
            one.start()

    v_x.wait_recv()
    vg[m] = vg[m] + decoded(mr[16:160], mr[0:16].astype(F32)[0:1], (6, 24, 384))
    v_out = pltpu.make_async_copy(vg.at[m], vout, load.at[11])
    v_out.start()

    for p in range(PIECES):
        for one in z_out[p]:
            one.wait_recv()
        for n in range(WIDE * p, WIDE * p + WIDE):
            wout[:, 128 * n : 128 * n + 128] = (a2[n, z] + zr[0, n] + (zr[1, n] + zr[2, n])) * (1.0 / 128.0)

    v_out.wait()
    for copy, sent, _ in halo + token_halo:
        pl.when(sent)(lambda copy=copy: copy.wait_send())
    pl.when(g_sent)(g_out.wait_send)
    for one in (
        *g_p, *g_m, g_in, gf_p, gf_m, *v_far_p, *v_far_m, *v_p, *v_m, vf_p, vf_m, e_p, e_m, e_far, v_x,
        *give, *far, *near, *last, *sum(z_out, []),
    ):
        one.wait_send()


def put_out(video_grad, weight_grad, vout, wout, held, sem):
    parts = 3
    arrive = [
        pltpu.make_async_copy(video_grad.at[pl.ds(2 * k, 2)], held.at[pl.ds(2 * k, 2)], sem.at[k])
        for k in range(parts)
    ]
    leave = [
        pltpu.make_async_copy(held.at[pl.ds(2 * k, 2)], vout.at[pl.ds(2 * k, 2)], sem.at[parts + k])
        for k in range(parts)
    ]
    last = pltpu.make_async_copy(weight_grad, wout, sem.at[2 * parts])
    for one in arrive:
        one.start()
    last.start()
    for a, b in zip(arrive, leave):
        a.wait()
        b.start()
    for one in leave:
        one.wait()
    last.wait()


def shards(video, grad_tokens, weight):
    packed = jnp.asarray(selections(), BF16)
    anywhere = pl.BlockSpec(memory_space=pltpu.HBM)
    in_vmem = pl.BlockSpec(memory_space=pltpu.VMEM)

    def v(*shape, kind=F32):
        return pltpu.VMEM(shape, kind)

    def b(*shape):
        return pltpu.VMEM(shape, BF16)

    video_grad, weight_grad = pl.pallas_call(
        kernel,
        out_shape=(
            jax.ShapeDtypeStruct((6, 24, 384), F32),
            jax.ShapeDtypeStruct((24, 512), F32),
        ),
        in_specs=[anywhere] * 5,
        out_specs=(pl.BlockSpec(memory_space=pl.ANY), in_vmem),
        scratch_shapes=[
            b(SELECTION_ROWS, 512),
            b(3072, 512), b(384, 384), b(12, 24, 384), b(4, 4, 32, 384), b(2, 2, 24, 384), b(64, 384),
            b(6, 16, 384), b(8, 16, 512), b(16, 384), b(16, 512), b(16, 384), b(4, 16, 512), b(4, 16, 512),
            b(2, 4, 32, 512), b(256, 512), b(2, 4, 2, 32, 512), b(144, 512),
            b(4, 2, 4, 16, 512), b(5, 16, 16, 256),
            v(3, 3072, 128), v(12, 12, 16, 128), b(768, 384), v(2, 6, 24, 384), b(160, 384), b(160, 384),
            v(4, 768, 128), v(4, 384, 128), v(4, 4, 4, 24, 128),
            *[b(2, PIECES, rows, 128) for rows in (CODED + 16, CODED + 16, CODED, CODED, CODED + 16, CODED + 16)],
            v(4, 4, 24, 128),
            v(3, 4, 24, 128),
            pltpu.SemaphoreType.DMA((12,)),
            pltpu.SemaphoreType.DMA((N_SEMS,)),
            pltpu.SemaphoreType.DMA((N_SEMS,)),
        ],
        compiler_params=pltpu.CompilerParams(
            collective_id=0, has_side_effects=True, vmem_limit_bytes=VMEM_BYTES
        ),
        name="tubelet_backward",
    )(video.reshape(288, 384), video.reshape(12, 24, 384), grad_tokens, weight, packed)
    video_grad, weight_grad = pl.pallas_call(
        put_out,
        out_shape=(
            jax.ShapeDtypeStruct((6, 24, 384), F32),
            jax.ShapeDtypeStruct((24, 512), F32),
        ),
        in_specs=[anywhere, in_vmem],
        out_specs=(anywhere, anywhere),
        scratch_shapes=[v(6, 24, 384), pltpu.SemaphoreType.DMA((7,))],
        compiler_params=pltpu.CompilerParams(vmem_limit_bytes=VMEM_BYTES),
        name="put_out",
    )(video_grad, weight_grad)
    return video_grad.reshape(3, 2, 24, 384), weight_grad


def solution(mesh):
    return jax.shard_map(
        shards,
        mesh=mesh,
        in_specs=(P(None, None, "row", "col"), P(None, "row", "col", "mp"), P(None, "mp")),
        out_specs=(P(None, "mp", "row", "col"), P(("row", "col"), "mp")),
        check_vma=False,
    )
```

```python
import jax
import jax.numpy as jnp
import numpy as np
from jax import lax
from jax.experimental import pallas as pl
from jax.experimental.pallas import tpu as pltpu
from jax.sharding import PartitionSpec as P

MESH = pl.DeviceIdType.MESH
F32 = jnp.float32
BF16 = jnp.bfloat16
N_SEMS = 80
TALL = 1536
FRAMES_OF = ((0, 1, 2, 3), (2, 4, 5, 6), (5, 6, 7, 9), (8, 9, 10, 11))
VMEM_BYTES = 56500000
PIECES = 2
WIDE = 4 // PIECES
CODED = WIDE * 48
SELECTION_AT = (0, 16, 80, 96, 480, 496, 880, 1008, 1072, 1200)
SELECTION_ROWS = 1584


def selections():
    cols = np.zeros((384, 512), np.float32)
    for e in range(16):
        for j in range(32):
            x = 12 * j + e - 2
            if 0 <= x < 384:
                cols[x, e * 32 + j] = 1
    side = np.zeros((16, 512), np.float32)
    side[2, 0] = side[3, 32] = 1
    side[0, 14 * 32 + 31] = side[1, 15 * 32 + 31] = 1
    rim_of = np.zeros((64, 64), np.float32)
    places = np.zeros((384, 512), np.float32)
    for at in range(4):
        for s, cf in enumerate(FRAMES_OF[at]):
            for k in range(24):
                places[cf * 24 + k, at * 128 + s * 32 + k] = 1
            for k in range(4):
                far = (k // 2) * 32 + cf * 2 + k % 2
                rim_of[at * 16 + s * 4 + k, far] = 1
                places[288 + far, at * 128 + s * 32 + 24 + k] = 1
    rows = np.zeros((128, 144), np.float32)
    for i in range(2):
        for s in range(4):
            for b in range(16):
                y = 12 * i + b - 2
                k = y + 2 if y < 0 else y - 22
                rows[i * 64 + s * 16 + b, s * 32 + (y if 0 <= y < 24 else 24 + k)] = 1
                if not 0 <= y < 24:
                    rows[i * 64 + s * 16 + b, 128 + s * 4 + k] = 1
    pick = np.zeros((16, 384), np.float32)
    for k, x in enumerate((0, 1, 382, 383)):
        pick[k, x] = 1
    rim = np.zeros((64, 288), np.float32)
    for cf in range(12):
        for k in range(2):
            rim[cf * 2 + k, cf * 24 + 22 + k] = 1
            rim[32 + cf * 2 + k, cf * 24 + k] = 1
    ends = np.zeros((16, 128), np.float32)
    for ti in range(4):
        ends[ti, ti * 32] = 1
        ends[4 + ti, ti * 32 + 31] = 1
    beside = np.zeros((128, 128), np.float32)
    for t in range(2):
        for n in range(4):
            i = (0, 1, 0, 1)[n]
            left = (0, 0, 3, 2)[n]
            right = (1, 1, 5, 4)[n]
            beside[n * 32 + 16 * t, left * 16 + 4 + t * 2 + i] = 1
            beside[n * 32 + 31 - 16 * t, right * 16 + t * 2 + i] = 1
    back = np.zeros((384, 384), np.float32)
    for e in range(12):
        for j in range(32):
            back[e * 32 + j, 12 * j + e] = 1
    packed = np.zeros((SELECTION_ROWS, 512), np.float32)
    for at, one in zip(SELECTION_AT, (pick, rim, ends, cols, side, places, rows, rim_of, beside, back)):
        packed[at : at + one.shape[0], : one.shape[1]] = one
    return packed


def chosen(at, values):
    out = jnp.int32(values[3])
    for k in range(3):
        out = jnp.where(at == k, jnp.int32(values[k]), out)
    return out


SLOTS_OF = (
    (((4, 0, 1), (1, 2, 3))),
    (((0, 4, 1), (4, 2, 3))),
    (((0, 1, 4), (2, 4, 3))),
    (((0, 1, 2), (2, 3, 4))),
)


def dot(a, b, dims=((1,), (0,))):
    return lax.dot_general(a, b, (dims, ((), ())), preferred_element_type=F32)


TOP = 2.0**15


def largest(x):
    top = jnp.abs(x).reshape(-1, x.shape[-1])
    top = jnp.max(jnp.max(top, axis=0, keepdims=True), axis=1, keepdims=True)
    return (jnp.maximum(top, 1e-25) * 1.01).astype(BF16).astype(F32)


def packed_rows(x):
    return x.reshape(-1, x.shape[-1])


def coded(x, top):
    t = packed_rows(x) * (TOP / top)
    t2 = t * t
    t4 = t2 * t2
    return (t4 * t2 * jnp.abs(t) * t).astype(BF16)


def decoded(code, top, shape):
    v = code.astype(F32)
    t = jnp.sqrt(jnp.sqrt(jnp.sqrt(jnp.abs(v)))) * (top * (1.0 / TOP))
    return jnp.where(v < 0, -t, t).reshape(shape)


def spread(top, lanes):
    return jnp.broadcast_to(top, (16, lanes)).astype(BF16)


def kernel(
    video, frames_h, tokens, weight, packed,
    vout, wout,
    sel,
    wv, vs, v3, rv, rq, hv, he, hg, sb, sg, hs, ex, er, gx, gh, gbuf, qs, qr, lm, pg, fs, ll, vg, ms, mr,
    wg, cr, a1, fo, fi, no, ni, lo, li, a2, zr,
    load, send, recv,
):
    r = lax.axis_index("row")
    c = lax.axis_index("col")
    m = lax.axis_index("mp")
    y, core = r // 2, r % 2
    z, x = c // 4, c % 4

    pairs = [
        (video, vs.at[0:288]), (packed.at[0:96], sel.at[0:96]), (tokens, gx.at[:, 0:2]),
        (tokens, gbuf.at[:, 0]), (frames_h, v3), (packed.at[96:SELECTION_ROWS], sel.at[96:SELECTION_ROWS]),
        (weight, wv),
    ]
    for s in range(4):
        pairs.append((frames_h.at[chosen(y, [f[s] for f in FRAMES_OF])], rv.at[0, s, 0:24]))
    loads = [pltpu.make_async_copy(a, b, load.at[k]) for k, (a, b) in enumerate(pairs)]
    for one in loads:
        one.start()

    pick, rim, ends = sel.at[0:16, 0:384], sel.at[16:80, 0:288], sel.at[80:96, 0:128]
    cols, side, places = sel.at[96:480], sel.at[480:496], sel.at[496:880]
    rows, rim_of = sel.at[880:1008, 0:144], sel.at[1008:1072, 0:64]
    beside, back = sel.at[1072:1200, 0:128], sel.at[1200:1584, 0:384]

    hv[...] = jnp.zeros_like(hv)
    he[...] = jnp.zeros_like(he)
    hg[...] = jnp.zeros_like(hg)
    vs[288:384, :] = jnp.zeros((96, 384), BF16)
    gx[:, 2:4] = jnp.zeros((2, 2, 32, 512), BF16)
    rv[:, :, 24:32] = jnp.zeros((4, 4, 8, 384), BF16)
    lm[4] = jnp.zeros((16, 16, 256), BF16)

    barrier = pltpu.get_barrier_semaphore()
    up, down, lef, rig = r > 0, r < 7, c > 0, c < 15
    near = [
        (up, {"row": r - 1}), (down, {"row": r + 1}), (lef, {"col": c - 1}), (rig, {"col": c + 1}),
        (up & lef, {"row": r - 1, "col": c - 1}), (up & rig, {"row": r - 1, "col": c + 1}),
        (down & lef, {"row": r + 1, "col": c - 1}), (down & rig, {"row": r + 1, "col": c + 1}),
    ]
    yp, ym = {"row": (r + 2) % 8}, {"row": (r + 6) % 8}
    xp, xm = {"col": z * 4 + (x + 1) % 4}, {"col": z * 4 + (x + 3) % 4}
    other = {"row": y * 2 + 1 - core}
    zs = [{"col": ((z + d) % 4) * 4 + x} for d in (1, 2, 3)]
    partner = {"mp": 1 - m}

    def greet(to):
        pl.semaphore_signal(barrier, inc=1, device_id=to, device_id_type=MESH)

    for to in (partner, *zs[::-1]):
        greet(to)
    for there, to in near[::-1]:
        pl.when(there)(lambda to=to: greet(to))
    for to in ({"row": (r + 4) % 8}, yp, ym, xp, xm, other):
        greet(to)

    def one_if(p):
        return jnp.where(p, jnp.int32(1), jnp.int32(0))

    n_near = (1 + one_if(up) + one_if(down)) * (1 + one_if(lef) + one_if(rig)) - 1

    count = iter(range(N_SEMS))

    def remote(src, dst, to):
        k = next(count)
        return pltpu.make_async_remote_copy(
            src_ref=src, dst_ref=dst, send_sem=send.at[k], recv_sem=recv.at[k],
            device_id=to, device_id_type=MESH,
        )

    for k in range(3):
        loads[k].wait()
    vs[288:352, :] = dot(rim[...], vs[0:288, :]).astype(BF16)
    sb[...] = dot(pick[...], vs[...], ((1,), (1,))).astype(BF16)
    sg[...] = dot(ends[...], gx[:, 0:2].reshape(128, 512)).astype(BF16)
    loads[3].wait()
    loads[4].wait()

    pl.semaphore_wait(barrier, 10 + n_near)

    corner = (slice(None), slice(256, 384))
    halo = [
        (remote(vs.at[288:320], hv.at[0:32], {"row": r + 1}), down, up),
        (remote(vs.at[320:352], hv.at[32:64], {"row": r - 1}), up, down),
        (remote(sb, he.at[0], {"col": c + 1}), rig, lef),
        (remote(sb, he.at[1], {"col": c - 1}), lef, rig),
        (remote(sb.at[corner], he.at[2].at[corner], {"row": r + 1, "col": c + 1}), down & rig, up & lef),
        (remote(sb.at[corner], he.at[3].at[corner], {"row": r - 1, "col": c + 1}), up & rig, down & lef),
        (remote(sb.at[corner], he.at[4].at[corner], {"row": r + 1, "col": c - 1}), down & lef, up & rig),
        (remote(sb.at[corner], he.at[5].at[corner], {"row": r - 1, "col": c - 1}), up & lef, down & rig),
    ]
    for copy, sent, _ in halo:
        pl.when(sent)(lambda copy=copy: copy.start())

    g_sent = ((core == 1) & down) | ((core == 0) & up)
    g_got = ((core == 0) & up) | ((core == 1) & down)
    g_out = remote(gx.at[:, core], gx.at[:, 2 + core], {"row": r + 2 * core - 1})

    def slice_of(to, s):
        return v3.at[chosen((y + to) % 4, [f[s] for f in FRAMES_OF])]

    v_far_p = [remote(slice_of(2, s), rq.at[0, s], yp) for s in (0, 1)]
    v_far_m = [remote(slice_of(2, s + 2), rq.at[1, s], ym) for s in (0, 1)]
    g_p = [remote(gbuf.at[t, 0], gbuf.at[t, 1], yp) for t in (0, 1)]
    g_m = [remote(gbuf.at[t, 0], gbuf.at[t, 2], ym) for t in (1, 0)]
    v_p = [remote(slice_of(1, s), rv.at[1, s, 0:24], yp) for s in range(4)]
    v_m = [remote(slice_of(3, s), rv.at[2, s, 0:24], ym) for s in range(4)]
    for one in (g_p[0], g_m[0]):
        one.start()
    pl.when(g_sent)(g_out.start)
    for one in (*v_far_p, *v_far_m, g_p[1], g_m[1], *v_p, *v_m):
        one.start()
    g_in = remote(gx.at[:, 1 - core], gx.at[:, 3 - core], other)
    g_in.start()
    token_halo = [
        (remote(sg, hg.at[0], {"col": c + 1}), rig, lef),
        (remote(sg, hg.at[1], {"col": c - 1}), lef, rig),
        (remote(sg, hg.at[2], {"row": r + 1, "col": c + 1}), down & rig, up & lef),
        (remote(sg, hg.at[3], {"row": r - 1, "col": c + 1}), up & rig, down & lef),
        (remote(sg, hg.at[4], {"row": r + 1, "col": c - 1}), down & lef, up & rig),
        (remote(sg, hg.at[5], {"row": r - 1, "col": c - 1}), up & lef, down & rig),
    ]
    for copy, sent, _ in token_halo:
        pl.when(sent)(lambda copy=copy: copy.start())

    loads[6].wait()

    @pl.loop(0, 3072 // TALL)
    def _(k):
        at = pl.ds(pl.multiple_of(k * TALL, TALL), TALL)
        out = dot(wv[at, :], gx[:, 0:2].reshape(128, 512), ((1,), (1,)))
        pg[0, at, 0:64] = out[:, 0:64]
        pg[1, at, 0:64] = pltpu.roll(out, 64, 1)[:, 0:64]

    loads[5].wait()
    for copy, _, got in halo:
        pl.when(got)(lambda copy=copy: copy.wait_recv())

    sub = lax.broadcasted_iota(jnp.int32, (16, 128), 0)
    lane = lax.broadcasted_iota(jnp.int32, (16, 128), 1)
    for n in range(3):
        tile = slice(128 * n, 128 * n + 128)

        def edge(beside_, above, below):
            out = he[beside_, :, tile].astype(F32)
            if n == 2:
                out = jnp.where(
                    lane < 32, out,
                    jnp.where(lane < 64, he[above, :, tile].astype(F32), he[below, :, tile].astype(F32)),
                )
            return out

        hs[:, tile] = jnp.where(sub < 2, edge(1, 4, 5), edge(0, 2, 3)).astype(BF16)
    rim_rows = dot(rim_of[...], hv[...]).astype(BF16)
    rim_cols = dot(hs[...], places[...]).astype(BF16)
    for at in range(4):
        ex[at, :, 0:384] = rim_rows[16 * at : 16 * at + 16]
        ex[at, :, 384:512] = rim_cols[:, 128 * at : 128 * at + 128]
    e_far = remote(ex.at[(y + 2) % 4], er.at[3], {"row": (r + 4) % 8})
    e_p = remote(ex.at[(y + 1) % 4], er.at[1], yp)
    e_m = remote(ex.at[(y + 3) % 4], er.at[2], ym)
    for one in (e_far, e_p, e_m):
        one.start()
    er[0] = ex[y]

    def unfold(*sources):
        pixels = []
        for n in sources:
            pixels += [rv[n].reshape(128, 384), er[n, :, 0:384]]
        at = dot(jnp.concatenate(pixels, axis=0), cols[...])
        for k, n in enumerate(sources):
            from_side = dot(er[n, :, 384:512], side[...], ((0,), (0,)))
            qs[0:128] = (at[144 * k : 144 * k + 128] + from_side).astype(BF16)
            qs[128:144] = at[144 * k + 128 : 144 * k + 144].astype(BF16)
            qr[n] = dot(rows[...], qs[...]).astype(BF16).reshape(2, 4, 16, 512)

    block = lax.broadcasted_iota(jnp.int32, (64, 128), 1) // 32

    def merge(half):
        for k in range(4):
            parts = [
                qr[2 * half + n // 2, n % 2, :, :, 128 * k : 128 * k + 128].astype(F32).reshape(64, 128)
                for n in range(4)
            ]
            for q in range(4):
                row = None
                for n in range(4):
                    by = ((n - q) * 32) % 128
                    part = pltpu.roll(parts[n], by, 1) if by else parts[n]
                    row = part if row is None else jnp.where(block == n, part, row)
                lm[0:4, 4 * k + q, :, 128 * half : 128 * half + 128] = row.astype(BF16).reshape(4, 16, 128)

    for k in range(7, 11):
        loads[k].wait()
    unfold(0)

    g_p[0].wait_recv()
    gf_p = remote(gbuf.at[0, 1], gbuf.at[0, 3], yp)
    gf_p.start()
    g_m[0].wait_recv()
    gf_m = remote(gbuf.at[1, 2], gbuf.at[1, 3], ym)
    gf_m.start()

    g_in.wait_recv()
    pl.when(g_got)(g_out.wait_recv)
    for copy, _, got in token_halo:
        pl.when(got)(lambda copy=copy: copy.wait_recv())

    gh[0:128] = gx[:, 2:4].reshape(128, 512)
    gh[128:256] = dot(beside[...], hg[...].reshape(128, 512)).astype(BF16)

    @pl.loop(0, 3072 // TALL)
    def _(k):
        at = pl.ds(pl.multiple_of(k * TALL, TALL), TALL)
        out = dot(wv[at, :], gh[...], ((1,), (1,)))
        pg[0, at, 64:128] = pltpu.roll(out[:, 0:128], 64, 1)[:, 64:128]
        pg[1, at, 64:128] = out[:, 64:128]
        pg[2, at, :] = out[:, 128:256]

    for one in v_far_p:
        one.wait_recv()
    vf_p = remote(rq.at[0], rv.at[3, 0:2, 0:24], yp)
    vf_p.start()
    for one in v_far_m:
        one.wait_recv()
    vf_m = remote(rq.at[1], rv.at[3, 2:4, 0:24], ym)
    vf_m.start()

    def summed(early, late):
        out = []
        for ch in range(0, 12, 4):
            out += [
                early[ch + 1], early[ch + 2] + late[ch], early[ch + 3] + late[ch + 1], late[ch + 2],
            ]
        return jnp.stack(out)

    def rows_of(n, e):
        return pg[n, pl.ds(e, 192, stride=16), :].reshape(12, 16, 128)

    def frames(e):
        return summed(rows_of(0, e), rows_of(1, e))

    def frames_beside(e):
        both = rows_of(2, e)
        return summed(both, pltpu.roll(both, 16 if e < 8 else 112, 2))

    j = lax.broadcasted_iota(jnp.int32, (12, 16, 128), 2) % 32
    sub = lax.broadcasted_iota(jnp.int32, (12, 8, 128), 1)
    wrap = {0: (14, 0, 1), 1: (15, 0, 1), 10: (0, 31, 127), 11: (1, 31, 127)}
    for e in range(12):
        cell = frames(e + 2)
        if e in wrap:
            far, at, by = wrap[e]
            cell = cell + jnp.where(j == at, frames_beside(far), pltpu.roll(frames(far), by, 2))
        low, high = cell[:, 0:8], cell[:, 8:16]
        to_low = pltpu.roll(pltpu.roll(high, 32, 2), 4, 1)
        to_high = pltpu.roll(pltpu.roll(low, 96, 2), 4, 1)
        fs[e, :, 0:8] = low + jnp.where((sub == 2) | (sub == 3), to_low, 0.0)
        fs[e, :, 8:16] = high + jnp.where((sub == 4) | (sub == 5), to_high, 0.0)
    quarter = lax.broadcasted_iota(jnp.int32, (192, 128), 1) // 32
    for i in range(2):
        for k in range(3):
            row = None
            for q in range(4):
                part = fs[4 * k + q].reshape(192, 128)
                by = ((q - i) * 32) % 128
                if by:
                    part = pltpu.roll(part, by, 1)
                row = part if row is None else jnp.where(quarter == q, part, row)
            upper = row.astype(BF16)
            ll[192 * i : 192 * i + 192, 128 * k : 128 * k + 128] = upper
            ll[384 + 192 * i : 576 + 192 * i, 128 * k : 128 * k + 128] = (row - upper.astype(F32)).astype(BF16)
    pixels = dot(ll[...], back[...])
    pixels = (pixels[0:384] + pixels[384:768]).reshape(2, 12, 16, 384)
    for i in range(2):
        for cf in range(12):
            ch, f = cf // 4, cf % 4
            vg[f // 2, ch * 2 + f % 2, 12 * i : 12 * i + 12, :] = pixels[i, cf, 2:14, :]
    top = largest(vg[1 - m])
    ms[0:16] = spread(top, 384)
    ms[16:160] = coded(vg[1 - m], top)
    v_x = remote(ms, mr, partner)
    v_x.start()

    for one in (*v_p, *v_m, e_p, e_m):
        one.wait_recv()
    unfold(1, 2)
    merge(0)

    for one in (vf_p, vf_m, e_far, g_p[1], g_m[1], gf_p, gf_m):
        one.wait_recv()

    unfold(3)
    merge(1)

    give = []
    for p in range(PIECES):
        for ca in range(3):
            total = None
            for t in range(2):
                at = chosen(y, [s[t][ca] for s in SLOTS_OF])
                right = gbuf[t, :, :, :, 128 * WIDE * p : 128 * WIDE * (p + 1)].reshape(256, 128 * WIDE)
                part = dot(lm[at].reshape(256, 256), right)
                total = part if total is None else total + part
            for e in range(16):
                for n in range(WIDE):
                    wg[WIDE * p + n, pl.ds(ca * 256 + e, 16, stride=16), :] = (
                        total[16 * e : 16 * e + 16, 128 * n : 128 * n + 128]
                    )
        tiles = slice(WIDE * p, WIDE * p + WIDE)
        give.append(remote(wg.at[tiles, pl.ds((1 - core) * 384, 384)], cr.at[tiles], other))
        give[p].start()

    x1, x2, x3 = (x + 1) % 4, (x + 2) % 4, (x + 3) % 4
    far, near, last, tops = [], [], [], []
    halves = (slice(0, 2), slice(2, 4))
    ring = (xp, xm)
    beyond = (x1, x3)
    block = (WIDE, 2, 24, 128)
    for p in range(PIECES):
        tiles = slice(WIDE * p, WIDE * p + WIDE)
        give[p].wait_recv()
        for n in range(WIDE * p, WIDE * p + WIDE):
            for k in range(16):
                a1[n, k // 4, k % 4] = wg[n, pl.ds(core * 384 + 24 * k, 24), :] + cr[n, 24 * k : 24 * k + 24, :]
        tops.append(largest(a1[tiles]))
        for d in range(2):
            fo[d, p, 0:16] = spread(tops[p], 128)
            fo[d, p, 16:] = coded(a1[tiles, halves[d], x2], tops[p])
            far.append(remote(fo.at[d, p], fi.at[d, p], ring[d]))
            far[-1].start()
    for p in range(PIECES):
        tiles = slice(WIDE * p, WIDE * p + WIDE)
        for d in range(2):
            no[d, p] = coded(a1[tiles, halves[1 - d], beyond[d]], tops[p])
            near.append(remote(no.at[d, p], ni.at[d, p], ring[d]))
            near[-1].start()

    for p in range(PIECES):
        tiles = slice(WIDE * p, WIDE * p + WIDE)
        for d in range(2):
            far[2 * p + d].wait_recv()
            top = fi[d, p, 0:16].astype(F32)[0:1]
            total = a1[tiles, halves[d], beyond[d]] + decoded(fi[d, p, 16:], top, block)
            top = ((top[:, 0:1] + tops[p]) * 1.01).astype(BF16).astype(F32)
            lo[d, p, 0:16] = spread(top, 128)
            lo[d, p, 16:] = coded(total, top)
            last.append(remote(lo.at[d, p], li.at[d, p], ring[d]))
            last[-1].start()

    z_out = []
    for p in range(PIECES):
        tiles = slice(WIDE * p, WIDE * p + WIDE)
        for d in range(2):
            near[2 * p + d].wait_recv()
            top = fi[d, p, 0:16].astype(F32)[0:1]
            a1[tiles, halves[1 - d], x] = a1[tiles, halves[1 - d], x] + decoded(ni[d, p], top, block)
        for d in range(2):
            last[2 * p + d].wait_recv()
            top = li[d, p, 0:16].astype(F32)[0:1]
            a2[tiles, halves[d]] = a1[tiles, halves[d], x] + decoded(li[d, p, 16:], top, block)
        z_out.append([remote(a2.at[tiles, (z + d + 1) % 4], zr.at[d, tiles], zs[d]) for d in (2, 1, 0)])
        for one in z_out[p]:
            one.start()

    v_x.wait_recv()
    vg[m] = vg[m] + decoded(mr[16:160], mr[0:16].astype(F32)[0:1], (6, 24, 384))
    v_out = pltpu.make_async_copy(vg.at[m], vout, load.at[11])
    v_out.start()

    for p in range(PIECES):
        for one in z_out[p]:
            one.wait_recv()
        for n in range(WIDE * p, WIDE * p + WIDE):
            wout[:, 128 * n : 128 * n + 128] = (a2[n, z] + zr[0, n] + (zr[1, n] + zr[2, n])) * (1.0 / 128.0)

    v_out.wait()
    for copy, sent, _ in halo + token_halo:
        pl.when(sent)(lambda copy=copy: copy.wait_send())
    pl.when(g_sent)(g_out.wait_send)
    for one in (
        *g_p, *g_m, g_in, gf_p, gf_m, *v_far_p, *v_far_m, *v_p, *v_m, vf_p, vf_m, e_p, e_m, e_far, v_x,
        *give, *far, *near, *last, *sum(z_out, []),
    ):
        one.wait_send()


def put_out(video_grad, weight_grad, vout, wout, held, sem):
    parts = 3
    arrive = [
        pltpu.make_async_copy(video_grad.at[pl.ds(2 * k, 2)], held.at[pl.ds(2 * k, 2)], sem.at[k])
        for k in range(parts)
    ]
    leave = [
        pltpu.make_async_copy(held.at[pl.ds(2 * k, 2)], vout.at[pl.ds(2 * k, 2)], sem.at[parts + k])
        for k in range(parts)
    ]
    last = pltpu.make_async_copy(weight_grad, wout, sem.at[2 * parts])
    for one in arrive:
        one.start()
    last.start()
    for a, b in zip(arrive, leave):
        a.wait()
        b.start()
    for one in leave:
        one.wait()
    last.wait()


def shards(video, grad_tokens, weight):
    packed = jnp.asarray(selections(), BF16)
    anywhere = pl.BlockSpec(memory_space=pltpu.HBM)
    in_vmem = pl.BlockSpec(memory_space=pltpu.VMEM)

    def v(*shape, kind=F32):
        return pltpu.VMEM(shape, kind)

    def b(*shape):
        return pltpu.VMEM(shape, BF16)

    video_grad, weight_grad = pl.pallas_call(
        kernel,
        out_shape=(
            jax.ShapeDtypeStruct((6, 24, 384), F32),
            jax.ShapeDtypeStruct((24, 512), F32),
        ),
        in_specs=[anywhere] * 5,
        out_specs=(pl.BlockSpec(memory_space=pl.ANY), in_vmem),
        scratch_shapes=[
            b(SELECTION_ROWS, 512),
            b(3072, 512), b(384, 384), b(12, 24, 384), b(4, 4, 32, 384), b(2, 2, 24, 384), b(64, 384),
            b(6, 16, 384), b(8, 16, 512), b(16, 384), b(16, 512), b(16, 384), b(4, 16, 512), b(4, 16, 512),
            b(2, 4, 32, 512), b(256, 512), b(2, 4, 2, 32, 512), b(144, 512),
            b(4, 2, 4, 16, 512), b(5, 16, 16, 256),
            v(3, 3072, 128), v(12, 12, 16, 128), b(768, 384), v(2, 6, 24, 384), b(160, 384), b(160, 384),
            v(4, 768, 128), v(4, 384, 128), v(4, 4, 4, 24, 128),
            *[b(2, PIECES, rows, 128) for rows in (CODED + 16, CODED + 16, CODED, CODED, CODED + 16, CODED + 16)],
            v(4, 4, 24, 128),
            v(3, 4, 24, 128),
            pltpu.SemaphoreType.DMA((12,)),
            pltpu.SemaphoreType.DMA((N_SEMS,)),
            pltpu.SemaphoreType.DMA((N_SEMS,)),
        ],
        compiler_params=pltpu.CompilerParams(
            collective_id=0, has_side_effects=True, vmem_limit_bytes=VMEM_BYTES
        ),
        name="tubelet_backward",
    )(video.reshape(288, 384), video.reshape(12, 24, 384), grad_tokens, weight, packed)
    video_grad, weight_grad = pl.pallas_call(
        put_out,
        out_shape=(
            jax.ShapeDtypeStruct((6, 24, 384), F32),
            jax.ShapeDtypeStruct((24, 512), F32),
        ),
        in_specs=[anywhere, in_vmem],
        out_specs=(anywhere, anywhere),
        scratch_shapes=[v(6, 24, 384), pltpu.SemaphoreType.DMA((7,))],
        compiler_params=pltpu.CompilerParams(vmem_limit_bytes=VMEM_BYTES),
        name="put_out",
    )(video_grad, weight_grad)
    return video_grad.reshape(3, 2, 24, 384), weight_grad


def solution(mesh):
    return jax.shard_map(
        shards,
        mesh=mesh,
        in_specs=(P(None, None, "row", "col"), P(None, "row", "col", "mp"), P(None, "mp")),
        out_specs=(P(None, "mp", "row", "col"), P(("row", "col"), "mp")),
        check_vma=False,
    )
```

```python
import jax
import jax.numpy as jnp
import numpy as np
from jax import lax
from jax.experimental import pallas as pl
from jax.experimental.pallas import tpu as pltpu
from jax.sharding import PartitionSpec as P

MESH = pl.DeviceIdType.MESH
F32 = jnp.float32
BF16 = jnp.bfloat16
N_SEMS = 80
TALL = 1536
FRAMES_OF = ((0, 1, 2, 3), (2, 4, 5, 6), (5, 6, 7, 9), (8, 9, 10, 11))
VMEM_BYTES = 56500000
PIECES = 2
WIDE = 4 // PIECES
CODED = WIDE * 48
SELECTION_AT = (0, 16, 80, 96, 480, 496, 880, 1008, 1072, 1200)
SELECTION_ROWS = 1584


def selections():
    cols = np.zeros((384, 512), np.float32)
    for e in range(16):
        for j in range(32):
            x = 12 * j + e - 2
            if 0 <= x < 384:
                cols[x, e * 32 + j] = 1
    side = np.zeros((16, 512), np.float32)
    side[2, 0] = side[3, 32] = 1
    side[0, 14 * 32 + 31] = side[1, 15 * 32 + 31] = 1
    rim_of = np.zeros((64, 64), np.float32)
    places = np.zeros((384, 512), np.float32)
    for at in range(4):
        for s, cf in enumerate(FRAMES_OF[at]):
            for k in range(24):
                places[cf * 24 + k, at * 128 + s * 32 + k] = 1
            for k in range(4):
                far = (k // 2) * 32 + cf * 2 + k % 2
                rim_of[at * 16 + s * 4 + k, far] = 1
                places[288 + far, at * 128 + s * 32 + 24 + k] = 1
    rows = np.zeros((128, 144), np.float32)
    for i in range(2):
        for s in range(4):
            for b in range(16):
                y = 12 * i + b - 2
                k = y + 2 if y < 0 else y - 22
                rows[i * 64 + s * 16 + b, s * 32 + (y if 0 <= y < 24 else 24 + k)] = 1
                if not 0 <= y < 24:
                    rows[i * 64 + s * 16 + b, 128 + s * 4 + k] = 1
    pick = np.zeros((16, 384), np.float32)
    for k, x in enumerate((0, 1, 382, 383)):
        pick[k, x] = 1
    rim = np.zeros((64, 288), np.float32)
    for cf in range(12):
        for k in range(2):
            rim[cf * 2 + k, cf * 24 + 22 + k] = 1
            rim[32 + cf * 2 + k, cf * 24 + k] = 1
    ends = np.zeros((16, 128), np.float32)
    for ti in range(4):
        ends[ti, ti * 32] = 1
        ends[4 + ti, ti * 32 + 31] = 1
    beside = np.zeros((128, 128), np.float32)
    for t in range(2):
        for n in range(4):
            i = (0, 1, 0, 1)[n]
            left = (0, 0, 3, 2)[n]
            right = (1, 1, 5, 4)[n]
            beside[n * 32 + 16 * t, left * 16 + 4 + t * 2 + i] = 1
            beside[n * 32 + 31 - 16 * t, right * 16 + t * 2 + i] = 1
    back = np.zeros((384, 384), np.float32)
    for e in range(12):
        for j in range(32):
            back[e * 32 + j, 12 * j + e] = 1
    packed = np.zeros((SELECTION_ROWS, 512), np.float32)
    for at, one in zip(SELECTION_AT, (pick, rim, ends, cols, side, places, rows, rim_of, beside, back)):
        packed[at : at + one.shape[0], : one.shape[1]] = one
    return packed


def chosen(at, values):
    out = jnp.int32(values[3])
    for k in range(3):
        out = jnp.where(at == k, jnp.int32(values[k]), out)
    return out


SLOTS_OF = (
    (((4, 0, 1), (1, 2, 3))),
    (((0, 4, 1), (4, 2, 3))),
    (((0, 1, 4), (2, 4, 3))),
    (((0, 1, 2), (2, 3, 4))),
)


def dot(a, b, dims=((1,), (0,))):
    return lax.dot_general(a, b, (dims, ((), ())), preferred_element_type=F32)


TOP = 2.0**15


def largest(x):
    top = jnp.abs(x).reshape(-1, x.shape[-1])
    top = jnp.max(jnp.max(top, axis=0, keepdims=True), axis=1, keepdims=True)
    return (jnp.maximum(top, 1e-25) * 1.01).astype(BF16).astype(F32)


def packed_rows(x):
    return x.reshape(-1, x.shape[-1])


def coded(x, top):
    t = packed_rows(x) * (TOP / top)
    t2 = t * t
    t4 = t2 * t2
    return (t4 * t2 * jnp.abs(t) * t).astype(BF16)


def decoded(code, top, shape):
    v = code.astype(F32)
    t = jnp.sqrt(jnp.sqrt(jnp.sqrt(jnp.abs(v)))) * (top * (1.0 / TOP))
    return jnp.where(v < 0, -t, t).reshape(shape)


def spread(top, lanes):
    return jnp.broadcast_to(top, (16, lanes)).astype(BF16)


def kernel(
    video, frames_h, tokens, weight, packed,
    vout, wout,
    sel,
    wv, vs, v3, rv, rq, hv, he, hg, sb, sg, hs, ex, er, gx, gh, gbuf, qs, qr, lm, pg, fs, ll, vg, ms, mr,
    wg, cr, a1, fo, fi, no, ni, lo, li, a2, zr,
    load, send, recv,
):
    r = lax.axis_index("row")
    c = lax.axis_index("col")
    m = lax.axis_index("mp")
    y, core = r // 2, r % 2
    z, x = c // 4, c % 4

    pairs = [
        (video, vs.at[0:288]), (packed.at[0:96], sel.at[0:96]), (tokens, gx.at[:, 0:2]),
        (tokens, gbuf.at[:, 0]), (frames_h, v3), (packed.at[96:SELECTION_ROWS], sel.at[96:SELECTION_ROWS]),
        (weight, wv),
    ]
    for s in range(4):
        pairs.append((frames_h.at[chosen(y, [f[s] for f in FRAMES_OF])], rv.at[0, s, 0:24]))
    loads = [pltpu.make_async_copy(a, b, load.at[k]) for k, (a, b) in enumerate(pairs)]
    for one in loads:
        one.start()

    pick, rim, ends = sel.at[0:16, 0:384], sel.at[16:80, 0:288], sel.at[80:96, 0:128]
    cols, side, places = sel.at[96:480], sel.at[480:496], sel.at[496:880]
    rows, rim_of = sel.at[880:1008, 0:144], sel.at[1008:1072, 0:64]
    beside, back = sel.at[1072:1200, 0:128], sel.at[1200:1584, 0:384]

    hv[...] = jnp.zeros_like(hv)
    he[...] = jnp.zeros_like(he)
    hg[...] = jnp.zeros_like(hg)
    vs[288:384, :] = jnp.zeros((96, 384), BF16)
    gx[:, 2:4] = jnp.zeros((2, 2, 32, 512), BF16)
    rv[:, :, 24:32] = jnp.zeros((4, 4, 8, 384), BF16)
    lm[4] = jnp.zeros((16, 16, 256), BF16)

    barrier = pltpu.get_barrier_semaphore()
    up, down, lef, rig = r > 0, r < 7, c > 0, c < 15
    near = [
        (up, {"row": r - 1}), (down, {"row": r + 1}), (lef, {"col": c - 1}), (rig, {"col": c + 1}),
        (up & lef, {"row": r - 1, "col": c - 1}), (up & rig, {"row": r - 1, "col": c + 1}),
        (down & lef, {"row": r + 1, "col": c - 1}), (down & rig, {"row": r + 1, "col": c + 1}),
    ]
    yp, ym = {"row": (r + 2) % 8}, {"row": (r + 6) % 8}
    xp, xm = {"col": z * 4 + (x + 1) % 4}, {"col": z * 4 + (x + 3) % 4}
    other = {"row": y * 2 + 1 - core}
    zs = [{"col": ((z + d) % 4) * 4 + x} for d in (1, 2, 3)]
    partner = {"mp": 1 - m}

    def greet(to):
        pl.semaphore_signal(barrier, inc=1, device_id=to, device_id_type=MESH)

    for to in (partner, *zs[::-1]):
        greet(to)
    for there, to in near[::-1]:
        pl.when(there)(lambda to=to: greet(to))
    for to in ({"row": (r + 4) % 8}, yp, ym, xp, xm, other):
        greet(to)

    def one_if(p):
        return jnp.where(p, jnp.int32(1), jnp.int32(0))

    n_near = (1 + one_if(up) + one_if(down)) * (1 + one_if(lef) + one_if(rig)) - 1

    count = iter(range(N_SEMS))

    def remote(src, dst, to):
        k = next(count)
        return pltpu.make_async_remote_copy(
            src_ref=src, dst_ref=dst, send_sem=send.at[k], recv_sem=recv.at[k],
            device_id=to, device_id_type=MESH,
        )

    for k in range(3):
        loads[k].wait()
    vs[288:352, :] = dot(rim[...], vs[0:288, :]).astype(BF16)
    sb[...] = dot(pick[...], vs[...], ((1,), (1,))).astype(BF16)
    sg[...] = dot(ends[...], gx[:, 0:2].reshape(128, 512)).astype(BF16)
    loads[3].wait()
    loads[4].wait()

    pl.semaphore_wait(barrier, 10 + n_near)

    corner = (slice(None), slice(256, 384))
    halo = [
        (remote(vs.at[288:320], hv.at[0:32], {"row": r + 1}), down, up),
        (remote(vs.at[320:352], hv.at[32:64], {"row": r - 1}), up, down),
        (remote(sb, he.at[0], {"col": c + 1}), rig, lef),
        (remote(sb, he.at[1], {"col": c - 1}), lef, rig),
        (remote(sb.at[corner], he.at[2].at[corner], {"row": r + 1, "col": c + 1}), down & rig, up & lef),
        (remote(sb.at[corner], he.at[3].at[corner], {"row": r - 1, "col": c + 1}), up & rig, down & lef),
        (remote(sb.at[corner], he.at[4].at[corner], {"row": r + 1, "col": c - 1}), down & lef, up & rig),
        (remote(sb.at[corner], he.at[5].at[corner], {"row": r - 1, "col": c - 1}), up & lef, down & rig),
    ]
    for copy, sent, _ in halo:
        pl.when(sent)(lambda copy=copy: copy.start())

    g_sent = ((core == 1) & down) | ((core == 0) & up)
    g_got = ((core == 0) & up) | ((core == 1) & down)
    g_out = remote(gx.at[:, core], gx.at[:, 2 + core], {"row": r + 2 * core - 1})

    def slice_of(to, s):
        return v3.at[chosen((y + to) % 4, [f[s] for f in FRAMES_OF])]

    v_far_p = [remote(slice_of(2, s), rq.at[0, s], yp) for s in (0, 1)]
    v_far_m = [remote(slice_of(2, s + 2), rq.at[1, s], ym) for s in (0, 1)]
    g_p = [remote(gbuf.at[t, 0], gbuf.at[t, 1], yp) for t in (0, 1)]
    g_m = [remote(gbuf.at[t, 0], gbuf.at[t, 2], ym) for t in (1, 0)]
    v_p = [remote(slice_of(1, s), rv.at[1, s, 0:24], yp) for s in range(4)]
    v_m = [remote(slice_of(3, s), rv.at[2, s, 0:24], ym) for s in range(4)]
    for one in (g_p[0], g_m[0]):
        one.start()
    pl.when(g_sent)(g_out.start)
    for one in (*v_far_p, *v_far_m, g_p[1], g_m[1], *v_p, *v_m):
        one.start()
    g_in = remote(gx.at[:, 1 - core], gx.at[:, 3 - core], other)
    g_in.start()
    token_halo = [
        (remote(sg, hg.at[0], {"col": c + 1}), rig, lef),
        (remote(sg, hg.at[1], {"col": c - 1}), lef, rig),
        (remote(sg, hg.at[2], {"row": r + 1, "col": c + 1}), down & rig, up & lef),
        (remote(sg, hg.at[3], {"row": r - 1, "col": c + 1}), up & rig, down & lef),
        (remote(sg, hg.at[4], {"row": r + 1, "col": c - 1}), down & lef, up & rig),
        (remote(sg, hg.at[5], {"row": r - 1, "col": c - 1}), up & lef, down & rig),
    ]
    for copy, sent, _ in token_halo:
        pl.when(sent)(lambda copy=copy: copy.start())

    loads[6].wait()

    @pl.loop(0, 3072 // TALL)
    def _(k):
        at = pl.ds(pl.multiple_of(k * TALL, TALL), TALL)
        out = dot(wv[at, :], gx[:, 0:2].reshape(128, 512), ((1,), (1,)))
        pg[0, at, 0:64] = out[:, 0:64]
        pg[1, at, 0:64] = pltpu.roll(out, 64, 1)[:, 0:64]

    loads[5].wait()
    for copy, _, got in halo:
        pl.when(got)(lambda copy=copy: copy.wait_recv())

    sub = lax.broadcasted_iota(jnp.int32, (16, 128), 0)
    lane = lax.broadcasted_iota(jnp.int32, (16, 128), 1)
    for n in range(3):
        tile = slice(128 * n, 128 * n + 128)

        def edge(beside_, above, below):
            out = he[beside_, :, tile].astype(F32)
            if n == 2:
                out = jnp.where(
                    lane < 32, out,
                    jnp.where(lane < 64, he[above, :, tile].astype(F32), he[below, :, tile].astype(F32)),
                )
            return out

        hs[:, tile] = jnp.where(sub < 2, edge(1, 4, 5), edge(0, 2, 3)).astype(BF16)
    rim_rows = dot(rim_of[...], hv[...]).astype(BF16)
    rim_cols = dot(hs[...], places[...]).astype(BF16)
    for at in range(4):
        ex[at, :, 0:384] = rim_rows[16 * at : 16 * at + 16]
        ex[at, :, 384:512] = rim_cols[:, 128 * at : 128 * at + 128]
    e_far = remote(ex.at[(y + 2) % 4], er.at[3], {"row": (r + 4) % 8})
    e_p = remote(ex.at[(y + 1) % 4], er.at[1], yp)
    e_m = remote(ex.at[(y + 3) % 4], er.at[2], ym)
    for one in (e_far, e_p, e_m):
        one.start()
    er[0] = ex[y]

    g_p[0].wait_recv()
    gf_p = remote(gbuf.at[0, 1], gbuf.at[0, 3], yp)
    gf_p.start()
    g_m[0].wait_recv()
    gf_m = remote(gbuf.at[1, 2], gbuf.at[1, 3], ym)
    gf_m.start()

    def unfold(*sources):
        pixels = []
        for n in sources:
            pixels += [rv[n].reshape(128, 384), er[n, :, 0:384]]
        at = dot(jnp.concatenate(pixels, axis=0), cols[...])
        for k, n in enumerate(sources):
            from_side = dot(er[n, :, 384:512], side[...], ((0,), (0,)))
            qs[0:128] = (at[144 * k : 144 * k + 128] + from_side).astype(BF16)
            qs[128:144] = at[144 * k + 128 : 144 * k + 144].astype(BF16)
            qr[n] = dot(rows[...], qs[...]).astype(BF16).reshape(2, 4, 16, 512)

    block = lax.broadcasted_iota(jnp.int32, (64, 128), 1) // 32

    def merge(half):
        for k in range(4):
            parts = [
                qr[2 * half + n // 2, n % 2, :, :, 128 * k : 128 * k + 128].astype(F32).reshape(64, 128)
                for n in range(4)
            ]
            for q in range(4):
                row = None
                for n in range(4):
                    by = ((n - q) * 32) % 128
                    part = pltpu.roll(parts[n], by, 1) if by else parts[n]
                    row = part if row is None else jnp.where(block == n, part, row)
                lm[0:4, 4 * k + q, :, 128 * half : 128 * half + 128] = row.astype(BF16).reshape(4, 16, 128)

    for k in range(7, 11):
        loads[k].wait()
    unfold(0)

    g_in.wait_recv()
    pl.when(g_got)(g_out.wait_recv)
    for copy, _, got in token_halo:
        pl.when(got)(lambda copy=copy: copy.wait_recv())

    gh[0:128] = gx[:, 2:4].reshape(128, 512)
    gh[128:256] = dot(beside[...], hg[...].reshape(128, 512)).astype(BF16)

    @pl.loop(0, 3072 // TALL)
    def _(k):
        at = pl.ds(pl.multiple_of(k * TALL, TALL), TALL)
        out = dot(wv[at, :], gh[...], ((1,), (1,)))
        pg[0, at, 64:128] = pltpu.roll(out[:, 0:128], 64, 1)[:, 64:128]
        pg[1, at, 64:128] = out[:, 64:128]
        pg[2, at, :] = out[:, 128:256]

    for one in v_far_p:
        one.wait_recv()
    vf_p = remote(rq.at[0], rv.at[3, 0:2, 0:24], yp)
    vf_p.start()
    for one in v_far_m:
        one.wait_recv()
    vf_m = remote(rq.at[1], rv.at[3, 2:4, 0:24], ym)
    vf_m.start()

    def summed(early, late):
        out = []
        for ch in range(0, 12, 4):
            out += [
                early[ch + 1], early[ch + 2] + late[ch], early[ch + 3] + late[ch + 1], late[ch + 2],
            ]
        return jnp.stack(out)

    def rows_of(n, e):
        return pg[n, pl.ds(e, 192, stride=16), :].reshape(12, 16, 128)

    def frames(e):
        return summed(rows_of(0, e), rows_of(1, e))

    def frames_beside(e):
        both = rows_of(2, e)
        return summed(both, pltpu.roll(both, 16 if e < 8 else 112, 2))

    j = lax.broadcasted_iota(jnp.int32, (12, 16, 128), 2) % 32
    sub = lax.broadcasted_iota(jnp.int32, (12, 8, 128), 1)
    wrap = {0: (14, 0, 1), 1: (15, 0, 1), 10: (0, 31, 127), 11: (1, 31, 127)}
    for e in range(12):
        cell = frames(e + 2)
        if e in wrap:
            far, at, by = wrap[e]
            cell = cell + jnp.where(j == at, frames_beside(far), pltpu.roll(frames(far), by, 2))
        low, high = cell[:, 0:8], cell[:, 8:16]
        to_low = pltpu.roll(pltpu.roll(high, 32, 2), 4, 1)
        to_high = pltpu.roll(pltpu.roll(low, 96, 2), 4, 1)
        fs[e, :, 0:8] = low + jnp.where((sub == 2) | (sub == 3), to_low, 0.0)
        fs[e, :, 8:16] = high + jnp.where((sub == 4) | (sub == 5), to_high, 0.0)
    quarter = lax.broadcasted_iota(jnp.int32, (192, 128), 1) // 32
    for i in range(2):
        for k in range(3):
            row = None
            for q in range(4):
                part = fs[4 * k + q].reshape(192, 128)
                by = ((q - i) * 32) % 128
                if by:
                    part = pltpu.roll(part, by, 1)
                row = part if row is None else jnp.where(quarter == q, part, row)
            upper = row.astype(BF16)
            ll[192 * i : 192 * i + 192, 128 * k : 128 * k + 128] = upper
            ll[384 + 192 * i : 576 + 192 * i, 128 * k : 128 * k + 128] = (row - upper.astype(F32)).astype(BF16)
    pixels = dot(ll[...], back[...])
    pixels = (pixels[0:384] + pixels[384:768]).reshape(2, 12, 16, 384)
    for i in range(2):
        for cf in range(12):
            ch, f = cf // 4, cf % 4
            vg[f // 2, ch * 2 + f % 2, 12 * i : 12 * i + 12, :] = pixels[i, cf, 2:14, :]
    top = largest(vg[1 - m])
    ms[0:16] = spread(top, 384)
    ms[16:160] = coded(vg[1 - m], top)
    v_x = remote(ms, mr, partner)
    v_x.start()

    for one in (*v_p, *v_m, e_p, e_m):
        one.wait_recv()
    unfold(1, 2)
    merge(0)

    for one in (vf_p, vf_m, e_far, g_p[1], g_m[1], gf_p, gf_m):
        one.wait_recv()

    unfold(3)
    merge(1)

    give = []
    for p in range(PIECES):
        for ca in range(3):
            total = None
            for t in range(2):
                at = chosen(y, [s[t][ca] for s in SLOTS_OF])
                right = gbuf[t, :, :, :, 128 * WIDE * p : 128 * WIDE * (p + 1)].reshape(256, 128 * WIDE)
                part = dot(lm[at].reshape(256, 256), right)
                total = part if total is None else total + part
            for e in range(16):
                for n in range(WIDE):
                    wg[WIDE * p + n, pl.ds(ca * 256 + e, 16, stride=16), :] = (
                        total[16 * e : 16 * e + 16, 128 * n : 128 * n + 128]
                    )
        tiles = slice(WIDE * p, WIDE * p + WIDE)
        give.append(remote(wg.at[tiles, pl.ds((1 - core) * 384, 384)], cr.at[tiles], other))
        give[p].start()

    x1, x2, x3 = (x + 1) % 4, (x + 2) % 4, (x + 3) % 4
    far, near, last, tops = [], [], [], []
    halves = (slice(0, 2), slice(2, 4))
    ring = (xp, xm)
    beyond = (x1, x3)
    block = (WIDE, 2, 24, 128)
    for p in range(PIECES):
        tiles = slice(WIDE * p, WIDE * p + WIDE)
        give[p].wait_recv()
        for n in range(WIDE * p, WIDE * p + WIDE):
            for k in range(16):
                a1[n, k // 4, k % 4] = wg[n, pl.ds(core * 384 + 24 * k, 24), :] + cr[n, 24 * k : 24 * k + 24, :]
        tops.append(largest(a1[tiles]))
        for d in range(2):
            fo[d, p, 0:16] = spread(tops[p], 128)
            fo[d, p, 16:] = coded(a1[tiles, halves[d], x2], tops[p])
            far.append(remote(fo.at[d, p], fi.at[d, p], ring[d]))
            far[-1].start()
    for p in range(PIECES):
        tiles = slice(WIDE * p, WIDE * p + WIDE)
        for d in range(2):
            no[d, p] = coded(a1[tiles, halves[1 - d], beyond[d]], tops[p])
            near.append(remote(no.at[d, p], ni.at[d, p], ring[d]))
            near[-1].start()

    for p in range(PIECES):
        tiles = slice(WIDE * p, WIDE * p + WIDE)
        for d in range(2):
            far[2 * p + d].wait_recv()
            top = fi[d, p, 0:16].astype(F32)[0:1]
            total = a1[tiles, halves[d], beyond[d]] + decoded(fi[d, p, 16:], top, block)
            top = ((top[:, 0:1] + tops[p]) * 1.01).astype(BF16).astype(F32)
            lo[d, p, 0:16] = spread(top, 128)
            lo[d, p, 16:] = coded(total, top)
            last.append(remote(lo.at[d, p], li.at[d, p], ring[d]))
            last[-1].start()

    z_out = []
    for p in range(PIECES):
        tiles = slice(WIDE * p, WIDE * p + WIDE)
        for d in range(2):
            near[2 * p + d].wait_recv()
            top = fi[d, p, 0:16].astype(F32)[0:1]
            a1[tiles, halves[1 - d], x] = a1[tiles, halves[1 - d], x] + decoded(ni[d, p], top, block)
        for d in range(2):
            last[2 * p + d].wait_recv()
            top = li[d, p, 0:16].astype(F32)[0:1]
            a2[tiles, halves[d]] = a1[tiles, halves[d], x] + decoded(li[d, p, 16:], top, block)
        z_out.append([remote(a2.at[tiles, (z + d + 1) % 4], zr.at[d, tiles], zs[d]) for d in (2, 1, 0)])
        for one in z_out[p]:
            one.start()

    v_x.wait_recv()
    vg[m] = vg[m] + decoded(mr[16:160], mr[0:16].astype(F32)[0:1], (6, 24, 384))
    v_out = pltpu.make_async_copy(vg.at[m], vout, load.at[11])
    v_out.start()

    for p in range(PIECES):
        for one in z_out[p]:
            one.wait_recv()
        for n in range(WIDE * p, WIDE * p + WIDE):
            wout[:, 128 * n : 128 * n + 128] = (a2[n, z] + zr[0, n] + (zr[1, n] + zr[2, n])) * (1.0 / 128.0)

    v_out.wait()
    for copy, sent, _ in halo + token_halo:
        pl.when(sent)(lambda copy=copy: copy.wait_send())
    pl.when(g_sent)(g_out.wait_send)
    for one in (
        *g_p, *g_m, g_in, gf_p, gf_m, *v_far_p, *v_far_m, *v_p, *v_m, vf_p, vf_m, e_p, e_m, e_far, v_x,
        *give, *far, *near, *last, *sum(z_out, []),
    ):
        one.wait_send()


def put_out(video_grad, weight_grad, vout, wout, held, sem):
    parts = 3
    arrive = [
        pltpu.make_async_copy(video_grad.at[pl.ds(2 * k, 2)], held.at[pl.ds(2 * k, 2)], sem.at[k])
        for k in range(parts)
    ]
    leave = [
        pltpu.make_async_copy(held.at[pl.ds(2 * k, 2)], vout.at[pl.ds(2 * k, 2)], sem.at[parts + k])
        for k in range(parts)
    ]
    last = pltpu.make_async_copy(weight_grad, wout, sem.at[2 * parts])
    for one in arrive:
        one.start()
    last.start()
    for a, b in zip(arrive, leave):
        a.wait()
        b.start()
    for one in leave:
        one.wait()
    last.wait()


def shards(video, grad_tokens, weight):
    packed = jnp.asarray(selections(), BF16)
    anywhere = pl.BlockSpec(memory_space=pltpu.HBM)
    in_vmem = pl.BlockSpec(memory_space=pltpu.VMEM)

    def v(*shape, kind=F32):
        return pltpu.VMEM(shape, kind)

    def b(*shape):
        return pltpu.VMEM(shape, BF16)

    video_grad, weight_grad = pl.pallas_call(
        kernel,
        out_shape=(
            jax.ShapeDtypeStruct((6, 24, 384), F32),
            jax.ShapeDtypeStruct((24, 512), F32),
        ),
        in_specs=[anywhere] * 5,
        out_specs=(pl.BlockSpec(memory_space=pl.ANY), in_vmem),
        scratch_shapes=[
            b(SELECTION_ROWS, 512),
            b(3072, 512), b(384, 384), b(12, 24, 384), b(4, 4, 32, 384), b(2, 2, 24, 384), b(64, 384),
            b(6, 16, 384), b(8, 16, 512), b(16, 384), b(16, 512), b(16, 384), b(4, 16, 512), b(4, 16, 512),
            b(2, 4, 32, 512), b(256, 512), b(2, 4, 2, 32, 512), b(144, 512),
            b(4, 2, 4, 16, 512), b(5, 16, 16, 256),
            v(3, 3072, 128), v(12, 12, 16, 128), b(768, 384), v(2, 6, 24, 384), b(160, 384), b(160, 384),
            v(4, 768, 128), v(4, 384, 128), v(4, 4, 4, 24, 128),
            *[b(2, PIECES, rows, 128) for rows in (CODED + 16, CODED + 16, CODED, CODED, CODED + 16, CODED + 16)],
            v(4, 4, 24, 128),
            v(3, 4, 24, 128),
            pltpu.SemaphoreType.DMA((12,)),
            pltpu.SemaphoreType.DMA((N_SEMS,)),
            pltpu.SemaphoreType.DMA((N_SEMS,)),
        ],
        compiler_params=pltpu.CompilerParams(
            collective_id=0, has_side_effects=True, vmem_limit_bytes=VMEM_BYTES
        ),
        name="tubelet_backward",
    )(video.reshape(288, 384), video.reshape(12, 24, 384), grad_tokens, weight, packed)
    video_grad, weight_grad = pl.pallas_call(
        put_out,
        out_shape=(
            jax.ShapeDtypeStruct((6, 24, 384), F32),
            jax.ShapeDtypeStruct((24, 512), F32),
        ),
        in_specs=[anywhere, in_vmem],
        out_specs=(anywhere, anywhere),
        scratch_shapes=[v(6, 24, 384), pltpu.SemaphoreType.DMA((7,))],
        compiler_params=pltpu.CompilerParams(vmem_limit_bytes=VMEM_BYTES),
        name="put_out",
    )(video_grad, weight_grad)
    return video_grad.reshape(3, 2, 24, 384), weight_grad


def solution(mesh):
    return jax.shard_map(
        shards,
        mesh=mesh,
        in_specs=(P(None, None, "row", "col"), P(None, "row", "col", "mp"), P(None, "mp")),
        out_specs=(P(None, "mp", "row", "col"), P(("row", "col"), "mp")),
        check_vma=False,
    )
```
